32 devices in a mesh: dp: 1 (over z), cp: 32 (over y, x, core).
Axes of the slice: x: 4, y: 4, z: 1, core: 2. Of those that a mesh axis runs over, the one named last changes fastest.
The devices are a block of a 4x4x8 slice.
Arguments:
- x: bfloat16 [8192, 3072], P(('dp', 'cp'))
- seg: int32 [8192], P(('dp', 'cp'))
- wq: bfloat16 [3072, 3072], replicated
- wk: bfloat16 [3072, 1024], replicated
- wv: bfloat16 [3072, 1024], replicated
- wo: bfloat16 [3072, 3072], replicated
Outputs:
- output: bfloat16 [8192, 3072], P(('dp', 'cp'))
All inputs are finite; a program needn't handle non-finite values.
Results may differ from the reference program's by a relative error of at most 0.00598599.
Values are sent between devices in bfloat16 or wider.
A program may use at most 768 MiB of HBM per device.

```python
import jax
import jax.numpy as jnp
from jax import lax
import numpy as np

CP = 32
L = 256
D = 3072
HQ = 24
HKV = 8
DH = 128

S = CP * L
HALF = L // 2
G = HQ // HKV
QB = min(128, HALF)


def row_positions():
    rows = []
    for d in range(CP):
        rows.append(np.arange(d * HALF, (d + 1) * HALF))
        rows.append(np.arange((2 * CP - 1 - d) * HALF, (2 * CP - d) * HALF))
    return np.concatenate(rows).astype(np.int32)


def setup_inputs(seed: int = 0, part: int = 0) -> dict:
    key = jax.random.key(seed)
    kshared, kpart = jax.random.split(key)
    kp = jax.random.fold_in(kpart, part)
    kx, _, _ = jax.random.split(kp, 3)
    kd = jax.random.fold_in(kp, 7)
    ku, kc, kl = jax.random.split(kd, 3)
    kq, kk, kv, ko = jax.random.split(kshared, 4)
    x = jax.random.normal(kx, (S, D), jnp.float32).astype(jnp.bfloat16)
    token_pos = jnp.arange(S, dtype=jnp.int32)
    long_end = jax.random.randint(kl, (), 3 * S // 10, 7 * S // 10, jnp.int32)
    coin_flip = jax.random.randint(kc, (2 * CP,), 0, 2, jnp.int32)
    break_bar = jnp.repeat(jnp.where(coin_flip == 0, jnp.int32(1 << 22), jnp.int32((1 << 24) // L)), HALF)
    draw_bits = (jax.random.bits(ku, (S,), jnp.uint32) >> 8).astype(jnp.int32)
    breaks = (draw_bits < break_bar) & (token_pos > long_end)
    seg_orig = 7 + jnp.cumsum(breaks.astype(jnp.int32))
    seg = seg_orig[jnp.asarray(row_positions())].astype(jnp.int32)
    wq = (jax.random.normal(kq, (D, HQ * DH), jnp.float32) * (2.0 * D ** -0.5)).astype(jnp.bfloat16)
    wk = (jax.random.normal(kk, (D, HKV * DH), jnp.float32) * D ** -0.5).astype(jnp.bfloat16)
    wv = (jax.random.normal(kv, (D, HKV * DH), jnp.float32) * D ** -0.5).astype(jnp.bfloat16)
    wo = (jax.random.normal(ko, (HQ * DH, D), jnp.float32) * (HQ * DH) ** -0.5).astype(jnp.bfloat16)
    return {"x": x, "seg": seg, "wq": wq, "wk": wk, "wv": wv, "wo": wo}


def reference(x, seg, wq, wk, wv, wo):
    pos = jnp.asarray(row_positions())
    q = jnp.dot(x, wq, preferred_element_type=jnp.float32).astype(jnp.bfloat16)
    k = jnp.dot(x, wk, preferred_element_type=jnp.float32).astype(jnp.bfloat16)
    v = jnp.dot(x, wv, preferred_element_type=jnp.float32).astype(jnp.bfloat16)
    kf = k.astype(jnp.float32).reshape(S, HKV, DH)
    vf = v.astype(jnp.float32).reshape(S, HKV, DH)
    qb = q.reshape(S // QB, QB, HKV, G, DH)
    pb = pos.reshape(S // QB, QB)
    sb = seg.reshape(S // QB, QB)

    def block(args):
        qi, pi, si = args
        s = jnp.einsum("qhgd,khd->hgqk", qi.astype(jnp.float32), kf) * DH ** -0.5
        allowed = (si[:, None] == seg[None, :]) & (pos[None, :] <= pi[:, None])
        s = jnp.where(allowed, s, -jnp.inf)
        p = jax.nn.softmax(s, axis=-1)
        o = jnp.einsum("hgqk,khd->qhgd", p, vf)
        return o.astype(jnp.bfloat16)

    o = lax.map(block, (qb, pb, sb)).reshape(S, HQ * DH)
    return jnp.dot(o, wo, preferred_element_type=jnp.float32).astype(jnp.bfloat16)
```

```python
import functools
import math

import jax
import jax.numpy as jnp
from jax import lax
from jax.experimental import pallas as pl
from jax.experimental.pallas import tpu as pltpu
from jax.sharding import PartitionSpec as P

DH = 128
PC = 128
KB = 4
MESH = pl.DeviceIdType.MESH
NEG_INF = float("-inf")


class Place:
    def __init__(self, n):
        me = lax.axis_index("cp")
        self.n, self.side = n, math.isqrt(n // 2)
        self.me = me
        self.c = lax.rem(me, 2)
        chip = me // 2
        self.x = lax.rem(chip, self.side)
        self.y = chip // self.side
        self.xin = self.x + 1 - 2 * lax.rem(self.x, 2)
        self.xcross = self.side - 1 - self.x
        self.px = lax.rem(lax.rem(self.x, 2) + self.x // 2, 2)

    def dev(self, x, y, c):
        return (y * self.side + x) * 2 + c

    def row(self, dy):
        return lax.rem(self.y + dy + self.side, self.side)

    def col(self, dx):
        return self.xin if dx else self.x

    def peer(self, dx, dy):
        return self.dev(self.col(dx), self.row(dy), self.c)

    def head(self, dx, dy):
        return lax.rem(self.px + dx, 2) * self.side + self.row(dy)

    def slot(self, dx, dy):
        return self.row(dy) * 2 + lax.rem(self.x + dx, 2)


def _order(side):
    return [2, 1, -1, 0]


def _project(n, g, x_ref, seg_ref, wk, wv, wq, kv_o, q_o, segs_o, wkvb, wqb, kvb, qb, skv, sq, segb,
             wkv_sem, wq_sem, kv_send, kv_recv, fx_send, fs_send, q_send, q_recv, seg_send, seg_recv, out_sem, qout_sem):
    pt = Place(n)
    me = pt.me
    order = _order(pt.side)
    steps = [(t, dx, dy) for t, dy in enumerate(order) for dx in range(2)]
    gd = g * DH

    def wkv_copies(t):
        for dx in range(2):
            h = pl.multiple_of(pt.head(dx, order[t]) * DH, DH)
            for i, w in enumerate((wk, wv)):
                yield pltpu.make_async_copy(w.at[:, pl.ds(h, DH)], wkvb.at[t, :, pl.ds((2 * dx + i) * DH, DH)],
                                            wkv_sem.at[t, 2 * dx + i])

    def wq_copies(t):
        for dx in range(2):
            h = pl.multiple_of(pt.head(dx, order[t]) * gd, DH)
            yield pltpu.make_async_copy(wq.at[:, pl.ds(h, gd)], wqb.at[t, :, pl.ds(dx * gd, gd)], wq_sem.at[t, dx])

    for t in range(len(order)):
        for cp in wkv_copies(t):
            cp.start()
    for t in range(len(order)):
        for cp in wq_copies(t):
            cp.start()

    barrier = pltpu.get_barrier_semaphore()

    @pl.loop(1, n)
    def _(i):
        pl.semaphore_signal(barrier, inc=1, device_id={"cp": lax.rem(me + i, n)}, device_id_type=MESH)

    pl.semaphore_wait(barrier, n - 1)

    def seg_copy(i):
        return pltpu.make_async_remote_copy(seg_ref, segb.at[pl.ds(me, 1)], seg_send.at[i], seg_recv.at[me],
                                            device_id={"cp": lax.rem(me + i, n)}, device_id_type=MESH)

    @pl.loop(1, n)
    def _(i):
        seg_copy(i).start()

    segb[pl.ds(me, 1)] = seg_ref[...]

    def kv_copy(t, dx, dy):
        return pltpu.make_async_remote_copy(skv.at[2 * t + dx], kvb.at[me], kv_send.at[2 * t + dx], kv_recv.at[me],
                                            device_id={"cp": pt.peer(dx, dy)}, device_id_type=MESH)

    def q_copy(t, dx, dy):
        return pltpu.make_async_remote_copy(sq.at[2 * t + dx], qb.at[pt.slot(0, 0)], q_send.at[2 * t + dx],
                                            q_recv.at[pt.slot(0, 0)],
                                            device_id={"cp": pt.peer(dx, dy)}, device_id_type=MESH)

    def kv_step(t):
        for cp in wkv_copies(t):
            cp.wait()
        r = jnp.dot(x_ref[...], wkvb[t], preferred_element_type=jnp.float32)
        for dx in range(2):
            kt = jnp.transpose(r[:, 2 * dx * DH:(2 * dx + 1) * DH]).astype(jnp.bfloat16)
            v = r[:, (2 * dx + 1) * DH:(2 * dx + 2) * DH].astype(jnp.bfloat16)
            own = order[t] == 0 and dx == 0
            for half in range(2):
                kth = kt[:, half * PC:(half + 1) * PC]
                vh = v[half * PC:(half + 1) * PC, :]
                if own:
                    kvb[me, half, 0] = kth
                    kvb[me, half, 1] = vh
                else:
                    skv[2 * t + dx, half, 0] = kth
                    skv[2 * t + dx, half, 1] = vh

    def q_step(t):
        for cp in wq_copies(t):
            cp.wait()
        r = jnp.dot(x_ref[...], wqb[t], preferred_element_type=jnp.float32).astype(jnp.bfloat16)
        for dx in range(2):
            own = order[t] == 0 and dx == 0
            for half in range(2):
                for i in range(g):
                    piece = r[half * PC:(half + 1) * PC, dx * gd + i * DH:dx * gd + (i + 1) * DH]
                    if own:
                        qb[pt.slot(0, 0), half, i] = piece
                    else:
                        sq[2 * t + dx, half, i] = piece

    def send(copy, t):
        for dx in range(2):
            if not (order[t] == 0 and dx == 0):
                copy(t, dx, order[t]).start()

    def to_cross(src, i):
        return pltpu.make_async_remote_copy(kvb.at[src], kvb.at[src], fx_send.at[i], kv_recv.at[src],
                                            device_id={"cp": pt.dev(pt.xcross, pt.y, pt.c)}, device_id_type=MESH)

    def to_sibling(src, i):
        return pltpu.make_async_remote_copy(kvb.at[src], kvb.at[src], fs_send.at[i], kv_recv.at[src],
                                            device_id={"cp": pt.dev(pt.x, pt.y, 1 - pt.c)}, device_id_type=MESH)

    def kv_out(src):
        return pltpu.make_async_copy(kvb.at[src], kv_o.at[src], out_sem.at[src])

    def q_out(slot):
        return pltpu.make_async_copy(qb.at[slot], q_o.at[slot], qout_sem.at[slot])

    def arrived(src):
        to_sibling(src, 0).wait_recv()

    def forward(t):
        for dx in range(2):
            dy = order[t]
            src = pt.peer(dx, -dy)
            if not (dy == 0 and dx == 0):
                arrived(src)
            to_cross(src, 2 * t + dx).start()
            to_sibling(src, 2 * t + dx).start()
            kv_out(src).start()

    kv_step(0)
    kv_step(1)
    send(kv_copy, 0)
    kv_step(2)
    send(kv_copy, 1)
    kv_step(3)
    send(kv_copy, 2)
    q_step(0)
    send(kv_copy, 3)
    q_step(1)
    send(q_copy, 0)
    forward(0)
    q_step(2)
    send(q_copy, 1)
    forward(1)
    q_step(3)
    send(q_copy, 2)
    forward(2)
    forward(3)
    send(q_copy, 3)

    def mirrored(dx, dy, c):
        x = pt.side - 1 - pt.col(dx)
        return pt.dev(x, pt.row(-dy), c)

    for t, dx, dy in steps:
        src = mirrored(dx, dy, pt.c)
        arrived(src)
        to_sibling(src, 8 + 2 * t + dx).start()
        kv_out(src).start()

    for t, dx, dy in steps:
        src = pt.dev(pt.col(dx), pt.row(-dy), 1 - pt.c)
        arrived(src)
        kv_out(src).start()
    for t, dx, dy in steps:
        slot = pt.slot(dx, -dy)
        if not (dy == 0 and dx == 0):
            pltpu.make_async_remote_copy(qb.at[slot], qb.at[slot], q_send.at[0], q_recv.at[slot],
                                         device_id={"cp": me}, device_id_type=MESH).wait_recv()
        q_out(slot).start()
    for t, dx, dy in steps:
        src = mirrored(dx, dy, 1 - pt.c)
        arrived(src)
        kv_out(src).start()

    @pl.loop(1, n)
    def _(i):
        src = lax.rem(me + i, n)
        pltpu.make_async_remote_copy(seg_ref, segb.at[pl.ds(src, 1)], seg_send.at[i], seg_recv.at[src],
                                     device_id={"cp": src}, device_id_type=MESH).wait_recv()

    segs_o[...] = segb[...]

    @pl.loop(1, n)
    def _(i):
        seg_copy(i).wait_send()

    for t, dx, dy in steps:
        if not (dy == 0 and dx == 0):
            kv_copy(t, dx, dy).wait_send()
            q_copy(t, dx, dy).wait_send()
        src = pt.peer(dx, -dy)
        to_cross(src, 2 * t + dx).wait_send()
        to_sibling(src, 2 * t + dx).wait_send()
        to_sibling(src, 8 + 2 * t + dx).wait_send()

    @pl.loop(0, n)
    def _(i):
        kv_out(i).wait()

    @pl.loop(0, n // 4)
    def _(i):
        q_out(i).wait()


def _attend(n, g, scale, seg_s, seg_v, kv, q_ref, o_ref, kvs, m_sc, l_sc, acc_sc, sem):
    pt = Place(n)
    last_piece = 2 * n - 1
    rows = g * PC

    def owner(p):
        return jnp.where(p < n, p, last_piece - p)

    def half_of(p):
        return jnp.where(p < n, 0, 1)

    def load(p):
        return pltpu.make_async_copy(kv.at[owner(p), half_of(p)], kvs.at[p], sem)

    @pl.loop(0, 2 * n)
    def _(p):
        load(p).start()

    @pl.loop(0, 2 * n)
    def _(p):
        load(p).wait()

    def lanes(col):
        return jnp.broadcast_to(col, (col.shape[0], DH))

    def one(i, carry):
        slot, half = i // 2, lax.rem(i, 2)
        xs = (pt.x // 2) * 2 + lax.rem(slot, 2)
        src = pt.dev(xs, slot // 2, pt.c)
        p = jnp.where(half == 0, src, last_piece - src)
        first = seg_s[src, half, 0]

        def search(_, lohi):
            lo, hi = lohi
            mid = (lo + hi) // 2
            ok = seg_s[owner(mid), half_of(mid), PC - 1] >= first
            return jnp.where(ok, lo, jnp.minimum(mid + 1, hi)), jnp.where(ok, mid, hi)

        lo, _ = lax.fori_loop(0, int(math.log2(2 * n)) + 1, search, (jnp.int32(0), p))
        q = q_ref[slot, half].reshape(rows, DH)

        m_sc[...] = jnp.full_like(m_sc, NEG_INF)
        l_sc[...] = jnp.zeros_like(l_sc)
        acc_sc[...] = jnp.zeros_like(acc_sc)

        def off(b, carry):
            j0 = lo + b * KB
            js = jnp.minimum(j0, 2 * n - KB)
            kt = jnp.concatenate([kvs[js + u, 0] for u in range(KB)], axis=1)
            v = jnp.concatenate([kvs[js + u, 1] for u in range(KB)], axis=0)
            bias = []
            for u in range(KB):
                j = js + u
                want = jnp.where((j >= j0) & (j < p), first, -1)
                ids = seg_v[owner(j), pl.ds(half_of(j), 1), :]
                bias.append(jnp.where(ids == want, 0.0, NEG_INF))
            s = jnp.dot(q, kt, preferred_element_type=jnp.float32) * scale
            parts = [s[:, u * PC:(u + 1) * PC] + bias[u] for u in range(KB)]
            top = functools.reduce(jnp.maximum, parts)
            m_old = m_sc[...]
            m_new = jnp.maximum(m_old, lanes(jnp.max(top, axis=1, keepdims=True)))
            corr = jnp.exp2(m_old - m_new)
            ps = [jnp.exp2(t - m_new) for t in parts]
            l_sc[...] = l_sc[...] * corr + functools.reduce(jnp.add, ps)
            pb = jnp.concatenate([t.astype(jnp.bfloat16) for t in ps], axis=1)
            acc_sc[...] = acc_sc[...] * corr + jnp.dot(pb, v, preferred_element_type=jnp.float32)
            m_sc[...] = m_new
            return carry

        lax.fori_loop(0, (p - lo + KB - 1) // KB, off, 0)

        ids = jnp.broadcast_to(seg_v[src, pl.ds(half, 1), :], (PC, PC))
        ids_t = jnp.transpose(ids)
        r = lax.broadcasted_iota(jnp.int32, (PC, PC), 0)
        cidx = lax.broadcasted_iota(jnp.int32, (PC, PC), 1)
        allowed = (ids == ids_t) & (cidx <= r)
        keep = jnp.concatenate([ids_t == first] * g, axis=0)
        allowed = jnp.concatenate([allowed] * g, axis=0)
        s = jnp.dot(q, kvs[p, 0], preferred_element_type=jnp.float32) * scale
        s = jnp.where(allowed, s, NEG_INF)
        m_old = jnp.where(keep, m_sc[...], NEG_INF)
        m_new = jnp.maximum(m_old, lanes(jnp.max(s, axis=1, keepdims=True)))
        corr = jnp.exp2(m_old - m_new)
        pr = jnp.exp2(s - m_new)
        l = jnp.where(keep, l_sc[...], 0.0) * corr + pr
        acc = jnp.where(keep, acc_sc[...], 0.0) * corr
        acc = acc + jnp.dot(pr.astype(jnp.bfloat16), kvs[p, 1], preferred_element_type=jnp.float32)
        o = (acc / lanes(jnp.sum(l, axis=1, keepdims=True))).astype(jnp.bfloat16)
        for u in range(g):
            o_ref[slot, pl.ds(pl.multiple_of(half * PC, PC), PC), u * DH:(u + 1) * DH] = o[u * PC:(u + 1) * PC]
        return carry

    lax.fori_loop(0, n // 2, one, 0)


def _combine(n, gd, o_in, wo, y_ref, obuf, wob, acc, w_sem, o_send, o_recv):
    pt = Place(n)
    me = pt.me
    order = [-d for d in reversed(_order(pt.side))]
    my_head = pt.head(0, 0)
    d_out = y_ref.shape[1]
    nc = 4
    wn = d_out // nc

    def w_copies(t):
        for dx in range(2):
            h = pl.multiple_of(pt.head(dx, order[t]) * gd, gd)
            yield pltpu.make_async_copy(wo.at[pl.ds(h, gd), :], wob.at[t, pl.ds(dx * gd, gd), :], w_sem.at[t, dx])

    for t in range(len(order)):
        for cp in w_copies(t):
            cp.start()
    own = pltpu.make_async_copy(o_in.at[pt.slot(0, 0)], obuf.at[my_head], o_recv.at[my_head])
    own.start()

    steps = [(t, dx, dy) for t, dy in enumerate(order) for dx in range(2)]
    others = [s for s in steps if (s[1], s[2]) != (0, 0)]
    barrier = pltpu.get_barrier_semaphore()
    for t, dx, dy in others:
        pl.semaphore_signal(barrier, inc=1, device_id={"cp": pt.peer(dx, dy)}, device_id_type=MESH)
    pl.semaphore_wait(barrier, len(others))

    def o_copy(t, dx, dy):
        return pltpu.make_async_remote_copy(o_in.at[pt.slot(dx, dy)], obuf.at[my_head], o_send.at[2 * t + dx],
                                            o_recv.at[my_head], device_id={"cp": pt.peer(dx, dy)}, device_id_type=MESH)

    for s in reversed(others):
        o_copy(*s).start()

    for t, dy in enumerate(order):
        for cp in w_copies(t):
            cp.wait()
        heads = [pt.head(dx, dy) for dx in range(2)]
        for dx in range(2):
            if dy == 0 and dx == 0:
                own.wait()
            else:
                pltpu.make_async_remote_copy(obuf.at[heads[dx]], obuf.at[heads[dx]], o_send.at[0], o_recv.at[heads[dx]],
                                             device_id={"cp": me}, device_id_type=MESH).wait_recv()
        a = jnp.concatenate([obuf[heads[0]], obuf[heads[1]]], axis=1)
        for u in range(nc):
            r = jnp.dot(a, wob[t, :, u * wn:(u + 1) * wn], preferred_element_type=jnp.float32)
            if t > 0:
                r = r + acc[:, u * wn:(u + 1) * wn]
            if t < len(order) - 1:
                acc[:, u * wn:(u + 1) * wn] = r
            else:
                y_ref[:, u * wn:(u + 1) * wn] = r.astype(y_ref.dtype)
    for s in others:
        o_copy(*s).wait_send()


def solution(mesh):
    n = mesh.shape["cp"]
    side = math.isqrt(n // 2)
    bf, f32 = jnp.bfloat16, jnp.float32
    vmem, anym = pl.BlockSpec(memory_space=pltpu.VMEM), pl.BlockSpec(memory_space=pl.ANY)
    dma = pltpu.SemaphoreType.DMA

    def local(x, seg, wq, wk, wv, wo):
        lq, d = x.shape
        hkv = wk.shape[1] // DH
        g = wq.shape[1] // wk.shape[1]
        gd = g * DH
        ng = 2 * side
        kv, q, segs = pl.pallas_call(
            functools.partial(_project, n, g),
            out_shape=(jax.ShapeDtypeStruct((n, 2, 2, PC, DH), bf), jax.ShapeDtypeStruct((ng, 2, g, PC, DH), bf),
                       jax.ShapeDtypeStruct((n, 2, PC), jnp.int32)),
            in_specs=[vmem, vmem, anym, anym, anym],
            out_specs=(anym, anym, vmem),
            scratch_shapes=[
                pltpu.VMEM((side, d, 4 * DH), bf), pltpu.VMEM((side, d, 2 * gd), bf),
                pltpu.VMEM((n, 2, 2, PC, DH), bf), pltpu.VMEM((ng, 2, g, PC, DH), bf),
                pltpu.VMEM((ng, 2, 2, PC, DH), bf), pltpu.VMEM((ng, 2, g, PC, DH), bf),
                pltpu.VMEM((n, 2, PC), jnp.int32),
                dma((side, 4)), dma((side, 2)), dma((ng,)), dma((n,)), dma((ng,)), dma((2 * ng,)),
                dma((ng,)), dma((ng,)), dma((n,)), dma((n,)), dma((n,)), dma((ng,)),
            ],
            compiler_params=pltpu.CompilerParams(collective_id=0, has_side_effects=True, vmem_limit_bytes=60 << 20),
            name="project",
        )(x, seg.reshape(1, 2, PC), wk, wv, wq)
        scale = DH ** -0.5 * math.log2(math.e)
        o = pl.pallas_call(
            functools.partial(_attend, n, g, scale),
            out_shape=jax.ShapeDtypeStruct((ng, lq, gd), bf),
            in_specs=[pl.BlockSpec(memory_space=pltpu.SMEM), vmem, anym, vmem],
            out_specs=vmem,
            scratch_shapes=[pltpu.VMEM((2 * n, 2, PC, DH), bf), pltpu.VMEM((g * PC, DH), f32),
                            pltpu.VMEM((g * PC, DH), f32), pltpu.VMEM((g * PC, DH), f32), dma],
            compiler_params=pltpu.CompilerParams(vmem_limit_bytes=40 << 20),
            name="attend",
        )(segs, segs, kv, q)
        return pl.pallas_call(
            functools.partial(_combine, n, gd),
            out_shape=jax.ShapeDtypeStruct((lq, wo.shape[1]), bf),
            in_specs=[anym, anym],
            out_specs=vmem,
            scratch_shapes=[pltpu.VMEM((hkv, lq, gd), bf), pltpu.VMEM((side, 2 * gd, wo.shape[1]), bf),
                            pltpu.VMEM((lq, wo.shape[1]), f32), dma((side, 2)), dma((ng,)), dma((ng,))],
            compiler_params=pltpu.CompilerParams(collective_id=1, has_side_effects=True, vmem_limit_bytes=60 << 20),
            name="combine",
        )(o, wo)

    rows = P(("dp", "cp"), None)
    return jax.shard_map(local, mesh=mesh, in_specs=(rows, P(("dp", "cp")), P(), P(), P(), P()), out_specs=rows, check_vma=False)
```

```python
import functools
import math

import jax
import jax.numpy as jnp
from jax import lax
from jax.experimental import pallas as pl
from jax.experimental.pallas import tpu as pltpu
from jax.sharding import PartitionSpec as P

DH = 128
PC = 128
KB = 4
MESH = pl.DeviceIdType.MESH
NEG_INF = float("-inf")


class Place:
    def __init__(self, n):
        me = lax.axis_index("cp")
        self.n, self.side = n, math.isqrt(n // 2)
        self.me = me
        self.c = lax.rem(me, 2)
        chip = me // 2
        self.x = lax.rem(chip, self.side)
        self.y = chip // self.side
        self.xin = self.x + 1 - 2 * lax.rem(self.x, 2)
        self.xcross = self.side - 1 - self.x
        self.px = lax.rem(lax.rem(self.x, 2) + self.x // 2, 2)

    def dev(self, x, y, c):
        return (y * self.side + x) * 2 + c

    def row(self, dy):
        return lax.rem(self.y + dy + self.side, self.side)

    def col(self, dx):
        return self.xin if dx else self.x

    def peer(self, dx, dy):
        return self.dev(self.col(dx), self.row(dy), self.c)

    def head(self, dx, dy):
        return lax.rem(self.px + dx, 2) * self.side + self.row(dy)

    def slot(self, dx, dy):
        return self.row(dy) * 2 + lax.rem(self.x + dx, 2)


FAR = 2
KV_ORDER = (FAR, 0, 1, -1)
Q_ORDER = (FAR, 1, -1, 0)
O_ORDER = (0, 1, -1, FAR)


def _project(n, g, x_ref, seg_ref, wk, wv, wq, kv_o, q_o, segs_o, wkvb, wqb, kvb, qb, skv, sq, rkv, rq, segb,
             wkv_sem, wq_sem, kv_send, kv_recv, kvf_recv, rkv_recv, rkv_send, fx_send, fs_send,
             q_send, q_recv, qf_recv, rq_recv, rq_send, seg_send, seg_recv, out_sem, qout_sem):
    pt = Place(n)
    me = pt.me
    kv_steps = [(t, dx, dy) for t, dy in enumerate(KV_ORDER) for dx in range(2)]
    q_steps = [(t, dx, dy) for t, dy in enumerate(Q_ORDER) for dx in range(2)]
    own_kv = (KV_ORDER.index(0), 0)
    own_q = (Q_ORDER.index(0), 0)
    gd = g * DH

    def wkv_copies(t):
        for dx in range(2):
            h = pl.multiple_of(pt.head(dx, KV_ORDER[t]) * DH, DH)
            for i, w in enumerate((wk, wv)):
                yield pltpu.make_async_copy(w.at[:, pl.ds(h, DH)], wkvb.at[t, :, pl.ds((2 * dx + i) * DH, DH)],
                                            wkv_sem.at[t, 2 * dx + i])

    def wq_copies(t):
        for dx in range(2):
            h = pl.multiple_of(pt.head(dx, Q_ORDER[t]) * gd, DH)
            yield pltpu.make_async_copy(wq.at[:, pl.ds(h, gd)], wqb.at[t, :, pl.ds(dx * gd, gd)], wq_sem.at[t, dx])

    for t in range(len(KV_ORDER)):
        for cp in wkv_copies(t):
            cp.start()
    for t in range(len(Q_ORDER)):
        for cp in wq_copies(t):
            cp.start()

    barrier = pltpu.get_barrier_semaphore()

    @pl.loop(1, n)
    def _(i):
        pl.semaphore_signal(barrier, inc=1, device_id={"cp": lax.rem(me + i, n)}, device_id_type=MESH)

    pl.semaphore_wait(barrier, n - 1)

    def seg_copy(i):
        return pltpu.make_async_remote_copy(seg_ref, segb.at[pl.ds(me, 1)], seg_send.at[i], seg_recv.at[me],
                                            device_id={"cp": lax.rem(me + i, n)}, device_id_type=MESH)

    @pl.loop(1, n)
    def _(i):
        seg_copy(i).start()

    segb[pl.ds(me, 1)] = seg_ref[...]

    def put(src, dst, send, recv, dev):
        return pltpu.make_async_remote_copy(src, dst, send, recv, device_id={"cp": dev}, device_id_type=MESH)

    def kv_copy(t, dx, dy):
        return put(skv.at[2 * t + dx], kvb.at[me], kv_send.at[2 * t + dx], kv_recv.at[me], pt.peer(dx, dy))

    def q_copy(t, dx, dy):
        return put(sq.at[2 * t + dx], qb.at[pt.slot(0, 0)], q_send.at[2 * t + dx], q_recv.at[pt.slot(0, 0)], pt.peer(dx, dy))

    way = (1, -1)
    hops = [(half, dx) for half in range(2) for dx in range(2)]

    def kv_hop(half, dx):
        return put(skv.at[dx, half], rkv.at[half, dx], kv_send.at[2 * half + dx if half == 0 else 2 * len(KV_ORDER) + dx],
                   rkv_recv.at[half, dx], pt.peer(0, way[half]))

    def kv_hand(half, dx):
        return put(rkv.at[half, dx], kvb.at[pt.peer(0, -way[half]), half], rkv_send.at[half, dx], kvf_recv.at[dx, half],
                   pt.peer(dx, way[half]))

    def q_hop(half, dx):
        return put(sq.at[dx, half], rq.at[half, dx], q_send.at[2 * half + dx if half == 0 else 2 * len(Q_ORDER) + dx],
                   rq_recv.at[half, dx], pt.peer(0, way[half]))

    def q_hand(half, dx):
        return put(rq.at[half, dx], qb.at[pt.slot(0, -way[half]), half], rq_send.at[half, dx], qf_recv.at[dx, half],
                   pt.peer(dx, way[half]))

    def kv_step(t):
        for cp in wkv_copies(t):
            cp.wait()
        r = jnp.dot(x_ref[...], wkvb[t], preferred_element_type=jnp.float32)
        for dx in range(2):
            kt = jnp.transpose(r[:, 2 * dx * DH:(2 * dx + 1) * DH]).astype(jnp.bfloat16)
            v = r[:, (2 * dx + 1) * DH:(2 * dx + 2) * DH].astype(jnp.bfloat16)
            own = (t, dx) == own_kv
            for half in range(2):
                kth = kt[:, half * PC:(half + 1) * PC]
                vh = v[half * PC:(half + 1) * PC, :]
                if own:
                    kvb[me, half, 0] = kth
                    kvb[me, half, 1] = vh
                else:
                    skv[2 * t + dx, half, 0] = kth
                    skv[2 * t + dx, half, 1] = vh

    def q_step(t):
        for cp in wq_copies(t):
            cp.wait()
        r = jnp.dot(x_ref[...], wqb[t], preferred_element_type=jnp.float32).astype(jnp.bfloat16)
        for dx in range(2):
            own = (t, dx) == own_q
            for half in range(2):
                for i in range(g):
                    piece = r[half * PC:(half + 1) * PC, dx * gd + i * DH:dx * gd + (i + 1) * DH]
                    if own:
                        qb[pt.slot(0, 0), half, i] = piece
                    else:
                        sq[2 * t + dx, half, i] = piece

    def send_kv(t):
        if KV_ORDER[t] == FAR:
            for hop in hops:
                kv_hop(*hop).start()
        else:
            for dx in range(2):
                if (t, dx) != own_kv:
                    kv_copy(t, dx, KV_ORDER[t]).start()

    def send_q(t):
        if Q_ORDER[t] == FAR:
            for hop in hops:
                q_hop(*hop).start()
        else:
            for dx in range(2):
                if (t, dx) != own_q:
                    q_copy(t, dx, Q_ORDER[t]).start()

    def to_cross(src, i):
        return put(kvb.at[src], kvb.at[src], fx_send.at[i], kv_recv.at[src], pt.dev(pt.xcross, pt.y, pt.c))

    def to_sibling(src, i):
        return put(kvb.at[src], kvb.at[src], fs_send.at[i], kv_recv.at[src], pt.dev(pt.x, pt.y, 1 - pt.c))

    def kv_out(src):
        return pltpu.make_async_copy(kvb.at[src], kv_o.at[src], out_sem.at[src])

    def q_out(slot):
        return pltpu.make_async_copy(qb.at[slot], q_o.at[slot], qout_sem.at[slot])

    def arrived(src):
        to_sibling(src, 0).wait_recv()

    def forward(t):
        dy = KV_ORDER[t]
        for dx in range(2):
            src = pt.peer(dx, -dy)
            if dy == FAR:
                for half in range(2):
                    put(rkv.at[half, dx], kvb.at[src, half], rkv_send.at[half, dx], kvf_recv.at[dx, half], me).wait_recv()
            elif (t, dx) != own_kv:
                arrived(src)
            to_cross(src, 2 * t + dx).start()
            to_sibling(src, 2 * t + dx).start()
            kv_out(src).start()

    def forward_own():
        to_cross(me, 2 * own_kv[0]).start()
        to_sibling(me, 2 * own_kv[0]).start()
        kv_out(me).start()

    def forward_next():
        src = pt.peer(1, 0)
        arrived(src)
        to_cross(src, 2 * own_kv[0] + 1).start()
        to_sibling(src, 2 * own_kv[0] + 1).start()
        kv_out(src).start()

    kv_step(0)
    kv_step(1)
    send_kv(0)
    kv_step(2)
    send_kv(1)
    forward_own()
    kv_step(3)
    send_kv(2)
    q_step(0)
    send_kv(3)
    forward_next()
    for hop in hops:
        put(skv.at[hop[1], hop[0]], rkv.at[hop], kv_send.at[0], rkv_recv.at[hop], me).wait_recv()
        kv_hand(*hop).start()
    q_step(1)
    send_q(0)
    forward(2)
    q_step(2)
    send_q(1)
    forward(3)
    q_step(3)
    send_q(2)
    forward(0)
    send_q(3)

    def mirrored(dx, dy, c):
        x = pt.side - 1 - pt.col(dx)
        return pt.dev(x, pt.row(-dy), c)

    passing = [(t, dx, KV_ORDER[t]) for t in (1, 2, 3, 0) for dx in range(2)]

    def pass_on(steps):
        for t, dx, dy in steps:
            src = mirrored(dx, dy, pt.c)
            arrived(src)
            to_sibling(src, 8 + 2 * t + dx).start()
            kv_out(src).start()

    pass_on(passing[:4])
    for hop in hops:
        put(sq.at[hop[1], hop[0]], rq.at[hop], q_send.at[0], rq_recv.at[hop], me).wait_recv()
        q_hand(*hop).start()
    pass_on(passing[4:])

    for t, dx, dy in passing:
        src = pt.dev(pt.col(dx), pt.row(-dy), 1 - pt.c)
        arrived(src)
        kv_out(src).start()
    for t, dx, dy in q_steps:
        slot = pt.slot(dx, -dy)
        if dy == FAR:
            for half in range(2):
                put(rq.at[half, dx], qb.at[slot, half], rq_send.at[half, dx], qf_recv.at[dx, half], me).wait_recv()
        elif (t, dx) != own_q:
            put(qb.at[slot], qb.at[slot], q_send.at[0], q_recv.at[slot], me).wait_recv()
        q_out(slot).start()
    for t, dx, dy in passing:
        src = mirrored(dx, dy, 1 - pt.c)
        arrived(src)
        kv_out(src).start()

    @pl.loop(1, n)
    def _(i):
        src = lax.rem(me + i, n)
        pltpu.make_async_remote_copy(seg_ref, segb.at[pl.ds(src, 1)], seg_send.at[i], seg_recv.at[src],
                                     device_id={"cp": src}, device_id_type=MESH).wait_recv()

    segs_o[...] = segb[...]

    @pl.loop(1, n)
    def _(i):
        seg_copy(i).wait_send()

    for hop in hops:
        kv_hop(*hop).wait_send()
        kv_hand(*hop).wait_send()
        q_hop(*hop).wait_send()
        q_hand(*hop).wait_send()
    for t, dx, dy in kv_steps:
        if dy != FAR and (t, dx) != own_kv:
            kv_copy(t, dx, dy).wait_send()
        src = pt.peer(dx, -dy)
        to_cross(src, 2 * t + dx).wait_send()
        to_sibling(src, 2 * t + dx).wait_send()
        to_sibling(src, 8 + 2 * t + dx).wait_send()
    for t, dx, dy in q_steps:
        if dy != FAR and (t, dx) != own_q:
            q_copy(t, dx, dy).wait_send()

    @pl.loop(0, n)
    def _(i):
        kv_out(i).wait()

    @pl.loop(0, n // 4)
    def _(i):
        q_out(i).wait()


def _attend(n, g, scale, segs, kv, q_in, o_out, seg_s, seg_v, kvs, qs, os, lo_s, m_sc, l_sc, acc_sc, seg_sem, kv_sem, q_sem, o_sem):
    pt = Place(n)
    last_piece = 2 * n - 1
    rows = g * PC
    ng = q_in.shape[0]

    def owner(p):
        return jnp.where(p < n, p, last_piece - p)

    def half_of(p):
        return jnp.where(p < n, 0, 1)

    def load(p):
        return pltpu.make_async_copy(kv.at[owner(p), half_of(p)], kvs.at[p], kv_sem)

    seg_copies = [pltpu.make_async_copy(segs, seg_v, seg_sem.at[0]), pltpu.make_async_copy(segs, seg_s, seg_sem.at[1])]
    q_copy = pltpu.make_async_copy(q_in, qs, q_sem)
    for cp in seg_copies:
        cp.start()
    q_copy.start()

    @pl.loop(0, 2 * n)
    def _(p):
        load(p).start()

    def source(i):
        slot, half = i // 2, i % 2
        xs = (pt.x // 2) * 2 + slot % 2
        return pt.dev(xs, slot // 2, pt.c), half

    for cp in seg_copies:
        cp.wait()
    for i in range(2 * ng):
        src, half = source(i)
        before = jnp.where(seg_v[...] < seg_s[src, half, 0], 1.0, 0.0)
        lo_s[i] = jnp.sum(before).astype(jnp.int32) // PC
    q_copy.wait()

    @pl.loop(0, 2 * n)
    def _(p):
        load(p).wait()

    def lanes(col):
        return jnp.broadcast_to(col, (col.shape[0], DH))

    def out(slot, half):
        at = pl.ds(pl.multiple_of(half * PC, PC), PC)
        return pltpu.make_async_copy(os.at[slot, at], o_out.at[slot, at], o_sem)

    def one(i, carry):
        slot, half = lax.div(i, 2), lax.rem(i, 2)
        xs = (pt.x // 2) * 2 + lax.rem(slot, 2)
        src = pt.dev(xs, lax.div(slot, 2), pt.c)
        p = jnp.where(half == 0, src, last_piece - src)
        first = seg_s[src, half, 0]
        lo = lo_s[i]
        q = qs[slot, half].reshape(rows, DH)

        m_sc[...] = jnp.full_like(m_sc, NEG_INF)
        l_sc[...] = jnp.zeros_like(l_sc)
        acc_sc[...] = jnp.zeros_like(acc_sc)

        def off(b, carry):
            j0 = lo + b * KB
            js = jnp.minimum(j0, 2 * n - KB)
            kt = jnp.concatenate([kvs[js + u, 0] for u in range(KB)], axis=1)
            v = jnp.concatenate([kvs[js + u, 1] for u in range(KB)], axis=0)
            bias = []
            for u in range(KB):
                j = js + u
                want = jnp.where((j >= j0) & (j < p), first, -1)
                ids = seg_v[owner(j), pl.ds(half_of(j), 1), :]
                bias.append(jnp.where(ids == want, 0.0, NEG_INF))
            s = jnp.dot(q, kt, preferred_element_type=jnp.float32) * scale
            parts = [s[:, u * PC:(u + 1) * PC] + bias[u] for u in range(KB)]
            top = functools.reduce(jnp.maximum, parts)
            m_old = m_sc[...]
            m_new = jnp.maximum(m_old, lanes(jnp.max(top, axis=1, keepdims=True)))
            corr = jnp.exp2(m_old - m_new)
            ps = [jnp.exp2(t - m_new) for t in parts]
            l_sc[...] = l_sc[...] * corr + functools.reduce(jnp.add, ps)
            pb = jnp.concatenate([t.astype(jnp.bfloat16) for t in ps], axis=1)
            acc_sc[...] = acc_sc[...] * corr + jnp.dot(pb, v, preferred_element_type=jnp.float32)
            m_sc[...] = m_new
            return carry

        lax.fori_loop(0, lax.div(p - lo + KB - 1, KB), off, 0)

        ids = jnp.broadcast_to(seg_v[src, pl.ds(half, 1), :], (PC, PC))
        ids_t = jnp.transpose(ids)
        r = lax.broadcasted_iota(jnp.int32, (PC, PC), 0)
        cidx = lax.broadcasted_iota(jnp.int32, (PC, PC), 1)
        allowed = (ids == ids_t) & (cidx <= r)
        keep = jnp.concatenate([ids_t == first] * g, axis=0)
        allowed = jnp.concatenate([allowed] * g, axis=0)
        s = jnp.dot(q, kvs[p, 0], preferred_element_type=jnp.float32) * scale
        s = jnp.where(allowed, s, NEG_INF)
        m_old = jnp.where(keep, m_sc[...], NEG_INF)
        m_new = jnp.maximum(m_old, lanes(jnp.max(s, axis=1, keepdims=True)))
        corr = jnp.exp2(m_old - m_new)
        pr = jnp.exp2(s - m_new)
        l = jnp.where(keep, l_sc[...], 0.0) * corr + pr
        acc = jnp.where(keep, acc_sc[...], 0.0) * corr
        acc = acc + jnp.dot(pr.astype(jnp.bfloat16), kvs[p, 1], preferred_element_type=jnp.float32)
        o = (acc / lanes(jnp.sum(l, axis=1, keepdims=True))).astype(jnp.bfloat16)
        for u in range(g):
            os[slot, pl.ds(pl.multiple_of(half * PC, PC), PC), u * DH:(u + 1) * DH] = o[u * PC:(u + 1) * PC]

        @pl.when(i > 0)
        def _():
            out(lax.div(i - 1, 2), lax.rem(i - 1, 2)).start()

        return carry

    lax.fori_loop(0, 2 * ng, one, 0)
    out(ng - 1, 1).start()

    @pl.loop(0, 2 * ng)
    def _(i):
        out(lax.div(i, 2), lax.rem(i, 2)).wait()


def _combine(n, gd, o_in, wo, y_ref, obuf, robuf, wob, acc, w_sem, o_send, o_recv, of_recv, ro_recv, ro_send):
    pt = Place(n)
    me = pt.me
    my_head = pt.head(0, 0)
    d_out = y_ref.shape[1]
    nc = 4
    wn = d_out // nc

    def w_copies(t):
        for dx in range(2):
            h = pl.multiple_of(pt.head(dx, O_ORDER[t]) * gd, gd)
            yield pltpu.make_async_copy(wo.at[pl.ds(h, gd), :], wob.at[t, pl.ds(dx * gd, gd), :], w_sem.at[t, dx])

    for t in range(len(O_ORDER)):
        for cp in w_copies(t):
            cp.start()
    own = pltpu.make_async_copy(o_in.at[pt.slot(0, 0)], obuf.at[my_head], o_recv.at[my_head])
    own.start()

    steps = [(t, dx, dy) for t, dy in enumerate(O_ORDER) for dx in range(2)]
    others = [s for s in steps if (s[1], s[2]) != (0, 0)]
    barrier = pltpu.get_barrier_semaphore()
    for t, dx, dy in others:
        pl.semaphore_signal(barrier, inc=1, device_id={"cp": pt.peer(dx, dy)}, device_id_type=MESH)
    pl.semaphore_wait(barrier, len(others))

    def put(src, dst, send, recv, dev):
        return pltpu.make_async_remote_copy(src, dst, send, recv, device_id={"cp": dev}, device_id_type=MESH)

    def o_copy(t, dx, dy):
        return put(o_in.at[pt.slot(dx, dy)], obuf.at[my_head], o_send.at[2 * t + dx], o_recv.at[my_head], pt.peer(dx, dy))

    way = (1, -1)
    hops = [(half, dx) for half in range(2) for dx in range(2)]

    def rows(half):
        return pl.ds(half * PC, PC)

    def o_hop(half, dx):
        return put(o_in.at[pt.slot(dx, FAR), rows(half)], robuf.at[half, dx], o_send.at[2 * len(O_ORDER) - 2 + 2 * half + dx],
                   ro_recv.at[half, dx], pt.peer(0, way[half]))

    def o_hand(half, dx):
        return put(robuf.at[half, dx], obuf.at[pt.head(0, -way[half]), rows(half)], ro_send.at[half, dx], of_recv.at[dx, half],
                   pt.peer(dx, way[half]))

    near = [s for s in others if s[2] != FAR]
    o_copy(*near[0]).start()
    for hop in hops:
        o_hop(*hop).start()
    for s in near[1:]:
        o_copy(*s).start()

    for t, dy in enumerate(O_ORDER):
        for cp in w_copies(t):
            cp.wait()
        heads = [pt.head(dx, dy) for dx in range(2)]
        for dx in range(2):
            if dy == 0 and dx == 0:
                own.wait()
            elif dy == FAR:
                for half in range(2):
                    put(robuf.at[half, dx], obuf.at[heads[dx], rows(half)], ro_send.at[half, dx], of_recv.at[dx, half],
                        me).wait_recv()
            else:
                put(obuf.at[heads[dx]], obuf.at[heads[dx]], o_send.at[0], o_recv.at[heads[dx]], me).wait_recv()
        a = jnp.concatenate([obuf[heads[0]], obuf[heads[1]]], axis=1)
        for u in range(nc):
            r = jnp.dot(a, wob[t, :, u * wn:(u + 1) * wn], preferred_element_type=jnp.float32)
            if t > 0:
                r = r + acc[:, u * wn:(u + 1) * wn]
            if t < len(O_ORDER) - 1:
                acc[:, u * wn:(u + 1) * wn] = r
            else:
                y_ref[:, u * wn:(u + 1) * wn] = r.astype(y_ref.dtype)
        if t == 0:
            for half, dx in hops:
                put(robuf.at[half, dx], robuf.at[half, dx], o_send.at[0], ro_recv.at[half, dx], me).wait_recv()
                o_hand(half, dx).start()
    for s in near:
        o_copy(*s).wait_send()
    for hop in hops:
        o_hop(*hop).wait_send()
        o_hand(*hop).wait_send()


def solution(mesh):
    n = mesh.shape["cp"]
    side = math.isqrt(n // 2)
    bf, f32 = jnp.bfloat16, jnp.float32
    vmem, anym = pl.BlockSpec(memory_space=pltpu.VMEM), pl.BlockSpec(memory_space=pltpu.HBM)
    dma = pltpu.SemaphoreType.DMA

    def local(x, seg, wq, wk, wv, wo):
        lq, d = x.shape
        hkv = wk.shape[1] // DH
        g = wq.shape[1] // wk.shape[1]
        gd = g * DH
        ng = 2 * side
        kv, q, segs = pl.pallas_call(
            functools.partial(_project, n, g),
            out_shape=(jax.ShapeDtypeStruct((n, 2, 2, PC, DH), bf), jax.ShapeDtypeStruct((ng, 2, g, PC, DH), bf),
                       jax.ShapeDtypeStruct((n, 2, PC), jnp.int32)),
            in_specs=[vmem, vmem, anym, anym, anym],
            out_specs=(anym, anym, vmem),
            scratch_shapes=[
                pltpu.VMEM((side, d, 4 * DH), bf), pltpu.VMEM((side, d, 2 * gd), bf),
                pltpu.VMEM((n, 2, 2, PC, DH), bf), pltpu.VMEM((ng, 2, g, PC, DH), bf),
                pltpu.VMEM((ng, 2, 2, PC, DH), bf), pltpu.VMEM((ng, 2, g, PC, DH), bf),
                pltpu.VMEM((2, 2, 2, PC, DH), bf), pltpu.VMEM((2, 2, g, PC, DH), bf), pltpu.VMEM((n, 2, PC), jnp.int32),
                dma((side, 4)), dma((side, 2)), dma((ng + 2,)), dma((n,)), dma((2, 2)), dma((2, 2)), dma((2, 2)),
                dma((ng,)), dma((2 * ng,)),
                dma((ng + 2,)), dma((ng,)), dma((2, 2)), dma((2, 2)), dma((2, 2)), dma((n,)), dma((n,)), dma((n,)), dma((ng,)),
            ],
            compiler_params=pltpu.CompilerParams(collective_id=0, has_side_effects=True, vmem_limit_bytes=60 << 20),
            name="project",
        )(x, seg.reshape(1, 2, PC), wk, wv, wq)
        scale = DH ** -0.5 * math.log2(math.e)
        o = pl.pallas_call(
            functools.partial(_attend, n, g, scale),
            out_shape=jax.ShapeDtypeStruct((ng, lq, gd), bf),
            in_specs=[anym] * 3,
            out_specs=anym,
            scratch_shapes=[pltpu.SMEM((n, 2, PC), jnp.int32), pltpu.VMEM((n, 2, PC), jnp.int32),
                            pltpu.VMEM((2 * n, 2, PC, DH), bf), pltpu.VMEM((ng, 2, g, PC, DH), bf),
                            pltpu.VMEM((ng, lq, gd), bf), pltpu.SMEM((2 * ng,), jnp.int32), pltpu.VMEM((g * PC, DH), f32),
                            pltpu.VMEM((g * PC, DH), f32), pltpu.VMEM((g * PC, DH), f32), dma((2,)), dma, dma, dma],
            compiler_params=pltpu.CompilerParams(vmem_limit_bytes=60 << 20),
            name="attend",
        )(segs, kv, q)
        return pl.pallas_call(
            functools.partial(_combine, n, gd),
            out_shape=jax.ShapeDtypeStruct((lq, wo.shape[1]), bf),
            in_specs=[anym, anym],
            out_specs=vmem,
            scratch_shapes=[pltpu.VMEM((hkv, lq, gd), bf), pltpu.VMEM((2, 2, PC, gd), bf),
                            pltpu.VMEM((side, 2 * gd, wo.shape[1]), bf),
                            pltpu.VMEM((lq, wo.shape[1]), f32), dma((side, 2)), dma((ng + 2,)), dma((ng,)), dma((2, 2)), dma((2, 2)),
                            dma((2, 2))],
            compiler_params=pltpu.CompilerParams(collective_id=1, has_side_effects=True, vmem_limit_bytes=60 << 20),
            name="combine",
        )(o, wo)

    rows = P(("dp", "cp"), None)
    return jax.shard_map(local, mesh=mesh, in_specs=(rows, P(("dp", "cp")), P(), P(), P(), P()), out_specs=rows, check_vma=False)
```

```python
import functools
import math

import jax
import jax.numpy as jnp
from jax import lax
from jax.experimental import pallas as pl
from jax.experimental.pallas import tpu as pltpu
from jax.sharding import PartitionSpec as P

DH = 128
PC = 128
KB = 4
MESH = pl.DeviceIdType.MESH
NEG_INF = float("-inf")
FLOOR = -3e38


class Place:
    def __init__(self, n):
        me = lax.axis_index("cp")
        self.n, self.side = n, math.isqrt(n // 2)
        self.me = me
        self.c = lax.rem(me, 2)
        chip = me // 2
        self.x = lax.rem(chip, self.side)
        self.y = chip // self.side
        self.xin = self.x + 1 - 2 * lax.rem(self.x, 2)
        self.xcross = self.side - 1 - self.x
        self.px = lax.rem(lax.rem(self.x, 2) + self.x // 2, 2)

    def dev(self, x, y, c):
        return (y * self.side + x) * 2 + c

    def row(self, dy):
        return lax.rem(self.y + dy + self.side, self.side)

    def col(self, dx):
        return self.xin if dx else self.x

    def peer(self, dx, dy):
        return self.dev(self.col(dx), self.row(dy), self.c)

    def head(self, dx, dy):
        return lax.rem(self.px + dx, 2) * self.side + self.row(dy)

    def slot(self, dx, dy):
        return self.row(dy) * 2 + lax.rem(self.x + dx, 2)


FAR = 2
KV_ORDER = (FAR, 0, 1, -1)
Q_ORDER = (FAR, 1, -1, 0)
O_ORDER = (0, 1, -1, FAR)


def _project(n, g, x_ref, seg_ref, wk, wv, wq, kv_o, q_o, segs_o, wkvb, wqb, kvb, qb, skv, sq, rkv, rq, segb,
             wkv_sem, wq_sem, kv_send, kv_recv, kvf_recv, rkv_recv, rkv_send, fx_send, fs_send,
             q_send, q_recv, qf_recv, rq_recv, rq_send, seg_send, seg_recv, out_sem, qout_sem):
    pt = Place(n)
    me = pt.me
    kv_steps = [(t, dx, dy) for t, dy in enumerate(KV_ORDER) for dx in range(2)]
    q_steps = [(t, dx, dy) for t, dy in enumerate(Q_ORDER) for dx in range(2)]
    own_kv = (KV_ORDER.index(0), 0)
    own_q = (Q_ORDER.index(0), 0)
    gd = g * DH

    def wkv_copies(t):
        for dx in range(2):
            h = pl.multiple_of(pt.head(dx, KV_ORDER[t]) * DH, DH)
            for i, w in enumerate((wk, wv)):
                yield pltpu.make_async_copy(w.at[:, pl.ds(h, DH)], wkvb.at[t, :, pl.ds((2 * dx + i) * DH, DH)],
                                            wkv_sem.at[t, 2 * dx + i])

    def wq_copies(t):
        for dx in range(2):
            h = pl.multiple_of(pt.head(dx, Q_ORDER[t]) * gd, DH)
            yield pltpu.make_async_copy(wq.at[:, pl.ds(h, gd)], wqb.at[t, :, pl.ds(dx * gd, gd)], wq_sem.at[t, dx])

    for t in range(len(KV_ORDER)):
        for cp in wkv_copies(t):
            cp.start()
    for t in range(len(Q_ORDER)):
        for cp in wq_copies(t):
            cp.start()

    barrier = pltpu.get_barrier_semaphore()

    @pl.loop(1, n)
    def _(i):
        pl.semaphore_signal(barrier, inc=1, device_id={"cp": lax.rem(me + i, n)}, device_id_type=MESH)

    pl.semaphore_wait(barrier, n - 1)

    def seg_copy(i):
        return pltpu.make_async_remote_copy(seg_ref, segb.at[pl.ds(me, 1)], seg_send.at[i], seg_recv.at[me],
                                            device_id={"cp": lax.rem(me + i, n)}, device_id_type=MESH)

    segb[pl.ds(me, 1)] = seg_ref[...]

    def put(src, dst, send, recv, dev):
        return pltpu.make_async_remote_copy(src, dst, send, recv, device_id={"cp": dev}, device_id_type=MESH)

    def kv_copy(t, dx, dy):
        return put(skv.at[2 * t + dx], kvb.at[me], kv_send.at[2 * t + dx], kv_recv.at[me], pt.peer(dx, dy))

    def q_copy(t, dx, dy):
        return put(sq.at[2 * t + dx], qb.at[pt.slot(0, 0)], q_send.at[2 * t + dx], q_recv.at[pt.slot(0, 0)], pt.peer(dx, dy))

    way = (1, -1)
    hops = [(half, dx) for half in range(2) for dx in range(2)]

    def kv_hop(half, dx):
        return put(skv.at[dx, half], rkv.at[half, dx], kv_send.at[2 * half + dx if half == 0 else 2 * len(KV_ORDER) + dx],
                   rkv_recv.at[half, dx], pt.peer(0, way[half]))

    def kv_hand(half, dx):
        return put(rkv.at[half, dx], kvb.at[pt.peer(0, -way[half]), half], rkv_send.at[half, dx], kvf_recv.at[dx, half],
                   pt.peer(dx, way[half]))

    def q_hop(half, dx):
        return put(sq.at[dx, half], rq.at[half, dx], q_send.at[2 * half + dx if half == 0 else 2 * len(Q_ORDER) + dx],
                   rq_recv.at[half, dx], pt.peer(0, way[half]))

    def q_hand(half, dx):
        return put(rq.at[half, dx], qb.at[pt.slot(0, -way[half]), half], rq_send.at[half, dx], qf_recv.at[dx, half],
                   pt.peer(dx, way[half]))

    def kv_step(t):
        for cp in wkv_copies(t):
            cp.wait()
        r = jnp.dot(x_ref[...], wkvb[t], preferred_element_type=jnp.float32)
        for dx in range(2):
            kt = jnp.transpose(r[:, 2 * dx * DH:(2 * dx + 1) * DH]).astype(jnp.bfloat16)
            v = r[:, (2 * dx + 1) * DH:(2 * dx + 2) * DH].astype(jnp.bfloat16)
            own = (t, dx) == own_kv
            for half in range(2):
                kth = kt[:, half * PC:(half + 1) * PC]
                vh = v[half * PC:(half + 1) * PC, :]
                if own:
                    kvb[me, half, 0] = kth
                    kvb[me, half, 1] = vh
                else:
                    skv[2 * t + dx, half, 0] = kth
                    skv[2 * t + dx, half, 1] = vh

    def q_step(t):
        for cp in wq_copies(t):
            cp.wait()
        r = jnp.dot(x_ref[...], wqb[t], preferred_element_type=jnp.float32).astype(jnp.bfloat16)
        for dx in range(2):
            own = (t, dx) == own_q
            for half in range(2):
                for i in range(g):
                    piece = r[half * PC:(half + 1) * PC, dx * gd + i * DH:dx * gd + (i + 1) * DH]
                    if own:
                        qb[pt.slot(0, 0), half, i] = piece
                    else:
                        sq[2 * t + dx, half, i] = piece

    def send_kv(t):
        if KV_ORDER[t] == FAR:
            for hop in hops:
                kv_hop(*hop).start()
        else:
            for dx in range(2):
                if (t, dx) != own_kv:
                    kv_copy(t, dx, KV_ORDER[t]).start()

    def send_q(t):
        if Q_ORDER[t] == FAR:
            for hop in hops:
                q_hop(*hop).start()
        else:
            for dx in range(2):
                if (t, dx) != own_q:
                    q_copy(t, dx, Q_ORDER[t]).start()

    def to_cross(src, i):
        return put(kvb.at[src], kvb.at[src], fx_send.at[i], kv_recv.at[src], pt.dev(pt.xcross, pt.y, pt.c))

    def to_sibling(src, i):
        return put(kvb.at[src], kvb.at[src], fs_send.at[i], kv_recv.at[src], pt.dev(pt.x, pt.y, 1 - pt.c))

    def kv_out(src):
        return pltpu.make_async_copy(kvb.at[src], kv_o.at[src], out_sem.at[src])

    def q_out(slot):
        return pltpu.make_async_copy(qb.at[slot], q_o.at[slot], qout_sem.at[slot])

    def arrived(src):
        to_sibling(src, 0).wait_recv()

    def forward(t):
        dy = KV_ORDER[t]
        for dx in range(2):
            src = pt.peer(dx, -dy)
            if dy == FAR:
                for half in range(2):
                    put(rkv.at[half, dx], kvb.at[src, half], rkv_send.at[half, dx], kvf_recv.at[dx, half], me).wait_recv()
            elif (t, dx) != own_kv:
                arrived(src)
            to_cross(src, 2 * t + dx).start()
            to_sibling(src, 2 * t + dx).start()
            kv_out(src).start()

    def forward_own():
        to_cross(me, 2 * own_kv[0]).start()
        to_sibling(me, 2 * own_kv[0]).start()
        kv_out(me).start()

    def forward_next():
        src = pt.peer(1, 0)
        arrived(src)
        to_cross(src, 2 * own_kv[0] + 1).start()
        to_sibling(src, 2 * own_kv[0] + 1).start()
        kv_out(src).start()

    kv_step(0)
    kv_step(1)
    send_kv(0)
    kv_step(2)
    send_kv(1)
    forward_own()
    kv_step(3)
    send_kv(2)
    q_step(0)
    send_kv(3)
    forward_next()
    for hop in hops:
        put(skv.at[hop[1], hop[0]], rkv.at[hop], kv_send.at[0], rkv_recv.at[hop], me).wait_recv()
        kv_hand(*hop).start()
    q_step(1)
    q_step(2)
    forward(2)
    forward(3)
    q_step(3)
    forward(0)
    for t in range(len(Q_ORDER)):
        send_q(t)

    @pl.loop(1, n)
    def _(i):
        seg_copy(i).start()


    def mirrored(dx, dy, c):
        x = pt.side - 1 - pt.col(dx)
        return pt.dev(x, pt.row(-dy), c)

    passing = [(t, dx, KV_ORDER[t]) for t in (1, 2, 3, 0) for dx in range(2)]

    def pass_on(steps):
        for t, dx, dy in steps:
            src = mirrored(dx, dy, pt.c)
            arrived(src)
            to_sibling(src, 8 + 2 * t + dx).start()
            kv_out(src).start()

    pass_on(passing[:4])
    for hop in hops:
        put(sq.at[hop[1], hop[0]], rq.at[hop], q_send.at[0], rq_recv.at[hop], me).wait_recv()
        q_hand(*hop).start()
    pass_on(passing[4:])

    for t, dx, dy in passing:
        src = pt.dev(pt.col(dx), pt.row(-dy), 1 - pt.c)
        arrived(src)
        kv_out(src).start()
    for t, dx, dy in q_steps:
        slot = pt.slot(dx, -dy)
        if dy == FAR:
            for half in range(2):
                put(rq.at[half, dx], qb.at[slot, half], rq_send.at[half, dx], qf_recv.at[dx, half], me).wait_recv()
        elif (t, dx) != own_q:
            put(qb.at[slot], qb.at[slot], q_send.at[0], q_recv.at[slot], me).wait_recv()
        q_out(slot).start()
    for t, dx, dy in passing:
        src = mirrored(dx, dy, 1 - pt.c)
        arrived(src)
        kv_out(src).start()

    @pl.loop(1, n)
    def _(i):
        src = lax.rem(me + i, n)
        pltpu.make_async_remote_copy(seg_ref, segb.at[pl.ds(src, 1)], seg_send.at[i], seg_recv.at[src],
                                     device_id={"cp": src}, device_id_type=MESH).wait_recv()

    segs_o[...] = segb[...]

    @pl.loop(1, n)
    def _(i):
        seg_copy(i).wait_send()

    for hop in hops:
        kv_hop(*hop).wait_send()
        kv_hand(*hop).wait_send()
        q_hop(*hop).wait_send()
        q_hand(*hop).wait_send()
    for t, dx, dy in kv_steps:
        if dy != FAR and (t, dx) != own_kv:
            kv_copy(t, dx, dy).wait_send()
        src = pt.peer(dx, -dy)
        to_cross(src, 2 * t + dx).wait_send()
        to_sibling(src, 2 * t + dx).wait_send()
        to_sibling(src, 8 + 2 * t + dx).wait_send()
    for t, dx, dy in q_steps:
        if dy != FAR and (t, dx) != own_q:
            q_copy(t, dx, dy).wait_send()

    @pl.loop(0, n)
    def _(i):
        kv_out(i).wait()

    @pl.loop(0, n // 4)
    def _(i):
        q_out(i).wait()


def _attend(n, g, scale, segs, kv, q_in, o_out, seg_s, seg_v, kvs, qs, os, lo_s, m_sc, l_sc, acc_sc, seg_sem, kv_sem, q_sem, o_sem):
    pt = Place(n)
    last_piece = 2 * n - 1
    rows = g * PC
    ng = q_in.shape[0]

    def owner(p):
        return jnp.where(p < n, p, last_piece - p)

    def half_of(p):
        return jnp.where(p < n, 0, 1)

    def load(p):
        return pltpu.make_async_copy(kv.at[owner(p), half_of(p)], kvs.at[p], kv_sem)

    seg_copies = [pltpu.make_async_copy(segs, seg_v, seg_sem.at[0]), pltpu.make_async_copy(segs, seg_s, seg_sem.at[1])]
    q_copy = pltpu.make_async_copy(q_in, qs, q_sem)
    for cp in seg_copies:
        cp.start()
    q_copy.start()

    @pl.loop(0, 2 * n)
    def _(p):
        load(p).start()

    def source(i):
        slot, half = i // 2, i % 2
        xs = (pt.x // 2) * 2 + slot % 2
        return pt.dev(xs, slot // 2, pt.c), half

    for cp in seg_copies:
        cp.wait()
    for i in range(2 * ng):
        src, half = source(i)
        before = jnp.where(seg_v[...] < seg_s[src, half, 0], 1.0, 0.0)
        lo_s[i] = jnp.sum(before).astype(jnp.int32) // PC
    q_copy.wait()

    @pl.loop(0, 2 * n)
    def _(p):
        load(p).wait()

    def lanes(col):
        return jnp.broadcast_to(col, (col.shape[0], DH))

    def out(slot, half):
        at = pl.ds(pl.multiple_of(half * PC, PC), PC)
        return pltpu.make_async_copy(os.at[slot, at], o_out.at[slot, at], o_sem)

    def pair(i, carry):
        row, half = lax.div(i, 2), lax.rem(i, 2)
        slots = [2 * row + u for u in range(2)]
        srcs = [pt.dev((pt.x // 2) * 2 + u, row, pt.c) for u in range(2)]
        ps = [jnp.where(half == 0, src, last_piece - src) for src in srcs]
        firsts = [seg_s[src, half, 0] for src in srcs]
        lo = jnp.minimum(lo_s[2 * slots[0] + half], lo_s[2 * slots[1] + half])
        end = jnp.maximum(ps[0], ps[1])
        m_sc[...] = jnp.full_like(m_sc, FLOOR)
        l_sc[...] = jnp.zeros_like(l_sc)
        acc_sc[...] = jnp.zeros_like(acc_sc)

        def query(u):
            return qs[slots[u], half].reshape(rows, DH)

        def off(b, carry):
            j0 = lo + b * KB
            js = jnp.minimum(j0, 2 * n - KB)
            kt = jnp.concatenate([kvs[js + w, 0] for w in range(KB)], axis=1)
            v = jnp.concatenate([kvs[js + w, 1] for w in range(KB)], axis=0)
            ids = [seg_v[owner(js + w), pl.ds(half_of(js + w), 1), :] for w in range(KB)]
            ss = [jnp.dot(query(u), kt, preferred_element_type=jnp.float32) for u in range(2)]
            for u in range(2):
                parts = []
                for w in range(KB):
                    j = js + w
                    want = jnp.where((j >= j0) & (j < ps[u]), firsts[u], -1)
                    parts.append(ss[u][:, w * PC:(w + 1) * PC] * scale + jnp.where(ids[w] == want, 0.0, NEG_INF))
                m_old = m_sc[u]
                m_new = jnp.maximum(m_old, lanes(jnp.max(functools.reduce(jnp.maximum, parts), axis=1, keepdims=True)))
                corr = jnp.exp2(m_old - m_new)
                pr = [jnp.exp2(t - m_new) for t in parts]
                l_sc[u] = l_sc[u] * corr + functools.reduce(jnp.add, pr)
                pb = jnp.concatenate([t.astype(jnp.bfloat16) for t in pr], axis=1)
                acc_sc[u] = acc_sc[u] * corr + jnp.dot(pb, v, preferred_element_type=jnp.float32)
                m_sc[u] = m_new
            return carry

        lax.fori_loop(0, lax.div(end - lo + KB - 1, KB), off, 0)

        r = lax.broadcasted_iota(jnp.int32, (PC, PC), 0)
        cidx = lax.broadcasted_iota(jnp.int32, (PC, PC), 1)
        ss = [jnp.dot(query(u), kvs[ps[u], 0], preferred_element_type=jnp.float32) * scale for u in range(2)]
        for u in range(2):
            ids = jnp.broadcast_to(seg_v[srcs[u], pl.ds(half, 1), :], (PC, PC))
            ids_t = jnp.transpose(ids)
            allowed = jnp.concatenate([(ids == ids_t) & (cidx <= r)] * g, axis=0)
            keep = jnp.concatenate([ids_t == firsts[u]] * g, axis=0)
            s = jnp.where(allowed, ss[u], NEG_INF)
            m_old = jnp.where(keep, m_sc[u], FLOOR)
            m_new = jnp.maximum(m_old, lanes(jnp.max(s, axis=1, keepdims=True)))
            corr = jnp.exp2(m_old - m_new)
            pr = jnp.exp2(s - m_new)
            l = jnp.where(keep, l_sc[u], 0.0) * corr + pr
            acc = jnp.where(keep, acc_sc[u], 0.0) * corr
            acc = acc + jnp.dot(pr.astype(jnp.bfloat16), kvs[ps[u], 1], preferred_element_type=jnp.float32)
            o = (acc / lanes(jnp.sum(l, axis=1, keepdims=True))).astype(jnp.bfloat16)
            for w in range(g):
                os[slots[u], pl.ds(pl.multiple_of(half * PC, PC), PC), w * DH:(w + 1) * DH] = o[w * PC:(w + 1) * PC]

        @pl.when(i > 0)
        def _():
            for u in range(2):
                out(2 * lax.div(i - 1, 2) + u, lax.rem(i - 1, 2)).start()

        return carry

    lax.fori_loop(0, ng, pair, 0)
    for u in range(2):
        out(ng - 2 + u, 1).start()

    @pl.loop(0, 2 * ng)
    def _(i):
        out(lax.div(i, 2), lax.rem(i, 2)).wait()


def _combine(n, gd, o_in, wo, y_ref, obuf, robuf, wob, acc, w_sem, o_send, o_recv, of_recv, ro_recv, ro_send):
    pt = Place(n)
    me = pt.me
    my_head = pt.head(0, 0)
    d_out = y_ref.shape[1]
    nc = 4
    wn = d_out // nc

    def w_copies(t):
        for dx in range(2):
            h = pl.multiple_of(pt.head(dx, O_ORDER[t]) * gd, gd)
            yield pltpu.make_async_copy(wo.at[pl.ds(h, gd), :], wob.at[t, pl.ds(dx * gd, gd), :], w_sem.at[t, dx])

    for t in range(len(O_ORDER)):
        for cp in w_copies(t):
            cp.start()
    own = pltpu.make_async_copy(o_in.at[pt.slot(0, 0)], obuf.at[my_head], o_recv.at[my_head])
    own.start()

    steps = [(t, dx, dy) for t, dy in enumerate(O_ORDER) for dx in range(2)]
    others = [s for s in steps if (s[1], s[2]) != (0, 0)]
    barrier = pltpu.get_barrier_semaphore()
    for t, dx, dy in others:
        pl.semaphore_signal(barrier, inc=1, device_id={"cp": pt.peer(dx, dy)}, device_id_type=MESH)
    pl.semaphore_wait(barrier, len(others))

    def put(src, dst, send, recv, dev):
        return pltpu.make_async_remote_copy(src, dst, send, recv, device_id={"cp": dev}, device_id_type=MESH)

    def o_copy(t, dx, dy):
        return put(o_in.at[pt.slot(dx, dy)], obuf.at[my_head], o_send.at[2 * t + dx], o_recv.at[my_head], pt.peer(dx, dy))

    way = (1, -1)
    hops = [(half, dx) for half in range(2) for dx in range(2)]

    def rows(half):
        return pl.ds(half * PC, PC)

    def o_hop(half, dx):
        return put(o_in.at[pt.slot(dx, FAR), rows(half)], robuf.at[half, dx], o_send.at[2 * len(O_ORDER) - 2 + 2 * half + dx],
                   ro_recv.at[half, dx], pt.peer(0, way[half]))

    def o_hand(half, dx):
        return put(robuf.at[half, dx], obuf.at[pt.head(0, -way[half]), rows(half)], ro_send.at[half, dx], of_recv.at[dx, half],
                   pt.peer(dx, way[half]))

    near = [s for s in others if s[2] != FAR]
    o_copy(*near[0]).start()
    for hop in hops:
        o_hop(*hop).start()
    for s in near[1:]:
        o_copy(*s).start()

    for t, dy in enumerate(O_ORDER):
        for cp in w_copies(t):
            cp.wait()
        heads = [pt.head(dx, dy) for dx in range(2)]
        for dx in range(2):
            if dy == 0 and dx == 0:
                own.wait()
            elif dy == FAR:
                for half in range(2):
                    put(robuf.at[half, dx], obuf.at[heads[dx], rows(half)], ro_send.at[half, dx], of_recv.at[dx, half],
                        me).wait_recv()
            else:
                put(obuf.at[heads[dx]], obuf.at[heads[dx]], o_send.at[0], o_recv.at[heads[dx]], me).wait_recv()
        a = jnp.concatenate([obuf[heads[0]], obuf[heads[1]]], axis=1)
        for u in range(nc):
            r = jnp.dot(a, wob[t, :, u * wn:(u + 1) * wn], preferred_element_type=jnp.float32)
            if t > 0:
                r = r + acc[:, u * wn:(u + 1) * wn]
            if t < len(O_ORDER) - 1:
                acc[:, u * wn:(u + 1) * wn] = r
            else:
                y_ref[:, u * wn:(u + 1) * wn] = r.astype(y_ref.dtype)
        if t == 0:
            for half, dx in hops:
                put(robuf.at[half, dx], robuf.at[half, dx], o_send.at[0], ro_recv.at[half, dx], me).wait_recv()
                o_hand(half, dx).start()
    for s in near:
        o_copy(*s).wait_send()
    for hop in hops:
        o_hop(*hop).wait_send()
        o_hand(*hop).wait_send()


def solution(mesh):
    n = mesh.shape["cp"]
    side = math.isqrt(n // 2)
    bf, f32 = jnp.bfloat16, jnp.float32
    vmem, anym = pl.BlockSpec(memory_space=pltpu.VMEM), pl.BlockSpec(memory_space=pltpu.HBM)
    dma = pltpu.SemaphoreType.DMA

    def local(x, seg, wq, wk, wv, wo):
        lq, d = x.shape
        hkv = wk.shape[1] // DH
        g = wq.shape[1] // wk.shape[1]
        gd = g * DH
        ng = 2 * side
        kv, q, segs = pl.pallas_call(
            functools.partial(_project, n, g),
            out_shape=(jax.ShapeDtypeStruct((n, 2, 2, PC, DH), bf), jax.ShapeDtypeStruct((ng, 2, g, PC, DH), bf),
                       jax.ShapeDtypeStruct((n, 2, PC), jnp.int32)),
            in_specs=[vmem, vmem, anym, anym, anym],
            out_specs=(anym, anym, vmem),
            scratch_shapes=[
                pltpu.VMEM((side, d, 4 * DH), bf), pltpu.VMEM((side, d, 2 * gd), bf),
                pltpu.VMEM((n, 2, 2, PC, DH), bf), pltpu.VMEM((ng, 2, g, PC, DH), bf),
                pltpu.VMEM((ng, 2, 2, PC, DH), bf), pltpu.VMEM((ng, 2, g, PC, DH), bf),
                pltpu.VMEM((2, 2, 2, PC, DH), bf), pltpu.VMEM((2, 2, g, PC, DH), bf), pltpu.VMEM((n, 2, PC), jnp.int32),
                dma((side, 4)), dma((side, 2)), dma((ng + 2,)), dma((n,)), dma((2, 2)), dma((2, 2)), dma((2, 2)),
                dma((ng,)), dma((2 * ng,)),
                dma((ng + 2,)), dma((ng,)), dma((2, 2)), dma((2, 2)), dma((2, 2)), dma((n,)), dma((n,)), dma((n,)), dma((ng,)),
            ],
            compiler_params=pltpu.CompilerParams(collective_id=0, has_side_effects=True, vmem_limit_bytes=60 << 20),
            name="project",
        )(x, seg.reshape(1, 2, PC), wk, wv, wq)
        scale = DH ** -0.5 * math.log2(math.e)
        o = pl.pallas_call(
            functools.partial(_attend, n, g, scale),
            out_shape=jax.ShapeDtypeStruct((ng, lq, gd), bf),
            in_specs=[anym] * 3,
            out_specs=anym,
            scratch_shapes=[pltpu.SMEM((n, 2, PC), jnp.int32), pltpu.VMEM((n, 2, PC), jnp.int32),
                            pltpu.VMEM((2 * n, 2, PC, DH), bf), pltpu.VMEM((ng, 2, g, PC, DH), bf),
                            pltpu.VMEM((ng, lq, gd), bf), pltpu.SMEM((2 * ng,), jnp.int32), pltpu.VMEM((2, g * PC, DH), f32),
                            pltpu.VMEM((2, g * PC, DH), f32), pltpu.VMEM((2, g * PC, DH), f32), dma((2,)), dma, dma, dma],
            compiler_params=pltpu.CompilerParams(vmem_limit_bytes=60 << 20),
            name="attend",
        )(segs, kv, q)
        return pl.pallas_call(
            functools.partial(_combine, n, gd),
            out_shape=jax.ShapeDtypeStruct((lq, wo.shape[1]), bf),
            in_specs=[anym, anym],
            out_specs=vmem,
            scratch_shapes=[pltpu.VMEM((hkv, lq, gd), bf), pltpu.VMEM((2, 2, PC, gd), bf),
                            pltpu.VMEM((side, 2 * gd, wo.shape[1]), bf),
                            pltpu.VMEM((lq, wo.shape[1]), f32), dma((side, 2)), dma((ng + 2,)), dma((ng,)), dma((2, 2)), dma((2, 2)),
                            dma((2, 2))],
            compiler_params=pltpu.CompilerParams(collective_id=1, has_side_effects=True, vmem_limit_bytes=60 << 20),
            name="combine",
        )(o, wo)

    rows = P(("dp", "cp"), None)
    return jax.shard_map(local, mesh=mesh, in_specs=(rows, P(("dp", "cp")), P(), P(), P(), P()), out_specs=rows, check_vma=False)
```

```python
import functools
import math

import jax
import jax.numpy as jnp
from jax import lax
from jax.experimental import pallas as pl
from jax.experimental.pallas import tpu as pltpu
from jax.sharding import PartitionSpec as P

DH = 128
PC = 128
KB = 4
MESH = pl.DeviceIdType.MESH
NEG_INF = float("-inf")
FLOOR = -3e38


class Place:
    def __init__(self, n):
        me = lax.axis_index("cp")
        self.n, self.side = n, math.isqrt(n // 2)
        self.me = me
        self.c = lax.rem(me, 2)
        chip = me // 2
        self.x = lax.rem(chip, self.side)
        self.y = chip // self.side
        self.xin = self.x + 1 - 2 * lax.rem(self.x, 2)
        self.xcross = self.side - 1 - self.x
        self.px = lax.rem(lax.rem(self.x, 2) + self.x // 2, 2)

    def dev(self, x, y, c):
        return (y * self.side + x) * 2 + c

    def row(self, dy):
        return lax.rem(self.y + dy + self.side, self.side)

    def col(self, dx):
        return self.xin if dx else self.x

    def peer(self, dx, dy):
        return self.dev(self.col(dx), self.row(dy), self.c)

    def head(self, dx, dy):
        return lax.rem(self.px + dx, 2) * self.side + self.row(dy)

    def slot(self, dx, dy):
        return self.row(dy) * 2 + lax.rem(self.x + dx, 2)


FAR = 2
KV_ORDER = (FAR, 0, 1, -1)
Q_ORDER = (FAR, 1, -1, 0)
O_ORDER = (0, 1, -1, FAR)


def _project(n, g, x_ref, wk, wv, wq, kv_o, q_o, wkvb, wqb, skv, sq, wkv_sem, wq_sem, out_sem):
    pt = Place(n)
    gd = g * DH

    def wkv_copies(t):
        for dx in range(2):
            h = pl.multiple_of(pt.head(dx, KV_ORDER[t]) * DH, DH)
            for i, w in enumerate((wk, wv)):
                yield pltpu.make_async_copy(w.at[:, pl.ds(h, DH)], wkvb.at[t, :, pl.ds((2 * dx + i) * DH, DH)],
                                            wkv_sem.at[t, 2 * dx + i])

    def wq_copies(t):
        for dx in range(2):
            h = pl.multiple_of(pt.head(dx, Q_ORDER[t]) * gd, DH)
            yield pltpu.make_async_copy(wq.at[:, pl.ds(h, gd)], wqb.at[t, :, pl.ds(dx * gd, gd)], wq_sem.at[t, dx])

    for t in range(len(KV_ORDER)):
        for cp in wkv_copies(t):
            cp.start()
    for t in range(len(Q_ORDER)):
        for cp in wq_copies(t):
            cp.start()

    def kv_step(t):
        for cp in wkv_copies(t):
            cp.wait()
        r = jnp.dot(x_ref[...], wkvb[t], preferred_element_type=jnp.float32)
        for dx in range(2):
            kt = jnp.transpose(r[:, 2 * dx * DH:(2 * dx + 1) * DH]).astype(jnp.bfloat16)
            v = r[:, (2 * dx + 1) * DH:(2 * dx + 2) * DH].astype(jnp.bfloat16)
            for half in range(2):
                skv[2 * t + dx, half, 0] = kt[:, half * PC:(half + 1) * PC]
                skv[2 * t + dx, half, 1] = v[half * PC:(half + 1) * PC, :]

    def q_step(t):
        for cp in wq_copies(t):
            cp.wait()
        r = jnp.dot(x_ref[...], wqb[t], preferred_element_type=jnp.float32).astype(jnp.bfloat16)
        for dx in range(2):
            for half in range(2):
                for i in range(g):
                    sq[2 * t + dx, half, i] = r[half * PC:(half + 1) * PC, dx * gd + i * DH:dx * gd + (i + 1) * DH]

    nkv, nq = len(KV_ORDER), len(Q_ORDER)
    outs = [pltpu.make_async_copy(skv.at[pl.ds(2 * t, 2)], kv_o.at[pl.ds(2 * t, 2)], out_sem.at[t]) for t in range(nkv)]
    outs += [pltpu.make_async_copy(sq.at[pl.ds(2 * t, 2)], q_o.at[pl.ds(2 * t, 2)], out_sem.at[nkv + t]) for t in range(nq)]
    for i in range(nkv + nq):
        if i < nkv:
            kv_step(i)
        else:
            q_step(i - nkv)
        if i > 0:
            outs[i - 1].start()
    outs[-1].start()
    for cp in outs:
        cp.wait()


def _exchange(n, seg_ref, skv, sq, kv_o, q_o, segs_o, kvb, qb, rkv, rq, segb,
              own_sem, kv_send, kv_recv, kvf_recv, rkv_recv, rkv_send, fx_send, fs_send,
              q_send, q_recv, qf_recv, rq_recv, rq_send, seg_send, seg_recv, out_sem, qout_sem):
    pt = Place(n)
    me = pt.me
    kv_steps = [(t, dx, dy) for t, dy in enumerate(KV_ORDER) for dx in range(2)]
    q_steps = [(t, dx, dy) for t, dy in enumerate(Q_ORDER) for dx in range(2)]
    own_kv = (KV_ORDER.index(0), 0)
    own_q = (Q_ORDER.index(0), 0)

    own_copies = [pltpu.make_async_copy(skv.at[2 * own_kv[0]], kvb.at[me], own_sem.at[0]),
                  pltpu.make_async_copy(sq.at[2 * own_q[0]], qb.at[pt.slot(0, 0)], own_sem.at[1])]
    for cp in own_copies:
        cp.start()
    barrier = pltpu.get_barrier_semaphore()

    @pl.loop(1, n)
    def _(i):
        pl.semaphore_signal(barrier, inc=1, device_id={"cp": lax.rem(me + i, n)}, device_id_type=MESH)

    pl.semaphore_wait(barrier, n - 1)

    def seg_copy(i):
        return pltpu.make_async_remote_copy(seg_ref, segb.at[pl.ds(me, 1)], seg_send.at[i], seg_recv.at[me],
                                            device_id={"cp": lax.rem(me + i, n)}, device_id_type=MESH)

    segb[pl.ds(me, 1)] = seg_ref[...]

    def put(src, dst, send, recv, dev):
        return pltpu.make_async_remote_copy(src, dst, send, recv, device_id={"cp": dev}, device_id_type=MESH)

    def kv_copy(t, dx, dy):
        return put(skv.at[2 * t + dx], kvb.at[me], kv_send.at[2 * t + dx], kv_recv.at[me], pt.peer(dx, dy))

    def q_copy(t, dx, dy):
        return put(sq.at[2 * t + dx], qb.at[pt.slot(0, 0)], q_send.at[2 * t + dx], q_recv.at[pt.slot(0, 0)], pt.peer(dx, dy))

    way = (1, -1)
    hops = [(half, dx) for half in range(2) for dx in range(2)]

    def kv_hop(half, dx):
        return put(skv.at[dx, half], rkv.at[half, dx], kv_send.at[2 * half + dx if half == 0 else 2 * len(KV_ORDER) + dx],
                   rkv_recv.at[half, dx], pt.peer(0, way[half]))

    def kv_hand(half, dx):
        return put(rkv.at[half, dx], kvb.at[pt.peer(0, -way[half]), half], rkv_send.at[half, dx], kvf_recv.at[dx, half],
                   pt.peer(dx, way[half]))

    def q_hop(half, dx):
        return put(sq.at[dx, half], rq.at[half, dx], q_send.at[2 * half + dx if half == 0 else 2 * len(Q_ORDER) + dx],
                   rq_recv.at[half, dx], pt.peer(0, way[half]))

    def q_hand(half, dx):
        return put(rq.at[half, dx], qb.at[pt.slot(0, -way[half]), half], rq_send.at[half, dx], qf_recv.at[dx, half],
                   pt.peer(dx, way[half]))

    def send_kv(t):
        if KV_ORDER[t] == FAR:
            for hop in hops:
                kv_hop(*hop).start()
        else:
            for dx in range(2):
                if (t, dx) != own_kv:
                    kv_copy(t, dx, KV_ORDER[t]).start()

    def send_q(t):
        if Q_ORDER[t] == FAR:
            for hop in hops:
                q_hop(*hop).start()
        else:
            for dx in range(2):
                if (t, dx) != own_q:
                    q_copy(t, dx, Q_ORDER[t]).start()

    def to_cross(src, i):
        return put(kvb.at[src], kvb.at[src], fx_send.at[i], kv_recv.at[src], pt.dev(pt.xcross, pt.y, pt.c))

    def to_sibling(src, i):
        return put(kvb.at[src], kvb.at[src], fs_send.at[i], kv_recv.at[src], pt.dev(pt.x, pt.y, 1 - pt.c))

    def kv_out(src):
        return pltpu.make_async_copy(kvb.at[src], kv_o.at[src], out_sem.at[src])

    def q_out(slot):
        return pltpu.make_async_copy(qb.at[slot], q_o.at[slot], qout_sem.at[slot])

    def arrived(src):
        to_sibling(src, 0).wait_recv()

    def forward(t):
        dy = KV_ORDER[t]
        for dx in range(2):
            src = pt.peer(dx, -dy)
            if dy == FAR:
                for half in range(2):
                    put(rkv.at[half, dx], kvb.at[src, half], rkv_send.at[half, dx], kvf_recv.at[dx, half], me).wait_recv()
            elif (t, dx) != own_kv:
                arrived(src)
            to_cross(src, 2 * t + dx).start()
            to_sibling(src, 2 * t + dx).start()
            kv_out(src).start()

    def forward_own():
        to_cross(me, 2 * own_kv[0]).start()
        to_sibling(me, 2 * own_kv[0]).start()
        kv_out(me).start()

    def forward_next():
        src = pt.peer(1, 0)
        arrived(src)
        to_cross(src, 2 * own_kv[0] + 1).start()
        to_sibling(src, 2 * own_kv[0] + 1).start()
        kv_out(src).start()

    for t in range(len(KV_ORDER)):
        send_kv(t)
    own_copies[0].wait()
    forward_own()
    forward_next()
    for hop in hops:
        put(skv.at[hop[1], hop[0]], rkv.at[hop], kv_send.at[0], rkv_recv.at[hop], me).wait_recv()
        kv_hand(*hop).start()
    forward(2)
    forward(3)
    forward(0)
    for t in range(len(Q_ORDER)):
        send_q(t)

    @pl.loop(1, n)
    def _(i):
        seg_copy(i).start()

    own_copies[1].wait()

    def mirrored(dx, dy, c):
        x = pt.side - 1 - pt.col(dx)
        return pt.dev(x, pt.row(-dy), c)

    passing = [(t, dx, KV_ORDER[t]) for t in (1, 2, 3, 0) for dx in range(2)]

    def pass_on(steps):
        for t, dx, dy in steps:
            src = mirrored(dx, dy, pt.c)
            arrived(src)
            to_sibling(src, 8 + 2 * t + dx).start()
            kv_out(src).start()

    pass_on(passing[:4])
    for hop in hops:
        put(sq.at[hop[1], hop[0]], rq.at[hop], q_send.at[0], rq_recv.at[hop], me).wait_recv()
        q_hand(*hop).start()
    pass_on(passing[4:])

    for t, dx, dy in passing:
        src = pt.dev(pt.col(dx), pt.row(-dy), 1 - pt.c)
        arrived(src)
        kv_out(src).start()
    for t, dx, dy in q_steps:
        slot = pt.slot(dx, -dy)
        if dy == FAR:
            for half in range(2):
                put(rq.at[half, dx], qb.at[slot, half], rq_send.at[half, dx], qf_recv.at[dx, half], me).wait_recv()
        elif (t, dx) != own_q:
            put(qb.at[slot], qb.at[slot], q_send.at[0], q_recv.at[slot], me).wait_recv()
        q_out(slot).start()
    for t, dx, dy in passing:
        src = mirrored(dx, dy, 1 - pt.c)
        arrived(src)
        kv_out(src).start()

    @pl.loop(1, n)
    def _(i):
        src = lax.rem(me + i, n)
        pltpu.make_async_remote_copy(seg_ref, segb.at[pl.ds(src, 1)], seg_send.at[i], seg_recv.at[src],
                                     device_id={"cp": src}, device_id_type=MESH).wait_recv()

    segs_o[...] = segb[...]

    @pl.loop(1, n)
    def _(i):
        seg_copy(i).wait_send()

    for hop in hops:
        kv_hop(*hop).wait_send()
        kv_hand(*hop).wait_send()
        q_hop(*hop).wait_send()
        q_hand(*hop).wait_send()
    for t, dx, dy in kv_steps:
        if dy != FAR and (t, dx) != own_kv:
            kv_copy(t, dx, dy).wait_send()
        src = pt.peer(dx, -dy)
        to_cross(src, 2 * t + dx).wait_send()
        to_sibling(src, 2 * t + dx).wait_send()
        to_sibling(src, 8 + 2 * t + dx).wait_send()
    for t, dx, dy in q_steps:
        if dy != FAR and (t, dx) != own_q:
            q_copy(t, dx, dy).wait_send()

    @pl.loop(0, n)
    def _(i):
        kv_out(i).wait()

    @pl.loop(0, n // 4)
    def _(i):
        q_out(i).wait()


def _attend(n, g, scale, segs, kv, q_in, o_out, seg_s, seg_v, kvs, qs, os, lo_s, m_sc, l_sc, acc_sc, seg_sem, kv_sem, q_sem, o_sem):
    pt = Place(n)
    last_piece = 2 * n - 1
    rows = g * PC
    ng = q_in.shape[0]

    def owner(p):
        return jnp.where(p < n, p, last_piece - p)

    def half_of(p):
        return jnp.where(p < n, 0, 1)

    def load(p):
        return pltpu.make_async_copy(kv.at[owner(p), half_of(p)], kvs.at[p], kv_sem)

    seg_copies = [pltpu.make_async_copy(segs, seg_v, seg_sem.at[0]), pltpu.make_async_copy(segs, seg_s, seg_sem.at[1])]
    q_copy = pltpu.make_async_copy(q_in, qs, q_sem)
    for cp in seg_copies:
        cp.start()
    q_copy.start()

    @pl.loop(0, 2 * n)
    def _(p):
        load(p).start()

    def source(i):
        slot, half = i // 2, i % 2
        xs = (pt.x // 2) * 2 + slot % 2
        return pt.dev(xs, slot // 2, pt.c), half

    for cp in seg_copies:
        cp.wait()
    for i in range(2 * ng):
        src, half = source(i)
        before = jnp.where(seg_v[...] < seg_s[src, half, 0], 1.0, 0.0)
        lo_s[i] = jnp.sum(before).astype(jnp.int32) // PC
    q_copy.wait()

    @pl.loop(0, 2 * n)
    def _(p):
        load(p).wait()

    def lanes(col):
        return jnp.broadcast_to(col, (col.shape[0], DH))

    def out(slot, half):
        at = pl.ds(pl.multiple_of(half * PC, PC), PC)
        return pltpu.make_async_copy(os.at[slot, at], o_out.at[slot, at], o_sem)

    def pair(i, carry):
        row, half = lax.div(i, 2), lax.rem(i, 2)
        slots = [2 * row + u for u in range(2)]
        srcs = [pt.dev((pt.x // 2) * 2 + u, row, pt.c) for u in range(2)]
        ps = [jnp.where(half == 0, src, last_piece - src) for src in srcs]
        firsts = [seg_s[src, half, 0] for src in srcs]
        lo = jnp.minimum(lo_s[2 * slots[0] + half], lo_s[2 * slots[1] + half])
        end = jnp.maximum(ps[0], ps[1])
        m_sc[...] = jnp.full_like(m_sc, FLOOR)
        l_sc[...] = jnp.zeros_like(l_sc)
        acc_sc[...] = jnp.zeros_like(acc_sc)

        def query(u):
            return qs[slots[u], half].reshape(rows, DH)

        def off(b, carry):
            j0 = lo + b * KB
            js = jnp.minimum(j0, 2 * n - KB)
            kt = jnp.concatenate([kvs[js + w, 0] for w in range(KB)], axis=1)
            v = jnp.concatenate([kvs[js + w, 1] for w in range(KB)], axis=0)
            ids = [seg_v[owner(js + w), pl.ds(half_of(js + w), 1), :] for w in range(KB)]
            ss = [jnp.dot(query(u), kt, preferred_element_type=jnp.float32) for u in range(2)]
            for u in range(2):
                parts = []
                for w in range(KB):
                    j = js + w
                    want = jnp.where((j >= j0) & (j < ps[u]), firsts[u], -1)
                    parts.append(ss[u][:, w * PC:(w + 1) * PC] * scale + jnp.where(ids[w] == want, 0.0, NEG_INF))
                m_old = m_sc[u]
                m_new = jnp.maximum(m_old, lanes(jnp.max(functools.reduce(jnp.maximum, parts), axis=1, keepdims=True)))
                corr = jnp.exp2(m_old - m_new)
                pr = [jnp.exp2(t - m_new) for t in parts]
                l_sc[u] = l_sc[u] * corr + functools.reduce(jnp.add, pr)
                pb = jnp.concatenate([t.astype(jnp.bfloat16) for t in pr], axis=1)
                acc_sc[u] = acc_sc[u] * corr + jnp.dot(pb, v, preferred_element_type=jnp.float32)
                m_sc[u] = m_new
            return carry

        lax.fori_loop(0, lax.div(end - lo + KB - 1, KB), off, 0)

        r = lax.broadcasted_iota(jnp.int32, (PC, PC), 0)
        cidx = lax.broadcasted_iota(jnp.int32, (PC, PC), 1)
        ss = [jnp.dot(query(u), kvs[ps[u], 0], preferred_element_type=jnp.float32) * scale for u in range(2)]
        for u in range(2):
            ids = jnp.broadcast_to(seg_v[srcs[u], pl.ds(half, 1), :], (PC, PC))
            ids_t = jnp.transpose(ids)
            allowed = jnp.concatenate([(ids == ids_t) & (cidx <= r)] * g, axis=0)
            keep = jnp.concatenate([ids_t == firsts[u]] * g, axis=0)
            s = jnp.where(allowed, ss[u], NEG_INF)
            m_old = jnp.where(keep, m_sc[u], FLOOR)
            m_new = jnp.maximum(m_old, lanes(jnp.max(s, axis=1, keepdims=True)))
            corr = jnp.exp2(m_old - m_new)
            pr = jnp.exp2(s - m_new)
            l = jnp.where(keep, l_sc[u], 0.0) * corr + pr
            acc = jnp.where(keep, acc_sc[u], 0.0) * corr
            acc = acc + jnp.dot(pr.astype(jnp.bfloat16), kvs[ps[u], 1], preferred_element_type=jnp.float32)
            o = (acc / lanes(jnp.sum(l, axis=1, keepdims=True))).astype(jnp.bfloat16)
            for w in range(g):
                os[slots[u], pl.ds(pl.multiple_of(half * PC, PC), PC), w * DH:(w + 1) * DH] = o[w * PC:(w + 1) * PC]

        @pl.when(i > 0)
        def _():
            for u in range(2):
                out(2 * lax.div(i - 1, 2) + u, lax.rem(i - 1, 2)).start()

        return carry

    lax.fori_loop(0, ng, pair, 0)
    for u in range(2):
        out(ng - 2 + u, 1).start()

    @pl.loop(0, 2 * ng)
    def _(i):
        out(lax.div(i, 2), lax.rem(i, 2)).wait()


def _combine(n, gd, o_in, wo, y_ref, obuf, robuf, wob, acc, w_sem, o_send, o_recv, of_recv, ro_recv, ro_send):
    pt = Place(n)
    me = pt.me
    my_head = pt.head(0, 0)
    d_out = y_ref.shape[1]
    nc = 4
    wn = d_out // nc

    def w_copies(t):
        for dx in range(2):
            h = pl.multiple_of(pt.head(dx, O_ORDER[t]) * gd, gd)
            yield pltpu.make_async_copy(wo.at[pl.ds(h, gd), :], wob.at[t, pl.ds(dx * gd, gd), :], w_sem.at[t, dx])

    for t in range(len(O_ORDER)):
        for cp in w_copies(t):
            cp.start()
    own = pltpu.make_async_copy(o_in.at[pt.slot(0, 0)], obuf.at[my_head], o_recv.at[my_head])
    own.start()

    steps = [(t, dx, dy) for t, dy in enumerate(O_ORDER) for dx in range(2)]
    others = [s for s in steps if (s[1], s[2]) != (0, 0)]
    barrier = pltpu.get_barrier_semaphore()
    for t, dx, dy in others:
        pl.semaphore_signal(barrier, inc=1, device_id={"cp": pt.peer(dx, dy)}, device_id_type=MESH)
    pl.semaphore_wait(barrier, len(others))

    def put(src, dst, send, recv, dev):
        return pltpu.make_async_remote_copy(src, dst, send, recv, device_id={"cp": dev}, device_id_type=MESH)

    def o_copy(t, dx, dy):
        return put(o_in.at[pt.slot(dx, dy)], obuf.at[my_head], o_send.at[2 * t + dx], o_recv.at[my_head], pt.peer(dx, dy))

    way = (1, -1)
    hops = [(half, dx) for half in range(2) for dx in range(2)]

    def rows(half):
        return pl.ds(half * PC, PC)

    def o_hop(half, dx):
        return put(o_in.at[pt.slot(dx, FAR), rows(half)], robuf.at[half, dx], o_send.at[2 * len(O_ORDER) - 2 + 2 * half + dx],
                   ro_recv.at[half, dx], pt.peer(0, way[half]))

    def o_hand(half, dx):
        return put(robuf.at[half, dx], obuf.at[pt.head(0, -way[half]), rows(half)], ro_send.at[half, dx], of_recv.at[dx, half],
                   pt.peer(dx, way[half]))

    near = [s for s in others if s[2] != FAR]
    o_copy(*near[0]).start()
    for hop in hops:
        o_hop(*hop).start()
    for s in near[1:]:
        o_copy(*s).start()

    for t, dy in enumerate(O_ORDER):
        for cp in w_copies(t):
            cp.wait()
        heads = [pt.head(dx, dy) for dx in range(2)]
        for dx in range(2):
            if dy == 0 and dx == 0:
                own.wait()
            elif dy == FAR:
                for half in range(2):
                    put(robuf.at[half, dx], obuf.at[heads[dx], rows(half)], ro_send.at[half, dx], of_recv.at[dx, half],
                        me).wait_recv()
            else:
                put(obuf.at[heads[dx]], obuf.at[heads[dx]], o_send.at[0], o_recv.at[heads[dx]], me).wait_recv()
        a = jnp.concatenate([obuf[heads[0]], obuf[heads[1]]], axis=1)
        for u in range(nc):
            r = jnp.dot(a, wob[t, :, u * wn:(u + 1) * wn], preferred_element_type=jnp.float32)
            if t > 0:
                r = r + acc[:, u * wn:(u + 1) * wn]
            if t < len(O_ORDER) - 1:
                acc[:, u * wn:(u + 1) * wn] = r
            else:
                y_ref[:, u * wn:(u + 1) * wn] = r.astype(y_ref.dtype)
        if t == 0:
            for half, dx in hops:
                put(robuf.at[half, dx], robuf.at[half, dx], o_send.at[0], ro_recv.at[half, dx], me).wait_recv()
                o_hand(half, dx).start()
    for s in near:
        o_copy(*s).wait_send()
    for hop in hops:
        o_hop(*hop).wait_send()
        o_hand(*hop).wait_send()


def solution(mesh):
    n = mesh.shape["cp"]
    side = math.isqrt(n // 2)
    bf, f32 = jnp.bfloat16, jnp.float32
    vmem, anym = pl.BlockSpec(memory_space=pltpu.VMEM), pl.BlockSpec(memory_space=pltpu.HBM)
    dma = pltpu.SemaphoreType.DMA

    def local(x, seg, wq, wk, wv, wo):
        lq, d = x.shape
        hkv = wk.shape[1] // DH
        g = wq.shape[1] // wk.shape[1]
        gd = g * DH
        ng = 2 * side
        kv_parts = jax.ShapeDtypeStruct((ng, 2, 2, PC, DH), bf)
        q_parts = jax.ShapeDtypeStruct((ng, 2, g, PC, DH), bf)
        skv, sq = pl.pallas_call(
            functools.partial(_project, n, g),
            out_shape=(kv_parts, q_parts),
            in_specs=[vmem, anym, anym, anym],
            out_specs=(anym, anym),
            scratch_shapes=[
                pltpu.VMEM((side, d, 4 * DH), bf), pltpu.VMEM((side, d, 2 * gd), bf),
                pltpu.VMEM(kv_parts.shape, bf), pltpu.VMEM(q_parts.shape, bf),
                dma((side, 4)), dma((side, 2)), dma((ng,)),
            ],
            compiler_params=pltpu.CompilerParams(vmem_limit_bytes=60 << 20),
            name="project",
        )(x, wk, wv, wq)
        kv, q, segs = pl.pallas_call(
            functools.partial(_exchange, n),
            out_shape=(jax.ShapeDtypeStruct((n, 2, 2, PC, DH), bf), q_parts, jax.ShapeDtypeStruct((n, 2, PC), jnp.int32)),
            in_specs=[vmem, anym, anym],
            out_specs=(anym, anym, vmem),
            scratch_shapes=[
                pltpu.VMEM((n, 2, 2, PC, DH), bf), pltpu.VMEM(q_parts.shape, bf),
                pltpu.VMEM((2, 2, 2, PC, DH), bf), pltpu.VMEM((2, 2, g, PC, DH), bf), pltpu.VMEM((n, 2, PC), jnp.int32),
                dma((2,)), dma((ng + 2,)), dma((n,)), dma((2, 2)), dma((2, 2)), dma((2, 2)),
                dma((ng,)), dma((2 * ng,)),
                dma((ng + 2,)), dma((ng,)), dma((2, 2)), dma((2, 2)), dma((2, 2)), dma((n,)), dma((n,)), dma((n,)), dma((ng,)),
            ],
            compiler_params=pltpu.CompilerParams(collective_id=0, has_side_effects=True, vmem_limit_bytes=60 << 20),
            name="exchange",
        )(seg.reshape(1, 2, PC), skv, sq)
        scale = DH ** -0.5 * math.log2(math.e)
        o = pl.pallas_call(
            functools.partial(_attend, n, g, scale),
            out_shape=jax.ShapeDtypeStruct((ng, lq, gd), bf),
            in_specs=[anym] * 3,
            out_specs=anym,
            scratch_shapes=[pltpu.SMEM((n, 2, PC), jnp.int32), pltpu.VMEM((n, 2, PC), jnp.int32),
                            pltpu.VMEM((2 * n, 2, PC, DH), bf), pltpu.VMEM((ng, 2, g, PC, DH), bf),
                            pltpu.VMEM((ng, lq, gd), bf), pltpu.SMEM((2 * ng,), jnp.int32), pltpu.VMEM((2, g * PC, DH), f32),
                            pltpu.VMEM((2, g * PC, DH), f32), pltpu.VMEM((2, g * PC, DH), f32), dma((2,)), dma, dma, dma],
            compiler_params=pltpu.CompilerParams(vmem_limit_bytes=60 << 20),
            name="attend",
        )(segs, kv, q)
        return pl.pallas_call(
            functools.partial(_combine, n, gd),
            out_shape=jax.ShapeDtypeStruct((lq, wo.shape[1]), bf),
            in_specs=[anym, anym],
            out_specs=vmem,
            scratch_shapes=[pltpu.VMEM((hkv, lq, gd), bf), pltpu.VMEM((2, 2, PC, gd), bf),
                            pltpu.VMEM((side, 2 * gd, wo.shape[1]), bf),
                            pltpu.VMEM((lq, wo.shape[1]), f32), dma((side, 2)), dma((ng + 2,)), dma((ng,)), dma((2, 2)), dma((2, 2)),
                            dma((2, 2))],
            compiler_params=pltpu.CompilerParams(collective_id=1, has_side_effects=True, vmem_limit_bytes=60 << 20),
            name="combine",
        )(o, wo)

    rows = P(("dp", "cp"), None)
    return jax.shard_map(local, mesh=mesh, in_specs=(rows, P(("dp", "cp")), P(), P(), P(), P()), out_specs=rows, check_vma=False)
```

```python
import functools
import math

import jax
import jax.numpy as jnp
from jax import lax
from jax.experimental import pallas as pl
from jax.experimental.pallas import tpu as pltpu
from jax.sharding import PartitionSpec as P

DH = 128
PC = 128
KB = 4
MESH = pl.DeviceIdType.MESH
NEG_INF = float("-inf")
FLOOR = -3e38


class Place:
    def __init__(self, n):
        me = lax.axis_index("cp")
        self.n, self.side = n, math.isqrt(n // 2)
        self.me = me
        self.c = lax.rem(me, 2)
        chip = me // 2
        self.x = lax.rem(chip, self.side)
        self.y = chip // self.side
        self.xin = self.x + 1 - 2 * lax.rem(self.x, 2)
        self.xcross = self.side - 1 - self.x
        self.px = lax.rem(lax.rem(self.x, 2) + self.x // 2, 2)

    def dev(self, x, y, c):
        return (y * self.side + x) * 2 + c

    def row(self, dy):
        return lax.rem(self.y + dy + self.side, self.side)

    def col(self, dx):
        return self.xin if dx else self.x

    def peer(self, dx, dy):
        return self.dev(self.col(dx), self.row(dy), self.c)

    def head(self, dx, dy):
        return lax.rem(self.px + dx, 2) * self.side + self.row(dy)

    def slot(self, dx, dy):
        return self.row(dy) * 2 + lax.rem(self.x + dx, 2)


FAR = 2
KV_ORDER = (FAR, 0, 1, -1)
Q_ORDER = (FAR, 1, -1, 0)
O_ORDER = (0, 1, -1, FAR)


def _project(n, g, x_ref, seg_ref, wk, wv, wq, kv_o, q_o, segs_o, wkvb, wqb, kvacc, qacc, kvb, qb, skv, sq, rkv, rq, segb,
             wkv_sem, wq_sem, kv_send, kv_recv, kvf_recv, rkv_recv, rkv_send, fx_send, fs_send,
             q_send, q_recv, qf_recv, rq_recv, rq_send, seg_send, seg_recv, out_sem, qout_sem):
    pt = Place(n)
    me = pt.me
    kv_steps = [(t, dx, dy) for t, dy in enumerate(KV_ORDER) for dx in range(2)]
    q_steps = [(t, dx, dy) for t, dy in enumerate(Q_ORDER) for dx in range(2)]
    own_kv = (KV_ORDER.index(0), 0)
    own_q = (Q_ORDER.index(0), 0)
    gd = g * DH
    kr = wqb.shape[1]
    nk = wqb.shape[0]
    my_head, my_slot = pt.head(0, 0), pt.slot(0, 0)

    kv_copies = [[pltpu.make_async_copy(w.at[pl.ds(t * kr, kr)], wkvb.at[i, t], wkv_sem.at[i, t]) for i, w in enumerate((wk, wv))]
                 for t in range(nk)]
    q_copies = [pltpu.make_async_copy(wq.at[pl.ds(t * kr, kr)], wqb.at[t], wq_sem.at[t]) for t in range(nk)]
    for cps in kv_copies:
        for cp in cps:
            cp.start()
    for cp in q_copies:
        cp.start()

    barrier = pltpu.get_barrier_semaphore()

    @pl.loop(1, n)
    def _(i):
        pl.semaphore_signal(barrier, inc=1, device_id={"cp": lax.rem(me + i, n)}, device_id_type=MESH)

    def seg_copy(i):
        return pltpu.make_async_remote_copy(seg_ref, segb.at[pl.ds(me, 1)], seg_send.at[i], seg_recv.at[me],
                                            device_id={"cp": lax.rem(me + i, n)}, device_id_type=MESH)

    segb[pl.ds(me, 1)] = seg_ref[...]

    def put(src, dst, send, recv, dev):
        return pltpu.make_async_remote_copy(src, dst, send, recv, device_id={"cp": dev}, device_id_type=MESH)

    def kv_copy(t, dx, dy):
        return put(skv.at[pt.head(dx, dy)], kvb.at[me], kv_send.at[2 * t + dx], kv_recv.at[me], pt.peer(dx, dy))

    def q_copy(t, dx, dy):
        return put(sq.at[pt.head(dx, dy)], qb.at[my_slot], q_send.at[2 * t + dx], q_recv.at[my_slot], pt.peer(dx, dy))

    way = (1, -1)
    hops = [(half, dx) for half in range(2) for dx in range(2)]

    def kv_hop(half, dx):
        return put(skv.at[pt.head(dx, FAR), half], rkv.at[half, dx], kv_send.at[2 * half + dx if half == 0 else 2 * len(KV_ORDER) + dx],
                   rkv_recv.at[half, dx], pt.peer(0, way[half]))

    def kv_hand(half, dx):
        return put(rkv.at[half, dx], kvb.at[pt.peer(0, -way[half]), half], rkv_send.at[half, dx], kvf_recv.at[dx, half],
                   pt.peer(dx, way[half]))

    def q_hop(half, dx):
        return put(sq.at[pt.head(dx, FAR), half], rq.at[half, dx], q_send.at[2 * half + dx if half == 0 else 2 * len(Q_ORDER) + dx],
                   rq_recv.at[half, dx], pt.peer(0, way[half]))

    def q_hand(half, dx):
        return put(rq.at[half, dx], qb.at[pt.slot(0, -way[half]), half], rq_send.at[half, dx], qf_recv.at[dx, half],
                   pt.peer(dx, way[half]))

    nb = 4 * DH

    def summed(t, w, acc, c):
        cols = slice(c * nb, (c + 1) * nb)
        r = jnp.dot(x_ref[:, t * kr:(t + 1) * kr], w[:, cols], preferred_element_type=jnp.float32)
        if t > 0:
            r = r + acc[:, cols]
        if t < nk - 1:
            acc[:, cols] = r
        return r

    def kv_step(t):
        for cp in kv_copies[t]:
            cp.wait()
        for c in range(wkvb.shape[3] // nb):
            for i in range(2):
                r = summed(t, wkvb.at[i, t], kvacc.at[i], c)
                if t == nk - 1:
                    for u in range(nb // DH):
                        part = r[:, u * DH:(u + 1) * DH]
                        part = (jnp.transpose(part) if i == 0 else part).astype(jnp.bfloat16)
                        for half in range(2):
                            rows = slice(half * PC, (half + 1) * PC)
                            skv[c * (nb // DH) + u, half, i] = part[:, rows] if i == 0 else part[rows]

    def q_step(t, first, last):
        if first == 0:
            q_copies[t].wait()
        for c in range(first, last):
            r = summed(t, wqb.at[t], qacc, c)
            if t == nk - 1:
                for u in range(nb // DH):
                    col = c * (nb // DH) + u
                    for half in range(2):
                        sq[col // g, half, col % g] = r[half * PC:(half + 1) * PC, u * DH:(u + 1) * DH].astype(jnp.bfloat16)

    def send_kv(t):
        if KV_ORDER[t] == FAR:
            for hop in hops:
                kv_hop(*hop).start()
        else:
            for dx in range(2):
                if (t, dx) != own_kv:
                    kv_copy(t, dx, KV_ORDER[t]).start()

    def send_q(t):
        if Q_ORDER[t] == FAR:
            for hop in hops:
                q_hop(*hop).start()
        else:
            for dx in range(2):
                if (t, dx) != own_q:
                    q_copy(t, dx, Q_ORDER[t]).start()

    def to_cross(src, i):
        return put(kvb.at[src], kvb.at[src], fx_send.at[i], kv_recv.at[src], pt.dev(pt.xcross, pt.y, pt.c))

    def to_sibling(src, i):
        return put(kvb.at[src], kvb.at[src], fs_send.at[i], kv_recv.at[src], pt.dev(pt.x, pt.y, 1 - pt.c))

    def kv_out(src):
        return pltpu.make_async_copy(kvb.at[src], kv_o.at[src], out_sem.at[src])

    def q_out(slot):
        return pltpu.make_async_copy(qb.at[slot], q_o.at[slot], qout_sem.at[slot])

    def arrived(src):
        to_sibling(src, 0).wait_recv()

    def forward(t):
        dy = KV_ORDER[t]
        for dx in range(2):
            src = pt.peer(dx, -dy)
            if dy == FAR:
                for half in range(2):
                    put(rkv.at[half, dx], kvb.at[src, half], rkv_send.at[half, dx], kvf_recv.at[dx, half], me).wait_recv()
            elif (t, dx) != own_kv:
                arrived(src)
            to_cross(src, 2 * t + dx).start()
            to_sibling(src, 2 * t + dx).start()
            kv_out(src).start()

    def own_out():
        return pltpu.make_async_copy(skv.at[my_head], kv_o.at[me], out_sem.at[me])

    def own_q_out():
        return pltpu.make_async_copy(sq.at[my_head], q_o.at[my_slot], qout_sem.at[my_slot])

    def forward_own():
        put(skv.at[my_head], kvb.at[me], fx_send.at[2 * own_kv[0]], kv_recv.at[me], pt.dev(pt.xcross, pt.y, pt.c)).start()
        put(skv.at[my_head], kvb.at[me], fs_send.at[2 * own_kv[0]], kv_recv.at[me], pt.dev(pt.x, pt.y, 1 - pt.c)).start()
        own_out().start()

    def forward_next():
        src = pt.peer(1, 0)
        arrived(src)
        to_cross(src, 2 * own_kv[0] + 1).start()
        to_sibling(src, 2 * own_kv[0] + 1).start()
        kv_out(src).start()

    for t in range(nk):
        kv_step(t)
    nq = wqb.shape[2] // nb
    q_step(0, 0, 1)

    pl.semaphore_wait(barrier, n - 1)
    for t in range(len(KV_ORDER)):
        send_kv(t)
    forward_own()
    q_step(0, 1, nq)
    q_step(1, 0, nq)
    q_step(2, 0, nq)
    forward_next()
    for hop in hops:
        put(rkv.at[hop], rkv.at[hop], kv_send.at[0], rkv_recv.at[hop], me).wait_recv()
        kv_hand(*hop).start()
    q_step(3, 0, nq)
    forward(2)
    for t in range(len(Q_ORDER)):
        send_q(t)
    own_q_out().start()
    forward(3)
    forward(0)

    @pl.loop(1, n)
    def _(i):
        seg_copy(i).start()


    def mirrored(dx, dy, c):
        x = pt.side - 1 - pt.col(dx)
        return pt.dev(x, pt.row(-dy), c)

    passing = [(t, dx, KV_ORDER[t]) for t in (1, 2, 3, 0) for dx in range(2)]

    def pass_on(steps):
        for t, dx, dy in steps:
            src = mirrored(dx, dy, pt.c)
            arrived(src)
            to_sibling(src, 8 + 2 * t + dx).start()
            kv_out(src).start()

    pass_on(passing[:2])
    for hop in hops:
        put(rq.at[hop], rq.at[hop], q_send.at[0], rq_recv.at[hop], me).wait_recv()
        q_hand(*hop).start()
    pass_on(passing[2:])

    for t, dx, dy in passing:
        src = pt.dev(pt.col(dx), pt.row(-dy), 1 - pt.c)
        arrived(src)
        kv_out(src).start()
    for t, dx, dy in q_steps:
        slot = pt.slot(dx, -dy)
        if dy == FAR:
            for half in range(2):
                put(rq.at[half, dx], qb.at[slot, half], rq_send.at[half, dx], qf_recv.at[dx, half], me).wait_recv()
        elif (t, dx) != own_q:
            put(qb.at[slot], qb.at[slot], q_send.at[0], q_recv.at[slot], me).wait_recv()
        if (t, dx) != own_q:
            q_out(slot).start()
    for t, dx, dy in passing:
        src = mirrored(dx, dy, 1 - pt.c)
        arrived(src)
        kv_out(src).start()

    @pl.loop(1, n)
    def _(i):
        src = lax.rem(me + i, n)
        pltpu.make_async_remote_copy(seg_ref, segb.at[pl.ds(src, 1)], seg_send.at[i], seg_recv.at[src],
                                     device_id={"cp": src}, device_id_type=MESH).wait_recv()

    segs_o[...] = segb[...]

    @pl.loop(1, n)
    def _(i):
        seg_copy(i).wait_send()

    for hop in hops:
        kv_hop(*hop).wait_send()
        kv_hand(*hop).wait_send()
        q_hop(*hop).wait_send()
        q_hand(*hop).wait_send()
    for t, dx, dy in kv_steps:
        if dy != FAR and (t, dx) != own_kv:
            kv_copy(t, dx, dy).wait_send()
        src = pt.peer(dx, -dy)
        to_cross(src, 2 * t + dx).wait_send()
        to_sibling(src, 2 * t + dx).wait_send()
        to_sibling(src, 8 + 2 * t + dx).wait_send()
    for t, dx, dy in q_steps:
        if dy != FAR and (t, dx) != own_q:
            q_copy(t, dx, dy).wait_send()

    @pl.loop(0, n)
    def _(i):
        kv_out(i).wait()

    @pl.loop(0, n // 4)
    def _(i):
        q_out(i).wait()


def _attend(n, g, scale, segs, kv, q_in, o_out, seg_s, seg_v, kvs, qs, os, lo_s, m_sc, l_sc, acc_sc, seg_sem, kv_sem, q_sem, o_sem):
    pt = Place(n)
    last_piece = 2 * n - 1
    rows = g * PC
    ng = q_in.shape[0]

    def owner(p):
        return jnp.where(p < n, p, last_piece - p)

    def half_of(p):
        return jnp.where(p < n, 0, 1)

    def load(p):
        return pltpu.make_async_copy(kv.at[owner(p), half_of(p)], kvs.at[p], kv_sem)

    seg_copies = [pltpu.make_async_copy(segs, seg_v, seg_sem.at[0]), pltpu.make_async_copy(segs, seg_s, seg_sem.at[1])]
    q_copy = pltpu.make_async_copy(q_in, qs, q_sem)
    for cp in seg_copies:
        cp.start()
    q_copy.start()

    @pl.loop(0, 2 * n)
    def _(p):
        load(p).start()

    def source(i):
        slot, half = i // 2, i % 2
        xs = (pt.x // 2) * 2 + slot % 2
        return pt.dev(xs, slot // 2, pt.c), half

    for cp in seg_copies:
        cp.wait()
    for i in range(2 * ng):
        src, half = source(i)
        before = jnp.where(seg_v[...] < seg_s[src, half, 0], 1.0, 0.0)
        lo_s[i] = jnp.sum(before).astype(jnp.int32) // PC
    q_copy.wait()

    @pl.loop(0, 2 * n)
    def _(p):
        load(p).wait()

    def lanes(col):
        return jnp.broadcast_to(col, (col.shape[0], DH))

    def out(slot, half):
        at = pl.ds(pl.multiple_of(half * PC, PC), PC)
        return pltpu.make_async_copy(os.at[slot, at], o_out.at[slot, at], o_sem)

    def pair(i, carry):
        row, half = lax.div(i, 2), lax.rem(i, 2)
        slots = [2 * row + u for u in range(2)]
        srcs = [pt.dev((pt.x // 2) * 2 + u, row, pt.c) for u in range(2)]
        ps = [jnp.where(half == 0, src, last_piece - src) for src in srcs]
        firsts = [seg_s[src, half, 0] for src in srcs]
        lo = jnp.minimum(lo_s[2 * slots[0] + half], lo_s[2 * slots[1] + half])
        end = jnp.maximum(ps[0], ps[1])
        m_sc[...] = jnp.full_like(m_sc, FLOOR)
        l_sc[...] = jnp.zeros_like(l_sc)
        acc_sc[...] = jnp.zeros_like(acc_sc)

        def query(u):
            return qs[slots[u], half].reshape(rows, DH)

        def off(b, carry):
            j0 = lo + b * KB
            js = jnp.minimum(j0, 2 * n - KB)
            kt = jnp.concatenate([kvs[js + w, 0] for w in range(KB)], axis=1)
            v = jnp.concatenate([kvs[js + w, 1] for w in range(KB)], axis=0)
            ids = [seg_v[owner(js + w), pl.ds(half_of(js + w), 1), :] for w in range(KB)]
            ss = [jnp.dot(query(u), kt, preferred_element_type=jnp.float32) for u in range(2)]
            for u in range(2):
                parts = []
                for w in range(KB):
                    j = js + w
                    want = jnp.where((j >= j0) & (j < ps[u]), firsts[u], -1)
                    parts.append(ss[u][:, w * PC:(w + 1) * PC] * scale + jnp.where(ids[w] == want, 0.0, NEG_INF))
                m_old = m_sc[u]
                m_new = jnp.maximum(m_old, lanes(jnp.max(functools.reduce(jnp.maximum, parts), axis=1, keepdims=True)))
                corr = jnp.exp2(m_old - m_new)
                pr = [jnp.exp2(t - m_new) for t in parts]
                l_sc[u] = l_sc[u] * corr + functools.reduce(jnp.add, pr)
                pb = jnp.concatenate([t.astype(jnp.bfloat16) for t in pr], axis=1)
                acc_sc[u] = acc_sc[u] * corr + jnp.dot(pb, v, preferred_element_type=jnp.float32)
                m_sc[u] = m_new
            return carry

        lax.fori_loop(0, lax.div(end - lo + KB - 1, KB), off, 0)

        r = lax.broadcasted_iota(jnp.int32, (PC, PC), 0)
        cidx = lax.broadcasted_iota(jnp.int32, (PC, PC), 1)
        ss = [jnp.dot(query(u), kvs[ps[u], 0], preferred_element_type=jnp.float32) * scale for u in range(2)]
        for u in range(2):
            ids = jnp.broadcast_to(seg_v[srcs[u], pl.ds(half, 1), :], (PC, PC))
            ids_t = jnp.transpose(ids)
            allowed = jnp.concatenate([(ids == ids_t) & (cidx <= r)] * g, axis=0)
            keep = jnp.concatenate([ids_t == firsts[u]] * g, axis=0)
            s = jnp.where(allowed, ss[u], NEG_INF)
            m_old = jnp.where(keep, m_sc[u], FLOOR)
            m_new = jnp.maximum(m_old, lanes(jnp.max(s, axis=1, keepdims=True)))
            corr = jnp.exp2(m_old - m_new)
            pr = jnp.exp2(s - m_new)
            l = jnp.where(keep, l_sc[u], 0.0) * corr + pr
            acc = jnp.where(keep, acc_sc[u], 0.0) * corr
            acc = acc + jnp.dot(pr.astype(jnp.bfloat16), kvs[ps[u], 1], preferred_element_type=jnp.float32)
            o = (acc / lanes(jnp.sum(l, axis=1, keepdims=True))).astype(jnp.bfloat16)
            for w in range(g):
                os[slots[u], pl.ds(pl.multiple_of(half * PC, PC), PC), w * DH:(w + 1) * DH] = o[w * PC:(w + 1) * PC]

        @pl.when(i > 0)
        def _():
            for u in range(2):
                out(2 * lax.div(i - 1, 2) + u, lax.rem(i - 1, 2)).start()

        return carry

    lax.fori_loop(0, ng, pair, 0)
    for u in range(2):
        out(ng - 2 + u, 1).start()

    @pl.loop(0, 2 * ng)
    def _(i):
        out(lax.div(i, 2), lax.rem(i, 2)).wait()


def _combine(n, gd, o_in, wo, y_ref, obuf, robuf, wob, acc, w_sem, o_send, o_recv, of_recv, ro_recv, ro_send):
    pt = Place(n)
    me = pt.me
    my_head = pt.head(0, 0)
    d_out = y_ref.shape[1]
    nc = 4
    wn = d_out // nc

    def w_copies(t):
        for dx in range(2):
            h = pl.multiple_of(pt.head(dx, O_ORDER[t]) * gd, gd)
            yield pltpu.make_async_copy(wo.at[pl.ds(h, gd), :], wob.at[t, pl.ds(dx * gd, gd), :], w_sem.at[t, dx])

    for t in range(len(O_ORDER)):
        for cp in w_copies(t):
            cp.start()
    own = pltpu.make_async_copy(o_in.at[pt.slot(0, 0)], obuf.at[my_head], o_recv.at[my_head])
    own.start()

    steps = [(t, dx, dy) for t, dy in enumerate(O_ORDER) for dx in range(2)]
    others = [s for s in steps if (s[1], s[2]) != (0, 0)]
    barrier = pltpu.get_barrier_semaphore()
    for t, dx, dy in others:
        pl.semaphore_signal(barrier, inc=1, device_id={"cp": pt.peer(dx, dy)}, device_id_type=MESH)
    pl.semaphore_wait(barrier, len(others))

    def put(src, dst, send, recv, dev):
        return pltpu.make_async_remote_copy(src, dst, send, recv, device_id={"cp": dev}, device_id_type=MESH)

    def o_copy(t, dx, dy):
        return put(o_in.at[pt.slot(dx, dy)], obuf.at[my_head], o_send.at[2 * t + dx], o_recv.at[my_head], pt.peer(dx, dy))

    way = (1, -1)
    hops = [(half, dx) for half in range(2) for dx in range(2)]

    def rows(half):
        return pl.ds(half * PC, PC)

    def o_hop(half, dx):
        return put(o_in.at[pt.slot(dx, FAR), rows(half)], robuf.at[half, dx], o_send.at[2 * len(O_ORDER) - 2 + 2 * half + dx],
                   ro_recv.at[half, dx], pt.peer(0, way[half]))

    def o_hand(half, dx):
        return put(robuf.at[half, dx], obuf.at[pt.head(0, -way[half]), rows(half)], ro_send.at[half, dx], of_recv.at[dx, half],
                   pt.peer(dx, way[half]))

    near = [s for s in others if s[2] != FAR]
    o_copy(*near[0]).start()
    for hop in hops:
        o_hop(*hop).start()
    for s in near[1:]:
        o_copy(*s).start()

    for t, dy in enumerate(O_ORDER):
        for cp in w_copies(t):
            cp.wait()
        heads = [pt.head(dx, dy) for dx in range(2)]
        for dx in range(2):
            if dy == 0 and dx == 0:
                own.wait()
            elif dy == FAR:
                for half in range(2):
                    put(robuf.at[half, dx], obuf.at[heads[dx], rows(half)], ro_send.at[half, dx], of_recv.at[dx, half],
                        me).wait_recv()
            else:
                put(obuf.at[heads[dx]], obuf.at[heads[dx]], o_send.at[0], o_recv.at[heads[dx]], me).wait_recv()
        a = jnp.concatenate([obuf[heads[0]], obuf[heads[1]]], axis=1)
        for u in range(nc):
            r = jnp.dot(a, wob[t, :, u * wn:(u + 1) * wn], preferred_element_type=jnp.float32)
            if t > 0:
                r = r + acc[:, u * wn:(u + 1) * wn]
            if t < len(O_ORDER) - 1:
                acc[:, u * wn:(u + 1) * wn] = r
            else:
                y_ref[:, u * wn:(u + 1) * wn] = r.astype(y_ref.dtype)
        if t == 0:
            for half, dx in hops:
                put(robuf.at[half, dx], robuf.at[half, dx], o_send.at[0], ro_recv.at[half, dx], me).wait_recv()
                o_hand(half, dx).start()
    for s in near:
        o_copy(*s).wait_send()
    for hop in hops:
        o_hop(*hop).wait_send()
        o_hand(*hop).wait_send()


def solution(mesh):
    n = mesh.shape["cp"]
    side = math.isqrt(n // 2)
    bf, f32 = jnp.bfloat16, jnp.float32
    vmem, anym = pl.BlockSpec(memory_space=pltpu.VMEM), pl.BlockSpec(memory_space=pltpu.HBM)
    dma = pltpu.SemaphoreType.DMA

    def local(x, seg, wq, wk, wv, wo):
        lq, d = x.shape
        hkv = wk.shape[1] // DH
        g = wq.shape[1] // wk.shape[1]
        gd = g * DH
        ng = 2 * side
        kv, q, segs = pl.pallas_call(
            functools.partial(_project, n, g),
            out_shape=(jax.ShapeDtypeStruct((n, 2, 2, PC, DH), bf), jax.ShapeDtypeStruct((ng, 2, g, PC, DH), bf),
                       jax.ShapeDtypeStruct((n, 2, PC), jnp.int32)),
            in_specs=[vmem, vmem, anym, anym, anym],
            out_specs=(anym, anym, vmem),
            scratch_shapes=[
                pltpu.VMEM((2, side, d // side, hkv * DH), bf), pltpu.VMEM((side, d // side, hkv * gd), bf),
                pltpu.VMEM((2, lq, hkv * DH), f32), pltpu.VMEM((lq, hkv * gd), f32),
                pltpu.VMEM((n, 2, 2, PC, DH), bf), pltpu.VMEM((ng, 2, g, PC, DH), bf),
                pltpu.VMEM((ng, 2, 2, PC, DH), bf), pltpu.VMEM((ng, 2, g, PC, DH), bf),
                pltpu.VMEM((2, 2, 2, PC, DH), bf), pltpu.VMEM((2, 2, g, PC, DH), bf), pltpu.VMEM((n, 2, PC), jnp.int32),
                dma((2, side)), dma((side,)), dma((ng + 2,)), dma((n,)), dma((2, 2)), dma((2, 2)), dma((2, 2)),
                dma((ng,)), dma((2 * ng,)),
                dma((ng + 2,)), dma((ng,)), dma((2, 2)), dma((2, 2)), dma((2, 2)), dma((n,)), dma((n,)), dma((n,)), dma((ng,)),
            ],
            compiler_params=pltpu.CompilerParams(collective_id=0, has_side_effects=True, vmem_limit_bytes=60 << 20),
            name="project",
        )(x, seg.reshape(1, 2, PC), wk, wv, wq)
        scale = DH ** -0.5 * math.log2(math.e)
        o = pl.pallas_call(
            functools.partial(_attend, n, g, scale),
            out_shape=jax.ShapeDtypeStruct((ng, lq, gd), bf),
            in_specs=[anym] * 3,
            out_specs=anym,
            scratch_shapes=[pltpu.SMEM((n, 2, PC), jnp.int32), pltpu.VMEM((n, 2, PC), jnp.int32),
                            pltpu.VMEM((2 * n, 2, PC, DH), bf), pltpu.VMEM((ng, 2, g, PC, DH), bf),
                            pltpu.VMEM((ng, lq, gd), bf), pltpu.SMEM((2 * ng,), jnp.int32), pltpu.VMEM((2, g * PC, DH), f32),
                            pltpu.VMEM((2, g * PC, DH), f32), pltpu.VMEM((2, g * PC, DH), f32), dma((2,)), dma, dma, dma],
            compiler_params=pltpu.CompilerParams(vmem_limit_bytes=60 << 20),
            name="attend",
        )(segs, kv, q)
        return pl.pallas_call(
            functools.partial(_combine, n, gd),
            out_shape=jax.ShapeDtypeStruct((lq, wo.shape[1]), bf),
            in_specs=[anym, anym],
            out_specs=vmem,
            scratch_shapes=[pltpu.VMEM((hkv, lq, gd), bf), pltpu.VMEM((2, 2, PC, gd), bf),
                            pltpu.VMEM((side, 2 * gd, wo.shape[1]), bf),
                            pltpu.VMEM((lq, wo.shape[1]), f32), dma((side, 2)), dma((ng + 2,)), dma((ng,)), dma((2, 2)), dma((2, 2)),
                            dma((2, 2))],
            compiler_params=pltpu.CompilerParams(collective_id=1, has_side_effects=True, vmem_limit_bytes=60 << 20),
            name="combine",
        )(o, wo)

    rows = P(("dp", "cp"), None)
    return jax.shard_map(local, mesh=mesh, in_specs=(rows, P(("dp", "cp")), P(), P(), P(), P()), out_specs=rows, check_vma=False)
```

```python
import functools
import math

import jax
import jax.numpy as jnp
from jax import lax
from jax.experimental import pallas as pl
from jax.experimental.pallas import tpu as pltpu
from jax.sharding import PartitionSpec as P

DH = 128
PC = 128
KB = 4
MESH = pl.DeviceIdType.MESH
NEG_INF = float("-inf")
FLOOR = -3e38


class Place:
    def __init__(self, n):
        me = lax.axis_index("cp")
        self.n, self.side = n, math.isqrt(n // 2)
        self.me = me
        self.c = lax.rem(me, 2)
        chip = me // 2
        self.x = lax.rem(chip, self.side)
        self.y = chip // self.side
        self.xin = self.x + 1 - 2 * lax.rem(self.x, 2)
        self.xcross = self.side - 1 - self.x
        self.px = lax.rem(lax.rem(self.x, 2) + self.x // 2, 2)

    def dev(self, x, y, c):
        return (y * self.side + x) * 2 + c

    def row(self, dy):
        return lax.rem(self.y + dy + self.side, self.side)

    def col(self, dx):
        return self.xin if dx else self.x

    def peer(self, dx, dy):
        return self.dev(self.col(dx), self.row(dy), self.c)

    def head(self, dx, dy):
        return lax.rem(self.px + dx, 2) * self.side + self.row(dy)

    def slot(self, dx, dy):
        return self.row(dy) * 2 + lax.rem(self.x + dx, 2)


FAR = 2
KV_ORDER = (FAR, 0, 1, -1)
Q_ORDER = (FAR, 1, -1, 0)
O_ORDER = (0, 1, -1, FAR)


def _project(n, g, x_ref, seg_ref, wk, wv, wq, kv_o, q_o, segs_o, wkvb, wqb, kvacc, qacc, kvb, qb, skv, sq, rkv, rq, segb,
             wkv_sem, wq_sem, kv_send, kv_recv, kvf_recv, rkv_recv, rkv_send, fx_send, fs_send,
             q_send, q_recv, qf_recv, rq_recv, rq_send, seg_send, seg_recv, out_sem, qout_sem):
    pt = Place(n)
    me = pt.me
    kv_steps = [(t, dx, dy) for t, dy in enumerate(KV_ORDER) for dx in range(2)]
    q_steps = [(t, dx, dy) for t, dy in enumerate(Q_ORDER) for dx in range(2)]
    own_kv = (KV_ORDER.index(0), 0)
    own_q = (Q_ORDER.index(0), 0)
    gd = g * DH
    kr = wqb.shape[1]
    nk = wqb.shape[0]
    my_head, my_slot = pt.head(0, 0), pt.slot(0, 0)

    kv_copies = [[pltpu.make_async_copy(w.at[pl.ds(t * kr, kr)], wkvb.at[i, t], wkv_sem.at[i, t]) for i, w in enumerate((wk, wv))]
                 for t in range(nk)]
    q_copies = [pltpu.make_async_copy(wq.at[pl.ds(t * kr, kr)], wqb.at[t], wq_sem.at[t]) for t in range(nk)]
    for cps in kv_copies:
        for cp in cps:
            cp.start()
    for cp in q_copies:
        cp.start()

    barrier = pltpu.get_barrier_semaphore()

    @pl.loop(1, n)
    def _(i):
        pl.semaphore_signal(barrier, inc=1, device_id={"cp": lax.rem(me + i, n)}, device_id_type=MESH)

    def seg_copy(i):
        return pltpu.make_async_remote_copy(seg_ref, segb.at[pl.ds(me, 1)], seg_send.at[i], seg_recv.at[me],
                                            device_id={"cp": lax.rem(me + i, n)}, device_id_type=MESH)

    segb[pl.ds(me, 1)] = seg_ref[...]

    def put(src, dst, send, recv, dev):
        return pltpu.make_async_remote_copy(src, dst, send, recv, device_id={"cp": dev}, device_id_type=MESH)

    def kv_copy(t, dx, dy):
        return put(skv.at[pt.head(dx, dy)], kvb.at[me], kv_send.at[2 * t + dx], kv_recv.at[me], pt.peer(dx, dy))

    def q_copy(t, dx, dy):
        return put(sq.at[pt.head(dx, dy)], qb.at[my_slot], q_send.at[2 * t + dx], q_recv.at[my_slot], pt.peer(dx, dy))

    way = (1, -1)
    hops = [(half, dx) for half in range(2) for dx in range(2)]

    def kv_hop(half, dx):
        return put(skv.at[pt.head(dx, FAR), half], rkv.at[half, dx], kv_send.at[2 * half + dx if half == 0 else 2 * len(KV_ORDER) + dx],
                   rkv_recv.at[half, dx], pt.peer(0, way[half]))

    def kv_hand(half, dx):
        return put(rkv.at[half, dx], kvb.at[pt.peer(0, -way[half]), half], rkv_send.at[half, dx], kvf_recv.at[dx, half],
                   pt.peer(dx, way[half]))

    def q_hop(half, dx):
        return put(sq.at[pt.head(dx, FAR), half], rq.at[half, dx], q_send.at[2 * half + dx if half == 0 else 2 * len(Q_ORDER) + dx],
                   rq_recv.at[half, dx], pt.peer(0, way[half]))

    def q_hand(half, dx):
        return put(rq.at[half, dx], qb.at[pt.slot(0, -way[half]), half], rq_send.at[half, dx], qf_recv.at[dx, half],
                   pt.peer(dx, way[half]))

    nb = 4 * DH

    def summed(t, w, acc, c):
        cols = slice(c * nb, (c + 1) * nb)
        r = jnp.dot(x_ref[:, t * kr:(t + 1) * kr], w[:, cols], preferred_element_type=jnp.float32)
        if t > 0:
            r = r + acc[:, cols]
        if t < nk - 1:
            acc[:, cols] = r
        return r

    def kv_step(t):
        for cp in kv_copies[t]:
            cp.wait()
        for c in range(wkvb.shape[3] // nb):
            for i in range(2):
                r = summed(t, wkvb.at[i, t], kvacc.at[i], c)
                if t == nk - 1:
                    for u in range(nb // DH):
                        part = r[:, u * DH:(u + 1) * DH]
                        part = (jnp.transpose(part) if i == 0 else part).astype(jnp.bfloat16)
                        for half in range(2):
                            rows = slice(half * PC, (half + 1) * PC)
                            skv[c * (nb // DH) + u, half, i] = part[:, rows] if i == 0 else part[rows]

    def q_step(t, first, last):
        if first == 0:
            q_copies[t].wait()
        for c in range(first, last):
            r = summed(t, wqb.at[t], qacc, c)
            if t == nk - 1:
                for u in range(nb // DH):
                    col = c * (nb // DH) + u
                    for half in range(2):
                        sq[col // g, half, col % g] = r[half * PC:(half + 1) * PC, u * DH:(u + 1) * DH].astype(jnp.bfloat16)

    def send_kv(t):
        if KV_ORDER[t] == FAR:
            for hop in hops:
                kv_hop(*hop).start()
        else:
            for dx in range(2):
                if (t, dx) != own_kv:
                    kv_copy(t, dx, KV_ORDER[t]).start()

    def send_q(t):
        if Q_ORDER[t] == FAR:
            for hop in hops:
                q_hop(*hop).start()
        else:
            for dx in range(2):
                if (t, dx) != own_q:
                    q_copy(t, dx, Q_ORDER[t]).start()

    def to_cross(src, i):
        return put(kvb.at[src], kvb.at[src], fx_send.at[i], kv_recv.at[src], pt.dev(pt.xcross, pt.y, pt.c))

    def to_sibling(src, i):
        return put(kvb.at[src], kvb.at[src], fs_send.at[i], kv_recv.at[src], pt.dev(pt.x, pt.y, 1 - pt.c))

    def kv_out(src):
        return pltpu.make_async_copy(kvb.at[src], kv_o.at[src], out_sem.at[src])

    def q_out(slot):
        return pltpu.make_async_copy(qb.at[slot], q_o.at[slot], qout_sem.at[slot])

    def arrived(src):
        to_sibling(src, 0).wait_recv()

    def forward(t):
        dy = KV_ORDER[t]
        for dx in range(2):
            src = pt.peer(dx, -dy)
            if dy == FAR:
                for half in range(2):
                    put(rkv.at[half, dx], kvb.at[src, half], rkv_send.at[half, dx], kvf_recv.at[dx, half], me).wait_recv()
            elif (t, dx) != own_kv:
                arrived(src)
            to_cross(src, 2 * t + dx).start()
            to_sibling(src, 2 * t + dx).start()
            kv_out(src).start()

    def own_out():
        return pltpu.make_async_copy(skv.at[my_head], kv_o.at[me], out_sem.at[me])

    def own_q_out():
        return pltpu.make_async_copy(sq.at[my_head], q_o.at[my_slot], qout_sem.at[my_slot])

    def forward_own():
        put(skv.at[my_head], kvb.at[me], fx_send.at[2 * own_kv[0]], kv_recv.at[me], pt.dev(pt.xcross, pt.y, pt.c)).start()
        put(skv.at[my_head], kvb.at[me], fs_send.at[2 * own_kv[0]], kv_recv.at[me], pt.dev(pt.x, pt.y, 1 - pt.c)).start()
        own_out().start()

    def forward_next():
        src = pt.peer(1, 0)
        arrived(src)
        to_cross(src, 2 * own_kv[0] + 1).start()
        to_sibling(src, 2 * own_kv[0] + 1).start()
        kv_out(src).start()

    for t in range(nk):
        kv_step(t)
    nq = wqb.shape[2] // nb
    q_step(0, 0, 1)

    pl.semaphore_wait(barrier, n - 1)
    for t in range(len(KV_ORDER)):
        send_kv(t)
    forward_own()
    q_step(0, 1, nq)
    q_step(1, 0, nq)
    q_step(2, 0, nq)
    forward_next()
    for hop in hops:
        put(rkv.at[hop], rkv.at[hop], kv_send.at[0], rkv_recv.at[hop], me).wait_recv()
        kv_hand(*hop).start()
    q_step(3, 0, nq)
    forward(2)
    for t in range(len(Q_ORDER)):
        send_q(t)
    own_q_out().start()
    forward(3)
    forward(0)

    @pl.loop(1, n)
    def _(i):
        seg_copy(i).start()


    def mirrored(dx, dy, c):
        x = pt.side - 1 - pt.col(dx)
        return pt.dev(x, pt.row(-dy), c)

    passing = [(t, dx, KV_ORDER[t]) for t in (1, 2, 3, 0) for dx in range(2)]

    def pass_on(steps):
        for t, dx, dy in steps:
            src = mirrored(dx, dy, pt.c)
            arrived(src)
            to_sibling(src, 8 + 2 * t + dx).start()
            kv_out(src).start()

    pass_on(passing[:2])
    for hop in hops:
        put(rq.at[hop], rq.at[hop], q_send.at[0], rq_recv.at[hop], me).wait_recv()
        q_hand(*hop).start()
    pass_on(passing[2:])

    for t, dx, dy in passing:
        src = pt.dev(pt.col(dx), pt.row(-dy), 1 - pt.c)
        arrived(src)
        kv_out(src).start()
    for t, dx, dy in q_steps:
        slot = pt.slot(dx, -dy)
        if dy == FAR:
            for half in range(2):
                put(rq.at[half, dx], qb.at[slot, half], rq_send.at[half, dx], qf_recv.at[dx, half], me).wait_recv()
        elif (t, dx) != own_q:
            put(qb.at[slot], qb.at[slot], q_send.at[0], q_recv.at[slot], me).wait_recv()
        if (t, dx) != own_q:
            q_out(slot).start()
    for t, dx, dy in passing:
        src = mirrored(dx, dy, 1 - pt.c)
        arrived(src)
        kv_out(src).start()

    @pl.loop(1, n)
    def _(i):
        src = lax.rem(me + i, n)
        pltpu.make_async_remote_copy(seg_ref, segb.at[pl.ds(src, 1)], seg_send.at[i], seg_recv.at[src],
                                     device_id={"cp": src}, device_id_type=MESH).wait_recv()

    segs_o[...] = segb[...]

    @pl.loop(1, n)
    def _(i):
        seg_copy(i).wait_send()

    for hop in hops:
        kv_hop(*hop).wait_send()
        kv_hand(*hop).wait_send()
        q_hop(*hop).wait_send()
        q_hand(*hop).wait_send()
    for t, dx, dy in kv_steps:
        if dy != FAR and (t, dx) != own_kv:
            kv_copy(t, dx, dy).wait_send()
        src = pt.peer(dx, -dy)
        to_cross(src, 2 * t + dx).wait_send()
        to_sibling(src, 2 * t + dx).wait_send()
        to_sibling(src, 8 + 2 * t + dx).wait_send()
    for t, dx, dy in q_steps:
        if dy != FAR and (t, dx) != own_q:
            q_copy(t, dx, dy).wait_send()

    @pl.loop(0, n)
    def _(i):
        kv_out(i).wait()

    @pl.loop(0, n // 4)
    def _(i):
        q_out(i).wait()


class Pairs:
    def __init__(self, pt, n, g, scale, first_of, seg_v, kvs, query, t_sc, mx_sc, m_sc, l_sc, acc_sc):
        self.pt, self.n, self.g, self.scale, self.first_of, self.seg_v, self.kvs = pt, n, g, scale, first_of, seg_v, kvs
        self.query, self.t_sc, self.mx_sc, self.m_sc, self.l_sc, self.acc_sc = query, t_sc, mx_sc, m_sc, l_sc, acc_sc

    def __call__(self, row, half, lo_of, store):
        pt, n, g, scale, seg_v, kvs = self.pt, self.n, self.g, self.scale, self.seg_v, self.kvs
        t_sc, mx_sc, m_sc, l_sc, acc_sc = self.t_sc, self.mx_sc, self.m_sc, self.l_sc, self.acc_sc
        last_piece, pieces = 2 * n - 1, kvs.shape[0]
        srcs = [pt.dev((pt.x // 2) * 2 + u, row, pt.c) for u in range(2)]
        ps = [last_piece - src if half else src for src in srcs]
        firsts = [self.first_of(src, half) for src in srcs]
        lo = lo_of(row)
        end = jnp.maximum(ps[0], ps[1])
        m_sc[...] = jnp.full_like(m_sc, FLOOR)
        l_sc[...] = jnp.zeros_like(l_sc)
        acc_sc[...] = jnp.zeros_like(acc_sc)

        def lanes(col):
            return jnp.broadcast_to(col, (col.shape[0], DH))

        def ids_of(p):
            return seg_v[jnp.where(p < n, p, last_piece - p), pl.ds(jnp.where(p < n, 0, 1), 1), :]

        def start(b):
            return jnp.minimum(lo + b * KB, pieces - KB)

        def scores(b):
            j0, js = lo + b * KB, start(b)
            kt = jnp.concatenate([kvs[js + w, 0] for w in range(KB)], axis=1)
            for u in range(2):
                s = jnp.dot(self.query(row, u), kt, preferred_element_type=jnp.float32)
                parts = []
                for w in range(KB):
                    j = js + w
                    want = jnp.where((j >= j0) & (j < ps[u]), firsts[u], -1)
                    part = s[:, w * PC:(w + 1) * PC] * scale + jnp.where(ids_of(j) == want, 0.0, NEG_INF)
                    t_sc[u, w] = part
                    parts.append(part)
                mx_sc[u] = lanes(jnp.max(functools.reduce(jnp.maximum, parts), axis=1, keepdims=True))

        def step(b, carry):
            js = start(b)
            v = jnp.concatenate([kvs[js + w, 1] for w in range(KB)], axis=0)
            for u in range(2):
                m_old = m_sc[u]
                m_new = jnp.maximum(m_old, mx_sc[u])
                corr = jnp.exp2(m_old - m_new)
                pr = [jnp.exp2(t_sc[u, w] - m_new) for w in range(KB)]
                l_sc[u] = l_sc[u] * corr + functools.reduce(jnp.add, pr)
                pb = jnp.concatenate([t.astype(jnp.bfloat16) for t in pr], axis=1)
                acc_sc[u] = acc_sc[u] * corr + jnp.dot(pb, v, preferred_element_type=jnp.float32)
                m_sc[u] = m_new
            scores(b + 1)
            return carry

        scores(0)
        lax.fori_loop(0, lax.div(end - lo + KB - 1, KB), step, 0)

        r = lax.broadcasted_iota(jnp.int32, (PC, PC), 0)
        cidx = lax.broadcasted_iota(jnp.int32, (PC, PC), 1)
        ss = [jnp.dot(self.query(row, u), kvs[ps[u], 0], preferred_element_type=jnp.float32) * scale for u in range(2)]
        for u in range(2):
            ids = jnp.broadcast_to(ids_of(ps[u]), (PC, PC))
            ids_t = jnp.transpose(ids)
            allowed = jnp.concatenate([(ids == ids_t) & (cidx <= r)] * g, axis=0)
            keep = jnp.concatenate([ids_t == firsts[u]] * g, axis=0)
            s = jnp.where(allowed, ss[u], NEG_INF)
            m_old = jnp.where(keep, m_sc[u], FLOOR)
            m_new = jnp.maximum(m_old, lanes(jnp.max(s, axis=1, keepdims=True)))
            corr = jnp.exp2(m_old - m_new)
            pr = jnp.exp2(s - m_new)
            l = jnp.where(keep, l_sc[u], 0.0) * corr + pr
            acc = jnp.where(keep, acc_sc[u], 0.0) * corr
            acc = acc + jnp.dot(pr.astype(jnp.bfloat16), kvs[ps[u], 1], preferred_element_type=jnp.float32)
            o = (acc / lanes(jnp.sum(l, axis=1, keepdims=True))).astype(jnp.bfloat16)
            for w in range(g):
                store(u, w, o[w * PC:(w + 1) * PC])


def _pair_scratch(g):
    f32 = jnp.float32
    return [pltpu.VMEM((2, KB, g * PC, PC), f32)] + [pltpu.VMEM((2, g * PC, DH), f32)] * 4


def _attend(n, g, scale, segs, kv, q_in, o_out, seg_s, seg_v, kvs, qs, os, lo_s, t_sc, mx_sc, m_sc, l_sc, acc_sc,
            seg_sem, kv_sem, q_sem, o_sem):
    pt = Place(n)
    last_piece = 2 * n - 1
    ng = q_in.shape[0]

    def load(p):
        owner = jnp.where(p < n, p, last_piece - p)
        return pltpu.make_async_copy(kv.at[owner, jnp.where(p < n, 0, 1)], kvs.at[p], kv_sem)

    seg_copies = [pltpu.make_async_copy(segs, seg_v, seg_sem.at[0]), pltpu.make_async_copy(segs, seg_s, seg_sem.at[1])]
    q_copies = [pltpu.make_async_copy(q_in.at[i, 1], qs.at[i], q_sem) for i in range(ng)]
    for cp in seg_copies + q_copies:
        cp.start()

    @pl.loop(0, 2 * n)
    def _(p):
        load(p).start()

    for cp in seg_copies:
        cp.wait()
    for i in range(ng):
        src = pt.dev((pt.x // 2) * 2 + i % 2, i // 2, pt.c)
        before = jnp.where(seg_v[...] < seg_s[src, 1, 0], 1.0, 0.0)
        lo_s[i] = jnp.sum(before).astype(jnp.int32) // PC
    for cp in q_copies:
        cp.wait()

    @pl.loop(0, 2 * n)
    def _(p):
        load(p).wait()

    def out(slot):
        return pltpu.make_async_copy(os.at[slot], o_out.at[slot], o_sem)

    pairs = Pairs(pt, n, g, scale, lambda src, half: seg_s[src, half, 0], seg_v, kvs,
                  lambda row, u: qs[2 * row + u].reshape(g * PC, DH), t_sc, mx_sc, m_sc, l_sc, acc_sc)

    def one(row, carry):
        def store(u, w, val):
            os[2 * row + u, :, w * DH:(w + 1) * DH] = val

        pairs(row, 1, lambda row: jnp.minimum(lo_s[2 * row], lo_s[2 * row + 1]), store)

        @pl.when(row > 0)
        def _():
            for u in range(2):
                out(2 * (row - 1) + u).start()

        return carry

    lax.fori_loop(0, ng // 2, one, 0)
    for u in range(2):
        out(ng - 2 + u).start()
    for i in range(ng):
        out(i).wait()


def _combine(n, g, scale, segs, kv, q_in, o_in, wo, y_ref, obuf, robuf, ol, wob, acc, seg_s, seg_v, kvs, qs,
             t_sc, mx_sc, m_sc, l_sc, acc_sc, w_sem, o_send, o_recv, ro_recv, ro_send, seg_sem, kv_sem, q_sem):
    pt = Place(n)
    me = pt.me
    gd = g * DH
    ng = q_in.shape[0]
    my_head, my_slot = pt.head(0, 0), pt.slot(0, 0)
    nc = 4
    wn = y_ref.shape[1] // nc
    lows, highs = pl.ds(0, PC), pl.ds(PC, PC)

    def load(p):
        return pltpu.make_async_copy(kv.at[p, 0], kvs.at[p], kv_sem.at[p])

    q_copies = [pltpu.make_async_copy(q_in.at[i, 0], qs.at[i], q_sem.at[i]) for i in range(ng)]
    seg_copies = [pltpu.make_async_copy(segs, seg_v, seg_sem.at[0]), pltpu.make_async_copy(segs, seg_s, seg_sem.at[1])]
    own = pltpu.make_async_copy(o_in.at[my_slot], obuf.at[my_head, highs], o_recv.at[1, my_head])
    for cp in seg_copies + q_copies + [own]:
        cp.start()

    @pl.loop(0, n)
    def _(p):
        load(p).start()

    def w_copies(t):
        for dx in range(2):
            h = pl.multiple_of(pt.head(dx, O_ORDER[t]) * gd, gd)
            yield pltpu.make_async_copy(wo.at[pl.ds(h, gd), :], wob.at[t, pl.ds(dx * gd, gd), :], w_sem.at[t, dx])

    for t in range(len(O_ORDER)):
        for cp in w_copies(t):
            cp.start()

    others = [(dx, dy) for dy in O_ORDER for dx in range(2) if (dx, dy) != (0, 0)]
    near = [s for s in others if s[1] != FAR]
    barrier = pltpu.get_barrier_semaphore()
    for dx, dy in others:
        pl.semaphore_signal(barrier, inc=1, device_id={"cp": pt.peer(dx, dy)}, device_id_type=MESH)
    pl.semaphore_wait(barrier, len(others))

    def put(src, dst, send, recv, dev):
        return pltpu.make_async_remote_copy(src, dst, send, recv, device_id={"cp": dev}, device_id_type=MESH)

    way = (1, -1)
    turn = {FAR: 0, 1: 1, 0: 2, -1: 3}

    def source(half, dx, dy):
        return o_in.at[pt.slot(dx, dy)] if half else ol.at[turn[dy], lax.rem(pt.x + dx, 2)]

    def o_copy(half, i):
        dx, dy = near[i]
        return put(source(half, dx, dy), obuf.at[my_head, highs if half else lows], o_send.at[half, i], o_recv.at[half, my_head],
                   pt.peer(dx, dy))

    def o_hop(half, dx):
        return put(source(half, dx, FAR), robuf.at[half, dx], o_send.at[half, len(near) + dx], ro_recv.at[half, dx],
                   pt.peer(0, way[half]))

    def o_hand(half, dx):
        head = pt.head(0, -way[half])
        return put(robuf.at[half, dx], obuf.at[head, highs if half else lows], ro_send.at[half, dx], o_recv.at[half, head],
                   pt.peer(dx, way[half]))

    def hand_on(half):
        for dx in range(2):
            put(robuf.at[half, dx], robuf.at[half, dx], o_send.at[0, 0], ro_recv.at[half, dx], me).wait_recv()
            o_hand(half, dx).start()

    for dx in range(2):
        o_hop(1, dx).start()
    for i in range(len(near)):
        o_copy(1, i).start()

    for cp in seg_copies + q_copies:
        cp.wait()

    @pl.loop(0, n)
    def _(p):
        load(p).wait()

    pairs = Pairs(pt, n, g, scale, lambda src, half: seg_s[src, half, 0], seg_v, kvs,
                  lambda row, u: qs[2 * row + u].reshape(g * PC, DH), t_sc, mx_sc, m_sc, l_sc, acc_sc)

    def send_low(dy):
        if dy == FAR:
            for dx in range(2):
                o_hop(0, dx).start()
        else:
            for i, (dx, to) in enumerate(near):
                if to == dy:
                    o_copy(0, i).start()

    def one(i, carry):
        row = lax.rem(pt.y + FAR - i + pt.side, pt.side)

        def store(u, w, val):
            ol[i, u, :, w * DH:(w + 1) * DH] = val

        pairs(row, 0, lambda row: 0, store)

        @pl.when(i == 1)
        def _():
            send_low(FAR)
            hand_on(1)

        @pl.when(i == 2)
        def _():
            send_low(1)

        @pl.when(i == 3)
        def _():
            send_low(0)
            hand_on(0)

        return carry

    lax.fori_loop(0, ng // 2, one, 0)
    obuf[my_head, 0:PC] = ol[turn[0], lax.rem(pt.x, 2)]
    send_low(-1)

    for t, dy in enumerate(O_ORDER):
        for cp in w_copies(t):
            cp.wait()
        heads = [pt.head(dx, dy) for dx in range(2)]
        for dx in range(2):
            if dy == 0 and dx == 0:
                own.wait()
            else:
                for half in range(2):
                    put(ol.at[0, 0], obuf.at[heads[dx], highs if half else lows], o_send.at[0, 0], o_recv.at[half, heads[dx]],
                        me).wait_recv()
        a = jnp.concatenate([obuf[heads[0]], obuf[heads[1]]], axis=1)
        for u in range(nc):
            r = jnp.dot(a, wob[t, :, u * wn:(u + 1) * wn], preferred_element_type=jnp.float32)
            if t > 0:
                r = r + acc[:, u * wn:(u + 1) * wn]
            if t < len(O_ORDER) - 1:
                acc[:, u * wn:(u + 1) * wn] = r
            else:
                y_ref[:, u * wn:(u + 1) * wn] = r.astype(y_ref.dtype)
    for half in range(2):
        for i in range(len(near)):
            o_copy(half, i).wait_send()
        for dx in range(2):
            o_hop(half, dx).wait_send()
            o_hand(half, dx).wait_send()


def solution(mesh):
    n = mesh.shape["cp"]
    side = math.isqrt(n // 2)
    bf, f32 = jnp.bfloat16, jnp.float32
    vmem, anym = pl.BlockSpec(memory_space=pltpu.VMEM), pl.BlockSpec(memory_space=pltpu.HBM)
    dma = pltpu.SemaphoreType.DMA

    def local(x, seg, wq, wk, wv, wo):
        lq, d = x.shape
        hkv = wk.shape[1] // DH
        g = wq.shape[1] // wk.shape[1]
        gd = g * DH
        ng = 2 * side
        kv, q, segs = pl.pallas_call(
            functools.partial(_project, n, g),
            out_shape=(jax.ShapeDtypeStruct((n, 2, 2, PC, DH), bf), jax.ShapeDtypeStruct((ng, 2, g, PC, DH), bf),
                       jax.ShapeDtypeStruct((n, 2, PC), jnp.int32)),
            in_specs=[vmem, vmem, anym, anym, anym],
            out_specs=(anym, anym, vmem),
            scratch_shapes=[
                pltpu.VMEM((2, side, d // side, hkv * DH), bf), pltpu.VMEM((side, d // side, hkv * gd), bf),
                pltpu.VMEM((2, lq, hkv * DH), f32), pltpu.VMEM((lq, hkv * gd), f32),
                pltpu.VMEM((n, 2, 2, PC, DH), bf), pltpu.VMEM((ng, 2, g, PC, DH), bf),
                pltpu.VMEM((ng, 2, 2, PC, DH), bf), pltpu.VMEM((ng, 2, g, PC, DH), bf),
                pltpu.VMEM((2, 2, 2, PC, DH), bf), pltpu.VMEM((2, 2, g, PC, DH), bf), pltpu.VMEM((n, 2, PC), jnp.int32),
                dma((2, side)), dma((side,)), dma((ng + 2,)), dma((n,)), dma((2, 2)), dma((2, 2)), dma((2, 2)),
                dma((ng,)), dma((2 * ng,)),
                dma((ng + 2,)), dma((ng,)), dma((2, 2)), dma((2, 2)), dma((2, 2)), dma((n,)), dma((n,)), dma((n,)), dma((ng,)),
            ],
            compiler_params=pltpu.CompilerParams(collective_id=0, has_side_effects=True, vmem_limit_bytes=60 << 20),
            name="project",
        )(x, seg.reshape(1, 2, PC), wk, wv, wq)
        scale = DH ** -0.5 * math.log2(math.e)
        o = pl.pallas_call(
            functools.partial(_attend, n, g, scale),
            out_shape=jax.ShapeDtypeStruct((ng, PC, gd), bf),
            in_specs=[anym] * 3,
            out_specs=anym,
            scratch_shapes=[pltpu.SMEM((n, 2, PC), jnp.int32), pltpu.VMEM((n, 2, PC), jnp.int32),
                            pltpu.VMEM((2 * n, 2, PC, DH), bf), pltpu.VMEM((ng, g, PC, DH), bf),
                            pltpu.VMEM((ng, PC, gd), bf), pltpu.SMEM((ng,), jnp.int32)] + _pair_scratch(g) + [dma((2,)), dma, dma, dma],
            compiler_params=pltpu.CompilerParams(vmem_limit_bytes=60 << 20),
            name="attend",
        )(segs, kv, q)
        return pl.pallas_call(
            functools.partial(_combine, n, g, scale),
            out_shape=jax.ShapeDtypeStruct((lq, wo.shape[1]), bf),
            in_specs=[anym] * 5,
            out_specs=vmem,
            scratch_shapes=[pltpu.VMEM((hkv, lq, gd), bf), pltpu.VMEM((2, 2, PC, gd), bf), pltpu.VMEM((ng // 2, 2, PC, gd), bf),
                            pltpu.VMEM((side, 2 * gd, wo.shape[1]), bf), pltpu.VMEM((lq, wo.shape[1]), f32),
                            pltpu.SMEM((n, 2, PC), jnp.int32), pltpu.VMEM((n, 2, PC), jnp.int32),
                            pltpu.VMEM((n, 2, PC, DH), bf), pltpu.VMEM((ng, g, PC, DH), bf)] + _pair_scratch(g) + [
                            dma((side, 2)), dma((2, ng)), dma((2, ng)), dma((2, 2)), dma((2, 2)), dma((2,)), dma((n,)), dma((ng,))],
            compiler_params=pltpu.CompilerParams(collective_id=1, has_side_effects=True, vmem_limit_bytes=60 << 20),
            name="combine",
        )(segs, kv, q, o, wo)

    rows = P(("dp", "cp"), None)
    return jax.shard_map(local, mesh=mesh, in_specs=(rows, P(("dp", "cp")), P(), P(), P(), P()), out_specs=rows, check_vma=False)
```

```python
import functools
import math

import jax
import jax.numpy as jnp
from jax import lax
from jax.experimental import pallas as pl
from jax.experimental.pallas import tpu as pltpu
from jax.sharding import PartitionSpec as P

DH = 128
PC = 128
KB = 4
MESH = pl.DeviceIdType.MESH
NEG_INF = float("-inf")
FLOOR = -3e38


class Place:
    def __init__(self, n):
        me = lax.axis_index("cp")
        self.n, self.side = n, math.isqrt(n // 2)
        self.me = me
        self.c = lax.rem(me, 2)
        chip = me // 2
        self.x = lax.rem(chip, self.side)
        self.y = chip // self.side
        self.xin = self.x + 1 - 2 * lax.rem(self.x, 2)
        self.xcross = self.side - 1 - self.x
        self.px = lax.rem(lax.rem(self.x, 2) + self.x // 2, 2)

    def dev(self, x, y, c):
        return (y * self.side + x) * 2 + c

    def row(self, dy):
        return lax.rem(self.y + dy + self.side, self.side)

    def col(self, dx):
        return self.xin if dx else self.x

    def peer(self, dx, dy):
        return self.dev(self.col(dx), self.row(dy), self.c)

    def head(self, dx, dy):
        return lax.rem(self.px + dx, 2) * self.side + self.row(dy)

    def slot(self, dx, dy):
        return self.row(dy) * 2 + lax.rem(self.x + dx, 2)


FAR = 2
KV_ORDER = (FAR, 0, 1, -1)
Q_ORDER = (FAR, 1, -1, 0)
O_ORDER = (0, 1, -1, FAR)


def _project(n, g, x_ref, seg_ref, wk, wv, wq, kv_o, q_o, segs_o, wkvb, wqb, kvacc, qacc, kvb, qb, skv, sq, rkv, rq, segb,
             wkv_sem, wq_sem, kv_send, kv_recv, kvf_recv, rkv_recv, rkv_send, fx_send, fs_send,
             q_send, q_recv, qf_recv, rq_recv, rq_send, seg_send, seg_recv, out_sem, qout_sem):
    pt = Place(n)
    me = pt.me
    kv_steps = [(t, dx, dy) for t, dy in enumerate(KV_ORDER) for dx in range(2)]
    q_steps = [(t, dx, dy) for t, dy in enumerate(Q_ORDER) for dx in range(2)]
    own_kv = (KV_ORDER.index(0), 0)
    own_q = (Q_ORDER.index(0), 0)
    gd = g * DH
    kr = wqb.shape[1]
    nk = wqb.shape[0]
    my_head, my_slot = pt.head(0, 0), pt.slot(0, 0)

    kv_copies = [[pltpu.make_async_copy(w.at[pl.ds(t * kr, kr)], wkvb.at[i, t], wkv_sem.at[i, t]) for i, w in enumerate((wk, wv))]
                 for t in range(nk)]
    q_copies = [pltpu.make_async_copy(wq.at[pl.ds(t * kr, kr)], wqb.at[t], wq_sem.at[t]) for t in range(nk)]
    for cps in kv_copies:
        for cp in cps:
            cp.start()
    for cp in q_copies:
        cp.start()

    barrier = pltpu.get_barrier_semaphore()

    @pl.loop(1, n)
    def _(i):
        pl.semaphore_signal(barrier, inc=1, device_id={"cp": lax.rem(me + i, n)}, device_id_type=MESH)

    def seg_copy(i):
        return pltpu.make_async_remote_copy(seg_ref, segb.at[pl.ds(me, 1)], seg_send.at[i], seg_recv.at[me],
                                            device_id={"cp": lax.rem(me + i, n)}, device_id_type=MESH)

    segb[pl.ds(me, 1)] = seg_ref[...]

    def put(src, dst, send, recv, dev):
        return pltpu.make_async_remote_copy(src, dst, send, recv, device_id={"cp": dev}, device_id_type=MESH)

    def kv_copy(t, dx, dy):
        return put(skv.at[pt.head(dx, dy)], kvb.at[me], kv_send.at[2 * t + dx], kv_recv.at[me], pt.peer(dx, dy))

    def q_copy(t, dx, dy):
        return put(sq.at[pt.head(dx, dy)], qb.at[my_slot], q_send.at[2 * t + dx], q_recv.at[my_slot], pt.peer(dx, dy))

    way = (1, -1)
    hops = [(half, dx) for half in range(2) for dx in range(2)]

    def kv_hop(half, dx):
        return put(skv.at[pt.head(dx, FAR), half], rkv.at[half, dx], kv_send.at[2 * half + dx if half == 0 else 2 * len(KV_ORDER) + dx],
                   rkv_recv.at[half, dx], pt.peer(0, way[half]))

    def kv_hand(half, dx):
        return put(rkv.at[half, dx], kvb.at[pt.peer(0, -way[half]), half], rkv_send.at[half, dx], kvf_recv.at[dx, half],
                   pt.peer(dx, way[half]))

    def q_hop(half, dx):
        return put(sq.at[pt.head(dx, FAR), half], rq.at[half, dx], q_send.at[2 * half + dx if half == 0 else 2 * len(Q_ORDER) + dx],
                   rq_recv.at[half, dx], pt.peer(0, way[half]))

    def q_hand(half, dx):
        return put(rq.at[half, dx], qb.at[pt.slot(0, -way[half]), half], rq_send.at[half, dx], qf_recv.at[dx, half],
                   pt.peer(dx, way[half]))

    nb = 4 * DH

    def summed(t, w, acc, c):
        cols = slice(c * nb, (c + 1) * nb)
        r = jnp.dot(x_ref[:, t * kr:(t + 1) * kr], w[:, cols], preferred_element_type=jnp.float32)
        if t > 0:
            r = r + acc[:, cols]
        if t < nk - 1:
            acc[:, cols] = r
        return r

    def kv_step(t):
        for cp in kv_copies[t]:
            cp.wait()
        for c in range(wkvb.shape[3] // nb):
            for i in range(2):
                r = summed(t, wkvb.at[i, t], kvacc.at[i], c)
                if t == nk - 1:
                    for u in range(nb // DH):
                        part = r[:, u * DH:(u + 1) * DH]
                        part = (jnp.transpose(part) if i == 1 else part).astype(jnp.bfloat16)
                        for half in range(2):
                            rows = slice(half * PC, (half + 1) * PC)
                            skv[c * (nb // DH) + u, half, i] = part[:, rows] if i == 1 else part[rows]

    def q_step(t, first, last):
        if first == 0:
            q_copies[t].wait()
        for c in range(first, last):
            r = summed(t, wqb.at[t], qacc, c)
            if t == nk - 1:
                for u in range(nb // DH):
                    col = c * (nb // DH) + u
                    part = jnp.transpose(r[:, u * DH:(u + 1) * DH]).astype(jnp.bfloat16)
                    for half in range(2):
                        sq[col // g, half, col % g] = part[:, half * PC:(half + 1) * PC]

    def send_kv(t):
        if KV_ORDER[t] == FAR:
            for hop in hops:
                kv_hop(*hop).start()
        else:
            for dx in range(2):
                if (t, dx) != own_kv:
                    kv_copy(t, dx, KV_ORDER[t]).start()

    def send_q(t):
        if Q_ORDER[t] == FAR:
            for hop in hops:
                q_hop(*hop).start()
        else:
            for dx in range(2):
                if (t, dx) != own_q:
                    q_copy(t, dx, Q_ORDER[t]).start()

    def to_cross(src, i):
        return put(kvb.at[src], kvb.at[src], fx_send.at[i], kv_recv.at[src], pt.dev(pt.xcross, pt.y, pt.c))

    def to_sibling(src, i):
        return put(kvb.at[src], kvb.at[src], fs_send.at[i], kv_recv.at[src], pt.dev(pt.x, pt.y, 1 - pt.c))

    def kv_out(src):
        return pltpu.make_async_copy(kvb.at[src], kv_o.at[src], out_sem.at[src])

    def q_out(slot):
        return pltpu.make_async_copy(qb.at[slot], q_o.at[slot], qout_sem.at[slot])

    def arrived(src):
        to_sibling(src, 0).wait_recv()

    def forward(t):
        dy = KV_ORDER[t]
        for dx in range(2):
            src = pt.peer(dx, -dy)
            if dy == FAR:
                for half in range(2):
                    put(rkv.at[half, dx], kvb.at[src, half], rkv_send.at[half, dx], kvf_recv.at[dx, half], me).wait_recv()
            elif (t, dx) != own_kv:
                arrived(src)
            to_cross(src, 2 * t + dx).start()
            to_sibling(src, 2 * t + dx).start()
            kv_out(src).start()

    def own_out():
        return pltpu.make_async_copy(skv.at[my_head], kv_o.at[me], out_sem.at[me])

    def own_q_out():
        return pltpu.make_async_copy(sq.at[my_head], q_o.at[my_slot], qout_sem.at[my_slot])

    def forward_own():
        put(skv.at[my_head], kvb.at[me], fx_send.at[2 * own_kv[0]], kv_recv.at[me], pt.dev(pt.xcross, pt.y, pt.c)).start()
        put(skv.at[my_head], kvb.at[me], fs_send.at[2 * own_kv[0]], kv_recv.at[me], pt.dev(pt.x, pt.y, 1 - pt.c)).start()
        own_out().start()

    def forward_next():
        src = pt.peer(1, 0)
        arrived(src)
        to_cross(src, 2 * own_kv[0] + 1).start()
        to_sibling(src, 2 * own_kv[0] + 1).start()
        kv_out(src).start()

    for t in range(nk):
        kv_step(t)
    nq = wqb.shape[2] // nb
    q_step(0, 0, 1)

    pl.semaphore_wait(barrier, n - 1)
    for t in range(len(KV_ORDER)):
        send_kv(t)
    forward_own()
    q_step(0, 1, nq)
    q_step(1, 0, nq)
    q_step(2, 0, nq)
    forward_next()
    for hop in hops:
        put(rkv.at[hop], rkv.at[hop], kv_send.at[0], rkv_recv.at[hop], me).wait_recv()
        kv_hand(*hop).start()
    q_step(3, 0, nq)
    forward(2)
    for t in range(len(Q_ORDER)):
        send_q(t)
    own_q_out().start()
    forward(3)
    forward(0)

    @pl.loop(1, n)
    def _(i):
        seg_copy(i).start()


    def mirrored(dx, dy, c):
        x = pt.side - 1 - pt.col(dx)
        return pt.dev(x, pt.row(-dy), c)

    passing = [(t, dx, KV_ORDER[t]) for t in (1, 2, 3, 0) for dx in range(2)]

    def pass_on(steps):
        for t, dx, dy in steps:
            src = mirrored(dx, dy, pt.c)
            arrived(src)
            to_sibling(src, 8 + 2 * t + dx).start()
            kv_out(src).start()

    pass_on(passing[:2])
    for hop in hops:
        put(rq.at[hop], rq.at[hop], q_send.at[0], rq_recv.at[hop], me).wait_recv()
        q_hand(*hop).start()
    pass_on(passing[2:])

    for t, dx, dy in passing:
        src = pt.dev(pt.col(dx), pt.row(-dy), 1 - pt.c)
        arrived(src)
        kv_out(src).start()
    for t, dx, dy in q_steps:
        slot = pt.slot(dx, -dy)
        if dy == FAR:
            for half in range(2):
                put(rq.at[half, dx], qb.at[slot, half], rq_send.at[half, dx], qf_recv.at[dx, half], me).wait_recv()
        elif (t, dx) != own_q:
            put(qb.at[slot], qb.at[slot], q_send.at[0], q_recv.at[slot], me).wait_recv()
        if (t, dx) != own_q:
            q_out(slot).start()
    for t, dx, dy in passing:
        src = mirrored(dx, dy, 1 - pt.c)
        arrived(src)
        kv_out(src).start()

    @pl.loop(1, n)
    def _(i):
        src = lax.rem(me + i, n)
        pltpu.make_async_remote_copy(seg_ref, segb.at[pl.ds(src, 1)], seg_send.at[i], seg_recv.at[src],
                                     device_id={"cp": src}, device_id_type=MESH).wait_recv()

    segs_o[...] = segb[...]

    @pl.loop(1, n)
    def _(i):
        seg_copy(i).wait_send()

    for hop in hops:
        kv_hop(*hop).wait_send()
        kv_hand(*hop).wait_send()
        q_hop(*hop).wait_send()
        q_hand(*hop).wait_send()
    for t, dx, dy in kv_steps:
        if dy != FAR and (t, dx) != own_kv:
            kv_copy(t, dx, dy).wait_send()
        src = pt.peer(dx, -dy)
        to_cross(src, 2 * t + dx).wait_send()
        to_sibling(src, 2 * t + dx).wait_send()
        to_sibling(src, 8 + 2 * t + dx).wait_send()
    for t, dx, dy in q_steps:
        if dy != FAR and (t, dx) != own_q:
            q_copy(t, dx, dy).wait_send()

    @pl.loop(0, n)
    def _(i):
        kv_out(i).wait()

    @pl.loop(0, n // 4)
    def _(i):
        q_out(i).wait()


class Pairs:
    def __init__(self, pt, n, g, scale, first_of, seg_v, kvs, qs, t_sc, acc_sc):
        self.pt, self.n, self.g, self.scale, self.first_of, self.seg_v, self.kvs = pt, n, g, scale, first_of, seg_v, kvs
        self.qs, self.t_sc, self.acc_sc = qs, t_sc, acc_sc

    def begins(self, row, half):
        out = []
        for u in range(2):
            src = self.pt.dev((self.pt.x // 2) * 2 + u, row, self.pt.c)
            before = jnp.where(self.seg_v[...] < self.first_of(src, half), 1.0, 0.0)
            out.append(jnp.sum(before).astype(jnp.int32))
        return out

    def __call__(self, row, half, lo, begins, store):
        pt, n, g, scale, seg_v, kvs, qs = self.pt, self.n, self.g, self.scale, self.seg_v, self.kvs, self.qs
        t_sc, acc_sc = self.t_sc, self.acc_sc
        last_piece, pieces = 2 * n - 1, kvs.shape[0]
        srcs = [pt.dev((pt.x // 2) * 2 + u, row, pt.c) for u in range(2)]
        ps = [last_piece - src if half else src for src in srcs]
        end = jnp.maximum(ps[0], ps[1])
        wide = g * PC
        acc_sc[...] = jnp.zeros_like(acc_sc)

        def queries(us):
            return jnp.concatenate([qs[2 * row + u, w] for u in us for w in range(g)], axis=1)

        def start(b):
            return jnp.minimum(lo + b * KB, pieces - KB)

        def scores(b):
            j0, js = lo + b * KB, start(b)
            k = jnp.concatenate([kvs[js + w, 0] for w in range(KB)], axis=0)
            s = jnp.dot(k, queries((0, 1)), preferred_element_type=jnp.float32) * scale
            pos = lax.broadcasted_iota(jnp.int32, (KB * PC, DH), 0) + js * PC
            tops = []
            for u in range(2):
                seen = (pos >= jnp.maximum(begins[u], j0 * PC)) & (pos < ps[u] * PC)
                for w in range(g):
                    at = slice(u * wide + w * PC, u * wide + (w + 1) * PC)
                    part = jnp.where(seen, s[:, at], NEG_INF)
                    t_sc[:, at] = part
                    tops.append(jnp.max(part, axis=0, keepdims=True))
            return jnp.concatenate(tops, axis=1)

        def step(b, carry):
            m, l, top = carry
            js = start(b)
            m_new = jnp.maximum(m, top)
            corr = jnp.exp2(m - m_new)
            p = jnp.exp2(t_sc[...] - m_new)
            l = l * corr + jnp.sum(p, axis=0, keepdims=True)
            vt = jnp.concatenate([kvs[js + w, 1] for w in range(KB)], axis=1)
            acc_sc[...] = acc_sc[...] * corr + jnp.dot(vt, p.astype(jnp.bfloat16), preferred_element_type=jnp.float32)
            return m_new, l, scores(b + 1)

        line = jnp.zeros((1, 2 * wide), jnp.float32)
        m, l, _ = lax.fori_loop(0, lax.div(end - lo + KB - 1, KB), step, (line + FLOOR, line, scores(0)))

        key = lax.broadcasted_iota(jnp.int32, (PC, PC), 0)
        query = lax.broadcasted_iota(jnp.int32, (PC, PC), 1)
        ss = [jnp.dot(kvs[ps[u], 0], queries((u,)), preferred_element_type=jnp.float32) * scale for u in range(2)]
        for u in range(2):
            at = slice(u * wide, (u + 1) * wide)
            ids = seg_v[srcs[u], pl.ds(half, 1), :]
            idb = jnp.broadcast_to(ids, (PC, PC))
            allowed = jnp.concatenate([(idb == jnp.transpose(idb)) & (key <= query)] * g, axis=1)
            keep = jnp.concatenate([ids == self.first_of(srcs[u], half)] * g, axis=1)
            s = jnp.where(allowed, ss[u], NEG_INF)
            m_old = jnp.where(keep, m[:, at], FLOOR)
            m_new = jnp.maximum(m_old, jnp.max(s, axis=0, keepdims=True))
            corr = jnp.where(keep, jnp.exp2(m_old - m_new), 0.0)
            p = jnp.exp2(s - m_new)
            ll = l[:, at] * corr + jnp.sum(p, axis=0, keepdims=True)
            acc = acc_sc[:, at] * corr + jnp.dot(kvs[ps[u], 1], p.astype(jnp.bfloat16), preferred_element_type=jnp.float32)
            o = acc * (1.0 / ll)
            for w in range(g):
                store(u, w, jnp.transpose(o[:, w * PC:(w + 1) * PC]).astype(jnp.bfloat16))


def _pair_scratch(g):
    f32 = jnp.float32
    return [pltpu.VMEM((KB * PC, 2 * g * PC), f32), pltpu.VMEM((DH, 2 * g * PC), f32)]


def _attend(n, g, scale, segs, kv, q_in, o_out, seg_s, seg_v, kvs, qs, os, lo_s, t_sc, acc_sc,
            seg_sem, kv_sem, q_sem, o_sem):
    pt = Place(n)
    last_piece = 2 * n - 1
    ng = q_in.shape[0]

    def load(p):
        owner = jnp.where(p < n, p, last_piece - p)
        return pltpu.make_async_copy(kv.at[owner, jnp.where(p < n, 0, 1)], kvs.at[p], kv_sem)

    seg_copies = [pltpu.make_async_copy(segs, seg_v, seg_sem.at[0]), pltpu.make_async_copy(segs, seg_s, seg_sem.at[1])]
    q_copies = [pltpu.make_async_copy(q_in.at[i, 1], qs.at[i], q_sem) for i in range(ng)]
    for cp in seg_copies + q_copies:
        cp.start()

    @pl.loop(0, 2 * n)
    def _(p):
        load(p).start()

    for cp in seg_copies:
        cp.wait()
    pairs = Pairs(pt, n, g, scale, lambda src, half: seg_s[src, half, 0], seg_v, kvs, qs, t_sc, acc_sc)
    for i in range(ng // 2):
        for u, at in enumerate(pairs.begins(i, 1)):
            lo_s[2 * i + u] = at
    for cp in q_copies:
        cp.wait()

    @pl.loop(0, 2 * n)
    def _(p):
        load(p).wait()

    def out(slot):
        return pltpu.make_async_copy(os.at[slot], o_out.at[slot], o_sem)

    def one(row, carry):
        def store(u, w, val):
            os[2 * row + u, :, w * DH:(w + 1) * DH] = val

        begins = [lo_s[2 * row + u] for u in range(2)]
        pairs(row, 1, lax.div(jnp.minimum(*begins), PC), begins, store)

        @pl.when(row > 0)
        def _():
            for u in range(2):
                out(2 * (row - 1) + u).start()

        return carry

    lax.fori_loop(0, ng // 2, one, 0)
    for u in range(2):
        out(ng - 2 + u).start()
    for i in range(ng):
        out(i).wait()


def _combine(n, g, scale, segs, kv, q_in, o_in, wo, y_ref, obuf, robuf, ol, wob, acc, seg_s, seg_v, kvs, qs,
             t_sc, acc_sc, w_sem, o_send, o_recv, ro_recv, ro_send, seg_sem, kv_sem, q_sem):
    pt = Place(n)
    me = pt.me
    gd = g * DH
    ng = q_in.shape[0]
    my_head, my_slot = pt.head(0, 0), pt.slot(0, 0)
    nc = 4
    wn = y_ref.shape[1] // nc
    lows, highs = pl.ds(0, PC), pl.ds(PC, PC)

    def load(p):
        return pltpu.make_async_copy(kv.at[p, 0], kvs.at[p], kv_sem.at[p])

    q_copies = [pltpu.make_async_copy(q_in.at[i, 0], qs.at[i], q_sem.at[i]) for i in range(ng)]
    seg_copies = [pltpu.make_async_copy(segs, seg_v, seg_sem.at[0]), pltpu.make_async_copy(segs, seg_s, seg_sem.at[1])]
    own = pltpu.make_async_copy(o_in.at[my_slot], obuf.at[my_head, highs], o_recv.at[1, my_head])
    for cp in seg_copies + q_copies + [own]:
        cp.start()

    @pl.loop(0, n)
    def _(p):
        load(p).start()

    def w_copies(t):
        for dx in range(2):
            h = pl.multiple_of(pt.head(dx, O_ORDER[t]) * gd, gd)
            yield pltpu.make_async_copy(wo.at[pl.ds(h, gd), :], wob.at[t, pl.ds(dx * gd, gd), :], w_sem.at[t, dx])

    for t in range(len(O_ORDER)):
        for cp in w_copies(t):
            cp.start()

    others = [(dx, dy) for dy in O_ORDER for dx in range(2) if (dx, dy) != (0, 0)]
    near = [s for s in others if s[1] != FAR]
    barrier = pltpu.get_barrier_semaphore()
    for dx, dy in others:
        pl.semaphore_signal(barrier, inc=1, device_id={"cp": pt.peer(dx, dy)}, device_id_type=MESH)
    pl.semaphore_wait(barrier, len(others))

    def put(src, dst, send, recv, dev):
        return pltpu.make_async_remote_copy(src, dst, send, recv, device_id={"cp": dev}, device_id_type=MESH)

    way = (1, -1)
    turn = {FAR: 0, 1: 1, 0: 2, -1: 3}

    def source(half, dx, dy):
        return o_in.at[pt.slot(dx, dy)] if half else ol.at[turn[dy], lax.rem(pt.x + dx, 2)]

    def o_copy(half, i):
        dx, dy = near[i]
        return put(source(half, dx, dy), obuf.at[my_head, highs if half else lows], o_send.at[half, i], o_recv.at[half, my_head],
                   pt.peer(dx, dy))

    def o_hop(half, dx):
        return put(source(half, dx, FAR), robuf.at[half, dx], o_send.at[half, len(near) + dx], ro_recv.at[half, dx],
                   pt.peer(0, way[half]))

    def o_hand(half, dx):
        head = pt.head(0, -way[half])
        return put(robuf.at[half, dx], obuf.at[head, highs if half else lows], ro_send.at[half, dx], o_recv.at[half, head],
                   pt.peer(dx, way[half]))

    def hand_on(half):
        for dx in range(2):
            put(robuf.at[half, dx], robuf.at[half, dx], o_send.at[0, 0], ro_recv.at[half, dx], me).wait_recv()
            o_hand(half, dx).start()

    for dx in range(2):
        o_hop(1, dx).start()
    for i in range(len(near)):
        o_copy(1, i).start()

    for cp in seg_copies + q_copies:
        cp.wait()

    @pl.loop(0, n)
    def _(p):
        load(p).wait()

    pairs = Pairs(pt, n, g, scale, lambda src, half: seg_s[src, half, 0], seg_v, kvs, qs, t_sc, acc_sc)

    def send_low(dy):
        if dy == FAR:
            for dx in range(2):
                o_hop(0, dx).start()
        else:
            for i, (dx, to) in enumerate(near):
                if to == dy:
                    o_copy(0, i).start()

    def one(i, carry):
        row = lax.rem(pt.y + FAR - i + pt.side, pt.side)

        def store(u, w, val):
            ol[i, u, :, w * DH:(w + 1) * DH] = val

        pairs(row, 0, 0, pairs.begins(row, 0), store)

        @pl.when(i == 1)
        def _():
            send_low(FAR)
            hand_on(1)

        @pl.when(i == 2)
        def _():
            send_low(1)

        @pl.when(i == 3)
        def _():
            send_low(0)
            hand_on(0)

        return carry

    lax.fori_loop(0, ng // 2, one, 0)
    obuf[my_head, 0:PC] = ol[turn[0], lax.rem(pt.x, 2)]
    send_low(-1)

    for t, dy in enumerate(O_ORDER):
        for cp in w_copies(t):
            cp.wait()
        heads = [pt.head(dx, dy) for dx in range(2)]
        for dx in range(2):
            if dy == 0 and dx == 0:
                own.wait()
            else:
                for half in range(2):
                    put(ol.at[0, 0], obuf.at[heads[dx], highs if half else lows], o_send.at[0, 0], o_recv.at[half, heads[dx]],
                        me).wait_recv()
        a = jnp.concatenate([obuf[heads[0]], obuf[heads[1]]], axis=1)
        for u in range(nc):
            r = jnp.dot(a, wob[t, :, u * wn:(u + 1) * wn], preferred_element_type=jnp.float32)
            if t > 0:
                r = r + acc[:, u * wn:(u + 1) * wn]
            if t < len(O_ORDER) - 1:
                acc[:, u * wn:(u + 1) * wn] = r
            else:
                y_ref[:, u * wn:(u + 1) * wn] = r.astype(y_ref.dtype)
    for half in range(2):
        for i in range(len(near)):
            o_copy(half, i).wait_send()
        for dx in range(2):
            o_hop(half, dx).wait_send()
            o_hand(half, dx).wait_send()


def solution(mesh):
    n = mesh.shape["cp"]
    side = math.isqrt(n // 2)
    bf, f32 = jnp.bfloat16, jnp.float32
    vmem, anym = pl.BlockSpec(memory_space=pltpu.VMEM), pl.BlockSpec(memory_space=pltpu.HBM)
    dma = pltpu.SemaphoreType.DMA

    def local(x, seg, wq, wk, wv, wo):
        lq, d = x.shape
        hkv = wk.shape[1] // DH
        g = wq.shape[1] // wk.shape[1]
        gd = g * DH
        ng = 2 * side
        kv, q, segs = pl.pallas_call(
            functools.partial(_project, n, g),
            out_shape=(jax.ShapeDtypeStruct((n, 2, 2, PC, DH), bf), jax.ShapeDtypeStruct((ng, 2, g, PC, DH), bf),
                       jax.ShapeDtypeStruct((n, 2, PC), jnp.int32)),
            in_specs=[vmem, vmem, anym, anym, anym],
            out_specs=(anym, anym, vmem),
            scratch_shapes=[
                pltpu.VMEM((2, side, d // side, hkv * DH), bf), pltpu.VMEM((side, d // side, hkv * gd), bf),
                pltpu.VMEM((2, lq, hkv * DH), f32), pltpu.VMEM((lq, hkv * gd), f32),
                pltpu.VMEM((n, 2, 2, PC, DH), bf), pltpu.VMEM((ng, 2, g, PC, DH), bf),
                pltpu.VMEM((ng, 2, 2, PC, DH), bf), pltpu.VMEM((ng, 2, g, PC, DH), bf),
                pltpu.VMEM((2, 2, 2, PC, DH), bf), pltpu.VMEM((2, 2, g, PC, DH), bf), pltpu.VMEM((n, 2, PC), jnp.int32),
                dma((2, side)), dma((side,)), dma((ng + 2,)), dma((n,)), dma((2, 2)), dma((2, 2)), dma((2, 2)),
                dma((ng,)), dma((2 * ng,)),
                dma((ng + 2,)), dma((ng,)), dma((2, 2)), dma((2, 2)), dma((2, 2)), dma((n,)), dma((n,)), dma((n,)), dma((ng,)),
            ],
            compiler_params=pltpu.CompilerParams(collective_id=0, has_side_effects=True, vmem_limit_bytes=60 << 20),
            name="project",
        )(x, seg.reshape(1, 2, PC), wk, wv, wq)
        scale = DH ** -0.5 * math.log2(math.e)
        o = pl.pallas_call(
            functools.partial(_attend, n, g, scale),
            out_shape=jax.ShapeDtypeStruct((ng, PC, gd), bf),
            in_specs=[anym] * 3,
            out_specs=anym,
            scratch_shapes=[pltpu.SMEM((n, 2, PC), jnp.int32), pltpu.VMEM((n, 2, PC), jnp.int32),
                            pltpu.VMEM((2 * n, 2, PC, DH), bf), pltpu.VMEM((ng, g, PC, DH), bf),
                            pltpu.VMEM((ng, PC, gd), bf), pltpu.SMEM((ng,), jnp.int32)] + _pair_scratch(g) + [dma((2,)), dma, dma, dma],
            compiler_params=pltpu.CompilerParams(vmem_limit_bytes=60 << 20),
            name="attend",
        )(segs, kv, q)
        return pl.pallas_call(
            functools.partial(_combine, n, g, scale),
            out_shape=jax.ShapeDtypeStruct((lq, wo.shape[1]), bf),
            in_specs=[anym] * 5,
            out_specs=vmem,
            scratch_shapes=[pltpu.VMEM((hkv, lq, gd), bf), pltpu.VMEM((2, 2, PC, gd), bf), pltpu.VMEM((ng // 2, 2, PC, gd), bf),
                            pltpu.VMEM((side, 2 * gd, wo.shape[1]), bf), pltpu.VMEM((lq, wo.shape[1]), f32),
                            pltpu.SMEM((n, 2, PC), jnp.int32), pltpu.VMEM((n, 2, PC), jnp.int32),
                            pltpu.VMEM((n, 2, PC, DH), bf), pltpu.VMEM((ng, g, PC, DH), bf)] + _pair_scratch(g) + [
                            dma((side, 2)), dma((2, ng)), dma((2, ng)), dma((2, 2)), dma((2, 2)), dma((2,)), dma((n,)), dma((ng,))],
            compiler_params=pltpu.CompilerParams(collective_id=1, has_side_effects=True, vmem_limit_bytes=60 << 20),
            name="combine",
        )(segs, kv, q, o, wo)

    rows = P(("dp", "cp"), None)
    return jax.shard_map(local, mesh=mesh, in_specs=(rows, P(("dp", "cp")), P(), P(), P(), P()), out_specs=rows, check_vma=False)
```

```python
import functools
import math

import jax
import jax.numpy as jnp
from jax import lax
from jax.experimental import pallas as pl
from jax.experimental.pallas import tpu as pltpu
from jax.sharding import PartitionSpec as P

DH = 128
PC = 128
KB = 4
MESH = pl.DeviceIdType.MESH
NEG_INF = float("-inf")
FLOOR = -3e38


class Place:
    def __init__(self, n):
        me = lax.axis_index("cp")
        self.n, self.side = n, math.isqrt(n // 2)
        self.me = me
        self.c = lax.rem(me, 2)
        chip = me // 2
        self.x = lax.rem(chip, self.side)
        self.y = chip // self.side
        self.xin = self.x + 1 - 2 * lax.rem(self.x, 2)
        self.xcross = self.side - 1 - self.x
        self.px = lax.rem(lax.rem(self.x, 2) + self.x // 2, 2)

    def dev(self, x, y, c):
        return (y * self.side + x) * 2 + c

    def row(self, dy):
        return lax.rem(self.y + dy + self.side, self.side)

    def col(self, dx):
        return self.xin if dx else self.x

    def peer(self, dx, dy):
        return self.dev(self.col(dx), self.row(dy), self.c)

    def head(self, dx, dy):
        return lax.rem(self.px + dx, 2) * self.side + self.row(dy)

    def slot(self, dx, dy):
        return self.row(dy) * 2 + lax.rem(self.x + dx, 2)


class Pairs:
    def __init__(self, pt, n, g, scale, first_of, seg_v, pieces, kv, q, t_sc, acc_sc):
        self.pt, self.n, self.g, self.scale, self.first_of, self.seg_v = pt, n, g, scale, first_of, seg_v
        self.pieces, self.kv, self.q, self.t_sc, self.acc_sc = pieces, kv, q, t_sc, acc_sc

    def begins(self, row, half):
        out = []
        for u in range(2):
            src = self.pt.dev((self.pt.x // 2) * 2 + u, row, self.pt.c)
            before = jnp.where(self.seg_v[...] < self.first_of(src, half), 1.0, 0.0)
            out.append(jnp.sum(before).astype(jnp.int32))
        return out

    def __call__(self, row, half, lo, begins, store):
        pt, n, g, scale, seg_v, kv = self.pt, self.n, self.g, self.scale, self.seg_v, self.kv
        t_sc, acc_sc = self.t_sc, self.acc_sc
        last_piece, pieces = 2 * n - 1, self.pieces
        srcs = [pt.dev((pt.x // 2) * 2 + u, row, pt.c) for u in range(2)]
        ps = [last_piece - src if half else src for src in srcs]
        end = jnp.maximum(ps[0], ps[1])
        wide = g * PC
        acc_sc[...] = jnp.zeros_like(acc_sc)

        def queries(us):
            return jnp.concatenate([self.q(row, u, w) for u in us for w in range(g)], axis=1)

        def start(b):
            return jnp.minimum(lo + b * KB, pieces - KB)

        def scores(b):
            j0, js = lo + b * KB, start(b)
            k = jnp.concatenate([kv(js + w, 0) for w in range(KB)], axis=0)
            s = jnp.dot(k, queries((0, 1)), preferred_element_type=jnp.float32)
            pos = lax.broadcasted_iota(jnp.int32, (KB * PC, DH), 0) + js * PC
            tops = []
            for u in range(2):
                seen = (pos >= jnp.maximum(begins[u], j0 * PC)) & (pos < ps[u] * PC)
                for w in range(g):
                    at = slice(u * wide + w * PC, u * wide + (w + 1) * PC)
                    part = jnp.where(seen, s[:, at], NEG_INF)
                    t_sc[:, at] = part
                    tops.append(jnp.max(part, axis=0, keepdims=True))
            return jnp.concatenate(tops, axis=1)

        def step(b, carry):
            m, l, top = carry
            js = start(b)
            m_new = jnp.maximum(m, top)
            corr = jnp.exp2((m - m_new) * scale)
            p = jnp.exp2((t_sc[...] - m_new) * scale)
            l = l * corr + jnp.sum(p, axis=0, keepdims=True)
            vt = jnp.concatenate([kv(js + w, 1) for w in range(KB)], axis=1)
            acc_sc[...] = acc_sc[...] * corr + jnp.dot(vt, p.astype(jnp.bfloat16), preferred_element_type=jnp.float32)
            return m_new, l, scores(b + 1)

        line = jnp.zeros((1, 2 * wide), jnp.float32)
        m, l, _ = lax.fori_loop(0, lax.div(end - lo + KB - 1, KB), step, (line + FLOOR, line, scores(0)))

        key = lax.broadcasted_iota(jnp.int32, (PC, PC), 0)
        query = lax.broadcasted_iota(jnp.int32, (PC, PC), 1)
        ss = [jnp.dot(kv(ps[u], 0), queries((u,)), preferred_element_type=jnp.float32) for u in range(2)]
        for u in range(2):
            at = slice(u * wide, (u + 1) * wide)
            ids = seg_v[srcs[u], pl.ds(half, 1), :]
            idb = jnp.broadcast_to(ids, (PC, PC))
            allowed = jnp.concatenate([(idb == jnp.transpose(idb)) & (key <= query)] * g, axis=1)
            keep = jnp.concatenate([ids == self.first_of(srcs[u], half)] * g, axis=1)
            s = jnp.where(allowed, ss[u], NEG_INF)
            m_old = jnp.where(keep, m[:, at], FLOOR)
            m_new = jnp.maximum(m_old, jnp.max(s, axis=0, keepdims=True))
            corr = jnp.where(keep, jnp.exp2((m_old - m_new) * scale), 0.0)
            p = jnp.exp2((s - m_new) * scale)
            ll = l[:, at] * corr + jnp.sum(p, axis=0, keepdims=True)
            acc = acc_sc[:, at] * corr + jnp.dot(kv(ps[u], 1), p.astype(jnp.bfloat16), preferred_element_type=jnp.float32)
            o = acc * (1.0 / ll)
            for w in range(g):
                store(u, w, jnp.transpose(o[:, w * PC:(w + 1) * PC]).astype(jnp.bfloat16))


def _pair_scratch(g):
    f32 = jnp.float32
    return [pltpu.VMEM((KB * PC, 2 * g * PC), f32), pltpu.VMEM((DH, 2 * g * PC), f32)]


FAR = 2
KV_ORDER = (FAR, 0, 1, -1)
Q_ORDER = (FAR, 1, -1, 0)
O_ORDER = (0, 1, -1, FAR)


def _project(n, g, scale, x_ref, seg_in, wk, wv, wq, kv_o, q_o, segs_o, o_o, wkvb, wqb, kvacc, qacc, kvb, qb, skv, sq, rkv, rq,
             segb, seg_s, ol, t_sc, acc_sc, wkv_sem, wq_sem, kv_send, kv_recv, rkv_recv, rkv_send, fx_send, fs_send,
             q_send, q_recv, rq_recv, rq_send, seg_send, seg_recv, seg_sem, out_sem, qout_sem, o_sem):
    pt = Place(n)
    me = pt.me
    ng = qb.shape[0]
    kv_steps = [(t, dx, dy) for t, dy in enumerate(KV_ORDER) for dx in range(2)]
    q_steps = [(t, dx, dy) for t, dy in enumerate(Q_ORDER) for dx in range(2)]
    own_kv = (KV_ORDER.index(0), 0)
    own_q = (Q_ORDER.index(0), 0)
    gd = g * DH
    kr = wqb.shape[1]
    nk = wqb.shape[0]
    my_head, my_slot = pt.head(0, 0), pt.slot(0, 0)

    kv_copies = [[pltpu.make_async_copy(w.at[pl.ds(t * kr, kr)], wkvb.at[i, t], wkv_sem.at[i, t]) for i, w in enumerate((wk, wv))]
                 for t in range(nk)]
    q_copies = [pltpu.make_async_copy(wq.at[pl.ds(t * kr, kr)], wqb.at[t], wq_sem.at[t]) for t in range(nk)]
    for cps in kv_copies:
        for cp in cps:
            cp.start()
    for cp in q_copies:
        cp.start()

    barrier = pltpu.get_barrier_semaphore()

    @pl.loop(1, n)
    def _(i):
        pl.semaphore_signal(barrier, inc=1, device_id={"cp": lax.rem(me + i, n)}, device_id_type=MESH)

    def put(src, dst, send, recv, dev):
        return pltpu.make_async_remote_copy(src, dst, send, recv, device_id={"cp": dev}, device_id_type=MESH)

    def seg_copy(i):
        return put(seg_in, segb.at[pl.ds(me, 1)], seg_send.at[i], seg_recv.at[me], lax.rem(me + i, n))

    seg_own = pltpu.make_async_copy(seg_in, segb.at[pl.ds(me, 1)], seg_sem.at[0])
    seg_own.start()

    way = (1, -1)

    def kv_copy(half, t, dx, dy):
        return put(skv.at[pt.head(dx, dy), half], kvb.at[me, half], kv_send.at[half, 2 * t + dx], kv_recv.at[half, me],
                   pt.peer(dx, dy))

    def kv_hop(half, dx):
        return put(skv.at[pt.head(dx, FAR), half], rkv.at[half, dx], kv_send.at[half, dx], rkv_recv.at[half, dx],
                   pt.peer(0, way[half]))

    def kv_hand(half, dx):
        src = pt.peer(0, -way[half])
        return put(rkv.at[half, dx], kvb.at[src, half], rkv_send.at[half, dx], kv_recv.at[half, src], pt.peer(dx, way[half]))

    def q_copy(half, t, dx, dy):
        return put(sq.at[pt.head(dx, dy), half], qb.at[my_slot, half], q_send.at[half, 2 * t + dx], q_recv.at[half, my_slot],
                   pt.peer(dx, dy))

    def q_hop(half, dx):
        return put(sq.at[pt.head(dx, FAR), half], rq.at[half, dx], q_send.at[half, dx], rq_recv.at[half, dx],
                   pt.peer(0, way[half]))

    def q_hand(half, dx):
        slot = pt.slot(0, -way[half])
        return put(rq.at[half, dx], qb.at[slot, half], rq_send.at[half, dx], q_recv.at[half, slot], pt.peer(dx, way[half]))

    nb = 4 * DH

    def summed(t, w, acc, c):
        cols = slice(c * nb, (c + 1) * nb)
        r = jnp.dot(x_ref[:, t * kr:(t + 1) * kr], w[:, cols], preferred_element_type=jnp.float32)
        if t > 0:
            r = r + acc[:, cols]
        if t < nk - 1:
            acc[:, cols] = r
        return r

    def kv_step(t):
        for cp in kv_copies[t]:
            cp.wait()
        for c in range(wkvb.shape[3] // nb):
            for i in range(2):
                r = summed(t, wkvb.at[i, t], kvacc.at[i], c)
                if t == nk - 1:
                    for u in range(nb // DH):
                        part = r[:, u * DH:(u + 1) * DH]
                        part = (jnp.transpose(part) if i == 1 else part).astype(jnp.bfloat16)
                        for half in range(2):
                            rows = slice(half * PC, (half + 1) * PC)
                            skv[c * (nb // DH) + u, half, i] = part[:, rows] if i == 1 else part[rows]

    def q_step(t, first, last):
        if first == 0:
            q_copies[t].wait()
        for c in range(first, last):
            r = summed(t, wqb.at[t], qacc, c)
            if t == nk - 1:
                for u in range(nb // DH):
                    col = c * (nb // DH) + u
                    part = jnp.transpose(r[:, u * DH:(u + 1) * DH]).astype(jnp.bfloat16)
                    for half in range(2):
                        sq[col // g, half, col % g] = part[:, half * PC:(half + 1) * PC]

    def send_kv(half):
        for dx in range(2):
            kv_hop(half, dx).start()
        for t, dx, dy in kv_steps:
            if dy != FAR and (t, dx) != own_kv:
                kv_copy(half, t, dx, dy).start()

    def send_q(half):
        for dx in range(2):
            q_hop(half, dx).start()
        for t, dx, dy in q_steps:
            if dy != FAR and (t, dx) != own_q:
                q_copy(half, t, dx, dy).start()

    def hand_on(half, kind):
        buf, recv, hand = (rkv, rkv_recv, kv_hand) if kind == "kv" else (rq, rq_recv, q_hand)
        for dx in range(2):
            put(buf.at[half, dx], buf.at[half, dx], kv_send.at[0, 0], recv.at[half, dx], me).wait_recv()
            hand(half, dx).start()

    def to_cross(half, src, i):
        return put(kvb.at[src, half], kvb.at[src, half], fx_send.at[half, i], kv_recv.at[half, src], pt.dev(pt.xcross, pt.y, pt.c))

    def to_sibling(half, src, i):
        return put(kvb.at[src, half], kvb.at[src, half], fs_send.at[half, i], kv_recv.at[half, src], pt.dev(pt.x, pt.y, 1 - pt.c))

    def kv_out(half, src):
        return pltpu.make_async_copy(kvb.at[src, half], kv_o.at[src, half], out_sem.at[half, src])

    def q_out(slot):
        return pltpu.make_async_copy(qb.at[slot, 1], q_o.at[slot], qout_sem.at[slot])

    def arrived(half, src):
        to_sibling(half, src, 0).wait_recv()

    def forward(half, t, dxs=(0, 1)):
        for dx in dxs:
            src = pt.peer(dx, -KV_ORDER[t])
            if (t, dx) != own_kv:
                arrived(half, src)
            to_cross(half, src, 2 * t + dx).start()
            to_sibling(half, src, 2 * t + dx).start()
            kv_out(half, src).start()

    def mirrored(dx, dy, c):
        return pt.dev(pt.side - 1 - pt.col(dx), pt.row(-dy), c)

    own_t = own_kv[0]
    passing = [(t, dx, KV_ORDER[t]) for t in (1, 2, 3, 0) for dx in range(2)]

    def pass_on(half, steps):
        for t, dx, dy in steps:
            src = mirrored(dx, dy, pt.c)
            arrived(half, src)
            to_sibling(half, src, 8 + 2 * t + dx).start()
            kv_out(half, src).start()

    def from_sibling(half):
        for far_side in range(2):
            for t, dx, dy in passing:
                src = mirrored(dx, dy, 1 - pt.c) if far_side else pt.dev(pt.col(dx), pt.row(-dy), 1 - pt.c)
                arrived(half, src)
                kv_out(half, src).start()

    def queries(half):
        for t, dx, dy in q_steps:
            slot = pt.slot(dx, -dy)
            if (t, dx) != own_q:
                put(qb.at[slot, half], qb.at[slot, half], q_send.at[0, 0], q_recv.at[half, slot], me).wait_recv()
            if half:
                q_out(slot).start()

    for t in range(nk):
        kv_step(t)
    kvb[me] = skv[my_head]
    nq = wqb.shape[2] // nb
    q_step(0, 0, 1)

    pl.semaphore_wait(barrier, n - 1)
    send_kv(0)
    forward(0, own_t, (0,))
    forward(1, own_t, (0,))

    @pl.loop(1, n)
    def _(i):
        seg_copy(i).start()

    q_step(0, 1, nq)
    q_step(1, 0, nq)
    q_step(2, 0, nq)
    forward(0, own_t, (1,))
    hand_on(0, "kv")
    q_step(3, 0, nq)
    qb[my_slot] = sq[my_head]
    forward(0, 2)
    send_q(0)
    send_kv(1)
    send_q(1)
    forward(0, 3)
    forward(0, 0)
    pass_on(0, passing[:4])
    hand_on(0, "q")
    pass_on(0, passing[4:])
    from_sibling(0)
    queries(0)
    seg_own.wait()

    @pl.loop(1, n)
    def _(i):
        src = lax.rem(me + i, n)
        put(seg_in, segb.at[pl.ds(src, 1)], seg_send.at[i], seg_recv.at[src], src).wait_recv()

    seg_copies = [pltpu.make_async_copy(segb, seg_s, seg_sem.at[1]), pltpu.make_async_copy(segb, segs_o, seg_sem.at[2])]
    for cp in seg_copies:
        cp.start()
    for cp in seg_copies:
        cp.wait()

    pairs = Pairs(pt, n, g, scale, lambda src, half: seg_s[src, half, 0], segb, n, lambda p, i: kvb[p, 0, i],
                  lambda row, u, w: qb[2 * row + u, 0, w], t_sc, acc_sc)

    def o_out(row):
        return pltpu.make_async_copy(ol.at[pl.ds(2 * row, 2)], o_o.at[pl.ds(2 * row, 2)], o_sem.at[row])

    def low(row, carry):
        def store(u, w, val):
            ol[2 * row + u, :, w * DH:(w + 1) * DH] = val

        pairs(row, 0, 0, pairs.begins(row, 0), store)

        @pl.when(row == 0)
        def _():
            forward(1, own_t, (1,))
            hand_on(1, "kv")
            forward(1, 2)

        @pl.when(row == 1)
        def _():
            forward(1, 3)
            o_out(0).start()

        @pl.when(row == 2)
        def _():
            forward(1, 0)
            hand_on(1, "q")
            pass_on(1, passing[:4])
            o_out(1).start()

        return carry

    lax.fori_loop(0, ng // 2, low, 0)
    pass_on(1, passing[4:])
    o_out(2).start()
    from_sibling(1)
    queries(1)
    o_out(3).start()

    @pl.loop(1, n)
    def _(i):
        seg_copy(i).wait_send()

    for half in range(2):
        for dx in range(2):
            kv_hop(half, dx).wait_send()
            kv_hand(half, dx).wait_send()
            q_hop(half, dx).wait_send()
            q_hand(half, dx).wait_send()
        for t, dx, dy in kv_steps:
            if dy != FAR and (t, dx) != own_kv:
                kv_copy(half, t, dx, dy).wait_send()
            src = pt.peer(dx, -dy)
            to_cross(half, src, 2 * t + dx).wait_send()
            to_sibling(half, src, 2 * t + dx).wait_send()
            to_sibling(half, src, 8 + 2 * t + dx).wait_send()
        for t, dx, dy in q_steps:
            if dy != FAR and (t, dx) != own_q:
                q_copy(half, t, dx, dy).wait_send()

        @pl.loop(0, n)
        def _(i):
            kv_out(half, i).wait()

    for i in range(ng):
        q_out(i).wait()
    for row in range(ng // 2):
        o_out(row).wait()


def _attend(n, g, scale, segs, kv, q_in, o_out, seg_s, seg_v, kvs, qs, os, lo_s, t_sc, acc_sc,
            seg_sem, kv_sem, q_sem, o_sem):
    pt = Place(n)
    last_piece = 2 * n - 1
    ng = q_in.shape[0]

    def load(p):
        owner = jnp.where(p < n, p, last_piece - p)
        return pltpu.make_async_copy(kv.at[owner, jnp.where(p < n, 0, 1)], kvs.at[p], kv_sem)

    seg_copies = [pltpu.make_async_copy(segs, seg_v, seg_sem.at[0]), pltpu.make_async_copy(segs, seg_s, seg_sem.at[1])]
    q_copies = [pltpu.make_async_copy(q_in.at[i], qs.at[i], q_sem) for i in range(ng)]
    for cp in seg_copies + q_copies:
        cp.start()

    @pl.loop(0, 2 * n)
    def _(p):
        load(p).start()

    for cp in seg_copies:
        cp.wait()
    pairs = Pairs(pt, n, g, scale, lambda src, half: seg_s[src, half, 0], seg_v, 2 * n, lambda p, i: kvs[p, i],
                  lambda row, u, w: qs[2 * row + u, w], t_sc, acc_sc)
    for i in range(ng // 2):
        for u, at in enumerate(pairs.begins(i, 1)):
            lo_s[2 * i + u] = at
    for cp in q_copies:
        cp.wait()

    @pl.loop(0, 2 * n)
    def _(p):
        load(p).wait()

    def out(slot):
        return pltpu.make_async_copy(os.at[slot], o_out.at[slot], o_sem)

    def one(row, carry):
        def store(u, w, val):
            os[2 * row + u, :, w * DH:(w + 1) * DH] = val

        begins = [lo_s[2 * row + u] for u in range(2)]
        pairs(row, 1, lax.div(jnp.minimum(*begins), PC), begins, store)

        @pl.when(row > 0)
        def _():
            for u in range(2):
                out(2 * (row - 1) + u).start()

        return carry

    lax.fori_loop(0, ng // 2, one, 0)
    for u in range(2):
        out(ng - 2 + u).start()
    for i in range(ng):
        out(i).wait()


def _combine(n, g, o_lo, o_hi, wo, y_ref, obuf, robuf, wob, acc, w_sem, o_send, o_recv, ro_recv, ro_send):
    pt = Place(n)
    me = pt.me
    gd = g * DH
    my_head, my_slot = pt.head(0, 0), pt.slot(0, 0)
    nc = 4
    wn = y_ref.shape[1] // nc
    rows = (pl.ds(0, PC), pl.ds(PC, PC))
    parts = (o_lo, o_hi)

    own = [pltpu.make_async_copy(parts[half].at[my_slot], obuf.at[my_head, rows[half]], o_recv.at[half, my_head]) for half in range(2)]
    for cp in own:
        cp.start()

    def w_copies(t):
        for dx in range(2):
            h = pl.multiple_of(pt.head(dx, O_ORDER[t]) * gd, gd)
            yield pltpu.make_async_copy(wo.at[pl.ds(h, gd), :], wob.at[t, pl.ds(dx * gd, gd), :], w_sem.at[t, dx])

    for t in range(len(O_ORDER)):
        for cp in w_copies(t):
            cp.start()

    others = [(dx, dy) for dy in O_ORDER for dx in range(2) if (dx, dy) != (0, 0)]
    near = [s for s in others if s[1] != FAR]
    barrier = pltpu.get_barrier_semaphore()
    for dx, dy in others:
        pl.semaphore_signal(barrier, inc=1, device_id={"cp": pt.peer(dx, dy)}, device_id_type=MESH)
    pl.semaphore_wait(barrier, len(others))

    def put(src, dst, send, recv, dev):
        return pltpu.make_async_remote_copy(src, dst, send, recv, device_id={"cp": dev}, device_id_type=MESH)

    way = (1, -1)

    def o_copy(half, i):
        dx, dy = near[i]
        return put(parts[half].at[pt.slot(dx, dy)], obuf.at[my_head, rows[half]], o_send.at[half, i], o_recv.at[half, my_head],
                   pt.peer(dx, dy))

    def o_hop(half, dx):
        return put(parts[half].at[pt.slot(dx, FAR)], robuf.at[half, dx], o_send.at[half, len(near) + dx], ro_recv.at[half, dx],
                   pt.peer(0, way[half]))

    def o_hand(half, dx):
        head = pt.head(0, -way[half])
        return put(robuf.at[half, dx], obuf.at[head, rows[half]], ro_send.at[half, dx], o_recv.at[half, head],
                   pt.peer(dx, way[half]))

    def hand_on(half):
        for dx in range(2):
            put(robuf.at[half, dx], robuf.at[half, dx], o_send.at[0, 0], ro_recv.at[half, dx], me).wait_recv()
            o_hand(half, dx).start()

    for half in range(2):
        o_copy(half, 0).start()
        for dx in range(2):
            o_hop(half, dx).start()
    for half in range(2):
        for i in range(1, len(near)):
            o_copy(half, i).start()

    for t, dy in enumerate(O_ORDER):
        for cp in w_copies(t):
            cp.wait()
        heads = [pt.head(dx, dy) for dx in range(2)]
        for dx in range(2):
            for half in range(2):
                if dy == 0 and dx == 0:
                    own[half].wait()
                else:
                    put(robuf.at[0, 0], obuf.at[heads[dx], rows[half]], o_send.at[0, 0], o_recv.at[half, heads[dx]], me).wait_recv()
        a = jnp.concatenate([obuf[heads[0]], obuf[heads[1]]], axis=1)
        for u in range(nc):
            r = jnp.dot(a, wob[t, :, u * wn:(u + 1) * wn], preferred_element_type=jnp.float32)
            if t > 0:
                r = r + acc[:, u * wn:(u + 1) * wn]
            if t < len(O_ORDER) - 1:
                acc[:, u * wn:(u + 1) * wn] = r
            else:
                y_ref[:, u * wn:(u + 1) * wn] = r.astype(y_ref.dtype)
        if t == 0:
            for half in range(2):
                hand_on(half)
    for half in range(2):
        for i in range(len(near)):
            o_copy(half, i).wait_send()
        for dx in range(2):
            o_hop(half, dx).wait_send()
            o_hand(half, dx).wait_send()


def solution(mesh):
    n = mesh.shape["cp"]
    side = math.isqrt(n // 2)
    bf, f32 = jnp.bfloat16, jnp.float32
    vmem, anym = pl.BlockSpec(memory_space=pltpu.VMEM), pl.BlockSpec(memory_space=pltpu.HBM)
    dma = pltpu.SemaphoreType.DMA

    def local(x, seg, wq, wk, wv, wo):
        lq, d = x.shape
        hkv = wk.shape[1] // DH
        g = wq.shape[1] // wk.shape[1]
        gd = g * DH
        ng = 2 * side
        scale = DH ** -0.5 * math.log2(math.e)
        i32 = jnp.int32
        o_part = jax.ShapeDtypeStruct((ng, PC, gd), bf)
        kv, q, segs, o_lo = pl.pallas_call(
            functools.partial(_project, n, g, scale),
            out_shape=(jax.ShapeDtypeStruct((n, 2, 2, PC, DH), bf), jax.ShapeDtypeStruct((ng, g, PC, DH), bf),
                       jax.ShapeDtypeStruct((n, 2, PC), i32), o_part),
            in_specs=[vmem, anym, anym, anym, anym],
            out_specs=(anym,) * 4,
            scratch_shapes=[
                pltpu.VMEM((2, side, d // side, hkv * DH), bf), pltpu.VMEM((side, d // side, hkv * gd), bf),
                pltpu.VMEM((2, lq, hkv * DH), f32), pltpu.VMEM((lq, hkv * gd), f32),
                pltpu.VMEM((n, 2, 2, PC, DH), bf), pltpu.VMEM((ng, 2, g, PC, DH), bf),
                pltpu.VMEM((ng, 2, 2, PC, DH), bf), pltpu.VMEM((ng, 2, g, PC, DH), bf),
                pltpu.VMEM((2, 2, 2, PC, DH), bf), pltpu.VMEM((2, 2, g, PC, DH), bf),
                pltpu.VMEM((n, 2, PC), i32), pltpu.SMEM((n, 2, PC), i32), pltpu.VMEM((ng, PC, gd), bf)] + _pair_scratch(g) + [
                dma((2, side)), dma((side,)), dma((2, ng)), dma((2, n)), dma((2, 2)), dma((2, 2)), dma((2, ng)), dma((2, 2 * ng)),
                dma((2, ng)), dma((2, ng)), dma((2, 2)), dma((2, 2)), dma((n,)), dma((n,)), dma((3,)), dma((2, n)), dma((ng,)),
                dma((ng // 2,)),
            ],
            compiler_params=pltpu.CompilerParams(collective_id=0, has_side_effects=True, vmem_limit_bytes=60 << 20),
            name="project",
        )(x, seg.reshape(1, 2, PC), wk, wv, wq)
        o = pl.pallas_call(
            functools.partial(_attend, n, g, scale),
            out_shape=o_part,
            in_specs=[anym] * 3,
            out_specs=anym,
            scratch_shapes=[pltpu.SMEM((n, 2, PC), jnp.int32), pltpu.VMEM((n, 2, PC), jnp.int32),
                            pltpu.VMEM((2 * n, 2, PC, DH), bf), pltpu.VMEM((ng, g, PC, DH), bf),
                            pltpu.VMEM((ng, PC, gd), bf), pltpu.SMEM((ng,), jnp.int32)] + _pair_scratch(g) + [dma((2,)), dma, dma, dma],
            compiler_params=pltpu.CompilerParams(vmem_limit_bytes=60 << 20),
            name="attend",
        )(segs, kv, q)
        return pl.pallas_call(
            functools.partial(_combine, n, g),
            out_shape=jax.ShapeDtypeStruct((lq, wo.shape[1]), bf),
            in_specs=[anym] * 3,
            out_specs=vmem,
            scratch_shapes=[pltpu.VMEM((hkv, lq, gd), bf), pltpu.VMEM((2, 2, PC, gd), bf),
                            pltpu.VMEM((side, 2 * gd, wo.shape[1]), bf), pltpu.VMEM((lq, wo.shape[1]), f32),
                            dma((side, 2)), dma((2, ng)), dma((2, ng)), dma((2, 2)), dma((2, 2))],
            compiler_params=pltpu.CompilerParams(collective_id=1, has_side_effects=True, vmem_limit_bytes=60 << 20),
            name="combine",
        )(o_lo, o, wo)

    rows = P(("dp", "cp"), None)
    return jax.shard_map(local, mesh=mesh, in_specs=(rows, P(("dp", "cp")), P(), P(), P(), P()), out_specs=rows, check_vma=False)
```

```python
import functools
import math

import jax
import jax.numpy as jnp
from jax import lax
from jax.experimental import pallas as pl
from jax.experimental.pallas import tpu as pltpu
from jax.sharding import PartitionSpec as P

DH = 128
PC = 128
KB = 4
MESH = pl.DeviceIdType.MESH
NEG_INF = float("-inf")
FLOOR = -3e38


class Place:
    def __init__(self, n):
        me = lax.axis_index("cp")
        self.n, self.side = n, math.isqrt(n // 2)
        self.me = me
        self.c = lax.rem(me, 2)
        chip = me // 2
        self.x = lax.rem(chip, self.side)
        self.y = chip // self.side
        self.xin = self.x + 1 - 2 * lax.rem(self.x, 2)
        self.xcross = self.side - 1 - self.x
        self.px = lax.rem(lax.rem(self.x, 2) + self.x // 2, 2)

    def dev(self, x, y, c):
        return (y * self.side + x) * 2 + c

    def row(self, dy):
        return lax.rem(self.y + dy + self.side, self.side)

    def col(self, dx):
        return self.xin if dx else self.x

    def peer(self, dx, dy):
        return self.dev(self.col(dx), self.row(dy), self.c)

    def head(self, dx, dy):
        return lax.rem(self.px + dx, 2) * self.side + self.row(dy)

    def slot(self, dx, dy):
        return self.row(dy) * 2 + lax.rem(self.x + dx, 2)


FAR = 2
KV_ORDER = (FAR, 0, 1, -1)
Q_ORDER = (FAR, 1, -1, 0)
O_ORDER = (1, -1, FAR, 0)


def _project(n, g, x_in, seg_ref, wk, wv, wq, kv_o, q_o, segs_o, x_ref, wkvb, wqb, kvacc, qacc, kvb, qb, skv, sq, rkv, rq, segb,
             x_sem, wkv_sem, wq_sem, kv_send, kv_recv, kvf_recv, rkv_recv, rkv_send, fx_send, fs_send,
             q_send, q_recv, qf_recv, rq_recv, rq_send, seg_send, seg_recv, out_sem, qout_sem):
    pt = Place(n)
    me = pt.me
    kv_steps = [(t, dx, dy) for t, dy in enumerate(KV_ORDER) for dx in range(2)]
    q_steps = [(t, dx, dy) for t, dy in enumerate(Q_ORDER) for dx in range(2)]
    own_kv = (KV_ORDER.index(0), 0)
    own_q = (Q_ORDER.index(0), 0)
    gd = g * DH
    kr = wqb.shape[1]
    nk = wqb.shape[0]
    my_head, my_slot = pt.head(0, 0), pt.slot(0, 0)

    kv_copies = [[pltpu.make_async_copy(w.at[pl.ds(t * kr, kr)], wkvb.at[i, t], wkv_sem.at[i, t]) for i, w in enumerate((wk, wv))]
                 for t in range(nk)]
    q_copies = [pltpu.make_async_copy(wq.at[pl.ds(t * kr, kr)], wqb.at[t], wq_sem.at[t]) for t in range(nk)]
    x_copy = pltpu.make_async_copy(x_in, x_ref, x_sem)
    x_copy.start()
    for cps in kv_copies:
        for cp in cps:
            cp.start()
    for cp in q_copies:
        cp.start()

    barrier = pltpu.get_barrier_semaphore()

    @pl.loop(1, n)
    def _(i):
        pl.semaphore_signal(barrier, inc=1, device_id={"cp": lax.rem(me + i, n)}, device_id_type=MESH)

    def seg_copy(i):
        return pltpu.make_async_remote_copy(seg_ref, segb.at[pl.ds(me, 1)], seg_send.at[i], seg_recv.at[me],
                                            device_id={"cp": lax.rem(me + i, n)}, device_id_type=MESH)

    segb[pl.ds(me, 1)] = seg_ref[...]

    def put(src, dst, send, recv, dev):
        return pltpu.make_async_remote_copy(src, dst, send, recv, device_id={"cp": dev}, device_id_type=MESH)

    def kv_copy(t, dx, dy):
        return put(skv.at[pt.head(dx, dy)], kvb.at[me], kv_send.at[2 * t + dx], kv_recv.at[me], pt.peer(dx, dy))

    def q_copy(t, dx, dy):
        return put(sq.at[pt.head(dx, dy)], qb.at[my_slot], q_send.at[2 * t + dx], q_recv.at[my_slot], pt.peer(dx, dy))

    way = (1, -1)
    hops = [(half, dx) for half in range(2) for dx in range(2)]

    def kv_hop(half, dx):
        return put(skv.at[pt.head(dx, FAR), half], rkv.at[half, dx], kv_send.at[2 * half + dx if half == 0 else 2 * len(KV_ORDER) + dx],
                   rkv_recv.at[half, dx], pt.peer(0, way[half]))

    def kv_hand(half, dx):
        return put(rkv.at[half, dx], kvb.at[pt.peer(0, -way[half]), half], rkv_send.at[half, dx], kvf_recv.at[dx, half],
                   pt.peer(dx, way[half]))

    def q_hop(half, dx):
        return put(sq.at[pt.head(dx, FAR), half], rq.at[half, dx], q_send.at[2 * half + dx if half == 0 else 2 * len(Q_ORDER) + dx],
                   rq_recv.at[half, dx], pt.peer(0, way[half]))

    def q_hand(half, dx):
        return put(rq.at[half, dx], qb.at[pt.slot(0, -way[half]), half], rq_send.at[half, dx], qf_recv.at[dx, half],
                   pt.peer(dx, way[half]))

    nb = 4 * DH

    def summed(t, w, acc, c):
        cols = slice(c * nb, (c + 1) * nb)
        r = jnp.dot(x_ref[:, t * kr:(t + 1) * kr], w[:, cols], preferred_element_type=jnp.float32)
        if t > 0:
            r = r + acc[:, cols]
        if t < nk - 1:
            acc[:, cols] = r
        return r

    def kv_step(t):
        for cp in kv_copies[t]:
            cp.wait()
        for c in range(wkvb.shape[3] // nb):
            for i in range(2):
                r = summed(t, wkvb.at[i, t], kvacc.at[i], c)
                if t == nk - 1:
                    for u in range(nb // DH):
                        part = r[:, u * DH:(u + 1) * DH]
                        part = (jnp.transpose(part) if i == 1 else part).astype(jnp.bfloat16)
                        for half in range(2):
                            rows = slice(half * PC, (half + 1) * PC)
                            skv[c * (nb // DH) + u, half, i] = part[:, rows] if i == 1 else part[rows]

    def q_step(t, first, last):
        if first == 0:
            q_copies[t].wait()
        for c in range(first, last):
            r = summed(t, wqb.at[t], qacc, c)
            if t == nk - 1:
                for u in range(nb // DH):
                    col = c * (nb // DH) + u
                    part = jnp.transpose(r[:, u * DH:(u + 1) * DH]).astype(jnp.bfloat16)
                    for half in range(2):
                        sq[col // g, half, col % g] = part[:, half * PC:(half + 1) * PC]

    def send_kv(t):
        if KV_ORDER[t] == FAR:
            for hop in hops:
                kv_hop(*hop).start()
        else:
            for dx in range(2):
                if (t, dx) != own_kv:
                    kv_copy(t, dx, KV_ORDER[t]).start()

    def send_q(t):
        if Q_ORDER[t] == FAR:
            for hop in hops:
                q_hop(*hop).start()
        else:
            for dx in range(2):
                if (t, dx) != own_q:
                    q_copy(t, dx, Q_ORDER[t]).start()

    def to_cross(src, i):
        return put(kvb.at[src], kvb.at[src], fx_send.at[i], kv_recv.at[src], pt.dev(pt.xcross, pt.y, pt.c))

    def to_sibling(src, i):
        return put(kvb.at[src], kvb.at[src], fs_send.at[i], kv_recv.at[src], pt.dev(pt.x, pt.y, 1 - pt.c))

    def kv_out(src):
        return pltpu.make_async_copy(kvb.at[src], kv_o.at[src], out_sem.at[src])

    def q_out(slot):
        return pltpu.make_async_copy(qb.at[slot], q_o.at[slot], qout_sem.at[slot])

    def arrived(src):
        to_sibling(src, 0).wait_recv()

    def forward(t):
        dy = KV_ORDER[t]
        for dx in range(2):
            src = pt.peer(dx, -dy)
            if dy == FAR:
                for half in range(2):
                    put(rkv.at[half, dx], kvb.at[src, half], rkv_send.at[half, dx], kvf_recv.at[dx, half], me).wait_recv()
            elif (t, dx) != own_kv:
                arrived(src)
            to_cross(src, 2 * t + dx).start()
            to_sibling(src, 2 * t + dx).start()
            kv_out(src).start()

    def own_out():
        return pltpu.make_async_copy(skv.at[my_head], kv_o.at[me], out_sem.at[me])

    def own_q_out():
        return pltpu.make_async_copy(sq.at[my_head], q_o.at[my_slot], qout_sem.at[my_slot])

    def forward_own():
        put(skv.at[my_head], kvb.at[me], fx_send.at[2 * own_kv[0]], kv_recv.at[me], pt.dev(pt.xcross, pt.y, pt.c)).start()
        put(skv.at[my_head], kvb.at[me], fs_send.at[2 * own_kv[0]], kv_recv.at[me], pt.dev(pt.x, pt.y, 1 - pt.c)).start()
        own_out().start()

    def forward_next():
        src = pt.peer(1, 0)
        arrived(src)
        to_cross(src, 2 * own_kv[0] + 1).start()
        to_sibling(src, 2 * own_kv[0] + 1).start()
        kv_out(src).start()

    x_copy.wait()
    for t in range(nk):
        kv_step(t)
    nq = wqb.shape[2] // nb

    pl.semaphore_wait(barrier, n - 1)
    for t in range(len(KV_ORDER)):
        send_kv(t)
    forward_own()
    q_step(0, 0, nq)
    q_step(1, 0, nq)
    q_step(2, 0, nq)
    forward_next()
    for hop in hops:
        put(rkv.at[hop], rkv.at[hop], kv_send.at[0], rkv_recv.at[hop], me).wait_recv()
        kv_hand(*hop).start()
    q_step(3, 0, nq)
    for t in range(len(Q_ORDER)):
        send_q(t)
    own_q_out().start()
    forward(2)
    forward(3)
    forward(0)

    @pl.loop(1, n)
    def _(i):
        seg_copy(i).start()


    def mirrored(dx, dy, c):
        x = pt.side - 1 - pt.col(dx)
        return pt.dev(x, pt.row(-dy), c)

    passing = [(t, dx, KV_ORDER[t]) for t in (1, 2, 3, 0) for dx in range(2)]

    def pass_on(steps):
        for t, dx, dy in steps:
            src = mirrored(dx, dy, pt.c)
            arrived(src)
            to_sibling(src, 8 + 2 * t + dx).start()
            kv_out(src).start()

    pass_on(passing[:2])
    for hop in hops:
        put(rq.at[hop], rq.at[hop], q_send.at[0], rq_recv.at[hop], me).wait_recv()
        q_hand(*hop).start()
    pass_on(passing[2:])

    for t, dx, dy in passing:
        src = pt.dev(pt.col(dx), pt.row(-dy), 1 - pt.c)
        arrived(src)
        kv_out(src).start()
    for t, dx, dy in q_steps:
        slot = pt.slot(dx, -dy)
        if dy == FAR:
            for half in range(2):
                put(rq.at[half, dx], qb.at[slot, half], rq_send.at[half, dx], qf_recv.at[dx, half], me).wait_recv()
        elif (t, dx) != own_q:
            put(qb.at[slot], qb.at[slot], q_send.at[0], q_recv.at[slot], me).wait_recv()
        if (t, dx) != own_q:
            q_out(slot).start()
    for t, dx, dy in passing:
        src = mirrored(dx, dy, 1 - pt.c)
        arrived(src)
        kv_out(src).start()

    @pl.loop(1, n)
    def _(i):
        src = lax.rem(me + i, n)
        pltpu.make_async_remote_copy(seg_ref, segb.at[pl.ds(src, 1)], seg_send.at[i], seg_recv.at[src],
                                     device_id={"cp": src}, device_id_type=MESH).wait_recv()

    segs_o[...] = segb[...]

    @pl.loop(1, n)
    def _(i):
        seg_copy(i).wait_send()

    for hop in hops:
        kv_hop(*hop).wait_send()
        kv_hand(*hop).wait_send()
        q_hop(*hop).wait_send()
        q_hand(*hop).wait_send()
    for t, dx, dy in kv_steps:
        if dy != FAR and (t, dx) != own_kv:
            kv_copy(t, dx, dy).wait_send()
        src = pt.peer(dx, -dy)
        to_cross(src, 2 * t + dx).wait_send()
        to_sibling(src, 2 * t + dx).wait_send()
        to_sibling(src, 8 + 2 * t + dx).wait_send()
    for t, dx, dy in q_steps:
        if dy != FAR and (t, dx) != own_q:
            q_copy(t, dx, dy).wait_send()

    @pl.loop(0, n)
    def _(i):
        kv_out(i).wait()

    @pl.loop(0, n // 4)
    def _(i):
        q_out(i).wait()


class Pairs:
    def __init__(self, pt, n, g, scale, first_of, seg_v, kvs, qs, t_sc, acc_sc):
        self.pt, self.n, self.g, self.scale, self.first_of, self.seg_v, self.kvs = pt, n, g, scale, first_of, seg_v, kvs
        self.qs, self.t_sc, self.acc_sc = qs, t_sc, acc_sc

    def begins(self, row, half):
        out = []
        for u in range(2):
            src = self.pt.dev((self.pt.x // 2) * 2 + u, row, self.pt.c)
            before = jnp.where(self.seg_v[...] < self.first_of(src, half), 1.0, 0.0)
            out.append(jnp.sum(before).astype(jnp.int32))
        return out

    def __call__(self, row, half, lo, begins, store):
        pt, n, g, scale, seg_v, kvs, qs = self.pt, self.n, self.g, self.scale, self.seg_v, self.kvs, self.qs
        t_sc, acc_sc = self.t_sc, self.acc_sc
        last_piece, pieces = 2 * n - 1, kvs.shape[0]
        srcs = [pt.dev((pt.x // 2) * 2 + u, row, pt.c) for u in range(2)]
        ps = [last_piece - src if half else src for src in srcs]
        end = jnp.maximum(ps[0], ps[1])
        wide = g * PC
        acc_sc[...] = jnp.zeros_like(acc_sc)

        def queries(us):
            return jnp.concatenate([qs[2 * row + u, w] for u in us for w in range(g)], axis=1)

        def start(b):
            return jnp.minimum(lo + b * KB, pieces - KB)

        def scores(b):
            j0, js = lo + b * KB, start(b)
            k = jnp.concatenate([kvs[js + w, 0] for w in range(KB)], axis=0)
            s = jnp.dot(k, queries((0, 1)), preferred_element_type=jnp.float32) * scale
            pos = lax.broadcasted_iota(jnp.int32, (KB * PC, DH), 0) + js * PC
            tops = []
            for u in range(2):
                seen = (pos >= jnp.maximum(begins[u], j0 * PC)) & (pos < ps[u] * PC)
                for w in range(g):
                    at = slice(u * wide + w * PC, u * wide + (w + 1) * PC)
                    part = jnp.where(seen, s[:, at], NEG_INF)
                    t_sc[:, at] = part
                    tops.append(jnp.max(part, axis=0, keepdims=True))
            return jnp.concatenate(tops, axis=1)

        def step(b, carry):
            m, l, top = carry
            js = start(b)
            m_new = jnp.maximum(m, top)
            corr = jnp.exp2(m - m_new)
            p = jnp.exp2(t_sc[...] - m_new)
            l = l * corr + jnp.sum(p, axis=0, keepdims=True)
            vt = jnp.concatenate([kvs[js + w, 1] for w in range(KB)], axis=1)
            acc_sc[...] = acc_sc[...] * corr + jnp.dot(vt, p.astype(jnp.bfloat16), preferred_element_type=jnp.float32)
            return m_new, l, scores(b + 1)

        line = jnp.zeros((1, 2 * wide), jnp.float32)
        m, l, _ = lax.fori_loop(0, lax.div(end - lo + KB - 1, KB), step, (line + FLOOR, line, scores(0)))

        key = lax.broadcasted_iota(jnp.int32, (PC, PC), 0)
        query = lax.broadcasted_iota(jnp.int32, (PC, PC), 1)
        ss = [jnp.dot(kvs[ps[u], 0], queries((u,)), preferred_element_type=jnp.float32) * scale for u in range(2)]
        for u in range(2):
            at = slice(u * wide, (u + 1) * wide)
            ids = seg_v[srcs[u], pl.ds(half, 1), :]
            idb = jnp.broadcast_to(ids, (PC, PC))
            allowed = jnp.concatenate([(idb == jnp.transpose(idb)) & (key <= query)] * g, axis=1)
            keep = jnp.concatenate([ids == self.first_of(srcs[u], half)] * g, axis=1)
            s = jnp.where(allowed, ss[u], NEG_INF)
            m_old = jnp.where(keep, m[:, at], FLOOR)
            m_new = jnp.maximum(m_old, jnp.max(s, axis=0, keepdims=True))
            corr = jnp.where(keep, jnp.exp2(m_old - m_new), 0.0)
            p = jnp.exp2(s - m_new)
            ll = l[:, at] * corr + jnp.sum(p, axis=0, keepdims=True)
            acc = acc_sc[:, at] * corr + jnp.dot(kvs[ps[u], 1], p.astype(jnp.bfloat16), preferred_element_type=jnp.float32)
            o = acc * (1.0 / ll)
            for w in range(g):
                store(u, w, jnp.transpose(o[:, w * PC:(w + 1) * PC]).astype(jnp.bfloat16))


def _pair_scratch(g):
    f32 = jnp.float32
    return [pltpu.VMEM((KB * PC, 2 * g * PC), f32), pltpu.VMEM((DH, 2 * g * PC), f32)]


def _attend(n, g, scale, segs, kv, q_in, o_out, seg_s, seg_v, kvs, qs, os, lo_s, t_sc, acc_sc,
            seg_sem, kv_sem, q_sem, o_sem):
    pt = Place(n)
    last_piece = 2 * n - 1
    ng = q_in.shape[0]

    def load(p):
        owner = jnp.where(p < n, p, last_piece - p)
        return pltpu.make_async_copy(kv.at[owner, jnp.where(p < n, 0, 1)], kvs.at[p], kv_sem)

    seg_copies = [pltpu.make_async_copy(segs, seg_v, seg_sem.at[0]), pltpu.make_async_copy(segs, seg_s, seg_sem.at[1])]
    q_copies = [pltpu.make_async_copy(q_in.at[i, 1], qs.at[i], q_sem) for i in range(ng)]
    for cp in seg_copies + q_copies:
        cp.start()

    @pl.loop(0, 2 * n)
    def _(p):
        load(p).start()

    for cp in seg_copies:
        cp.wait()
    pairs = Pairs(pt, n, g, scale, lambda src, half: seg_s[src, half, 0], seg_v, kvs, qs, t_sc, acc_sc)
    for i in range(ng // 2):
        for u, at in enumerate(pairs.begins(i, 1)):
            lo_s[2 * i + u] = at
    for cp in q_copies:
        cp.wait()

    @pl.loop(0, 2 * n)
    def _(p):
        load(p).wait()

    def out(slot):
        return pltpu.make_async_copy(os.at[slot], o_out.at[slot], o_sem)

    def one(row, carry):
        def store(u, w, val):
            os[2 * row + u, :, w * DH:(w + 1) * DH] = val

        begins = [lo_s[2 * row + u] for u in range(2)]
        pairs(row, 1, lax.div(jnp.minimum(*begins), PC), begins, store)

        @pl.when(row > 0)
        def _():
            for u in range(2):
                out(2 * (row - 1) + u).start()

        return carry

    lax.fori_loop(0, ng // 2, one, 0)
    for u in range(2):
        out(ng - 2 + u).start()
    for i in range(ng):
        out(i).wait()


def _combine(n, g, scale, segs, kv, q_in, o_in, wo, y_ref, obuf, robuf, ol, wob, acc, seg_s, seg_v, kvs, qs,
             t_sc, acc_sc, w_sem, o_send, o_recv, ro_recv, ro_send, seg_sem, kv_sem, q_sem):
    pt = Place(n)
    me = pt.me
    gd = g * DH
    ng = q_in.shape[0]
    my_head, my_slot = pt.head(0, 0), pt.slot(0, 0)
    nc = 4
    wn = y_ref.shape[1] // nc
    lows, highs = pl.ds(0, PC), pl.ds(PC, PC)

    def load(p):
        return pltpu.make_async_copy(kv.at[p, 0], kvs.at[p], kv_sem.at[p])

    q_copies = [pltpu.make_async_copy(q_in.at[i, 0], qs.at[i], q_sem.at[i]) for i in range(ng)]
    seg_copies = [pltpu.make_async_copy(segs, seg_v, seg_sem.at[0]), pltpu.make_async_copy(segs, seg_s, seg_sem.at[1])]
    own = pltpu.make_async_copy(o_in.at[my_slot], obuf.at[my_head, highs], o_recv.at[1, my_head])
    for cp in seg_copies + q_copies + [own]:
        cp.start()

    @pl.loop(0, n)
    def _(p):
        load(p).start()

    def w_copies(t):
        for dx in range(2):
            h = pl.multiple_of(pt.head(dx, O_ORDER[t]) * gd, gd)
            yield pltpu.make_async_copy(wo.at[pl.ds(h, gd), :], wob.at[t, pl.ds(dx * gd, gd), :], w_sem.at[t, dx])

    for t in range(len(O_ORDER)):
        for cp in w_copies(t):
            cp.start()

    others = [(dx, dy) for dy in O_ORDER for dx in range(2) if (dx, dy) != (0, 0)]
    near = [s for s in others if s[1] != FAR]
    barrier = pltpu.get_barrier_semaphore()
    for dx, dy in others:
        pl.semaphore_signal(barrier, inc=1, device_id={"cp": pt.peer(dx, dy)}, device_id_type=MESH)
    pl.semaphore_wait(barrier, len(others))

    def put(src, dst, send, recv, dev):
        return pltpu.make_async_remote_copy(src, dst, send, recv, device_id={"cp": dev}, device_id_type=MESH)

    way = (1, -1)
    turn = {FAR: 0, 1: 1, -1: 2, 0: 3}

    def source(half, dx, dy):
        return o_in.at[pt.slot(dx, dy)] if half else ol.at[turn[dy], lax.rem(pt.x + dx, 2)]

    def o_copy(half, i):
        dx, dy = near[i]
        return put(source(half, dx, dy), obuf.at[my_head, highs if half else lows], o_send.at[half, i], o_recv.at[half, my_head],
                   pt.peer(dx, dy))

    def o_hop(half, dx):
        return put(source(half, dx, FAR), robuf.at[half, dx], o_send.at[half, len(near) + dx], ro_recv.at[half, dx],
                   pt.peer(0, way[half]))

    def o_hand(half, dx):
        head = pt.head(0, -way[half])
        return put(robuf.at[half, dx], obuf.at[head, highs if half else lows], ro_send.at[half, dx], o_recv.at[half, head],
                   pt.peer(dx, way[half]))

    def hand_on(half):
        for dx in range(2):
            put(robuf.at[half, dx], robuf.at[half, dx], o_send.at[0, 0], ro_recv.at[half, dx], me).wait_recv()
            o_hand(half, dx).start()

    for dx in range(2):
        o_hop(1, dx).start()
    for i in range(len(near)):
        o_copy(1, i).start()

    for cp in seg_copies + q_copies:
        cp.wait()

    @pl.loop(0, n)
    def _(p):
        load(p).wait()

    pairs = Pairs(pt, n, g, scale, lambda src, half: seg_s[src, half, 0], seg_v, kvs, qs, t_sc, acc_sc)

    def send_low(dy):
        if dy == FAR:
            for dx in range(2):
                o_hop(0, dx).start()
        else:
            for i, (dx, to) in enumerate(near):
                if to == dy:
                    o_copy(0, i).start()

    def one(i, carry):
        turned = jnp.where(i == 2, -1, jnp.where(i == 3, 0, FAR - i))
        row = lax.rem(pt.y + turned + pt.side, pt.side)

        def store(u, w, val):
            ol[i, u, :, w * DH:(w + 1) * DH] = val

        pairs(row, 0, 0, pairs.begins(row, 0), store)

        @pl.when(i == 1)
        def _():
            send_low(FAR)
            hand_on(1)

        @pl.when(i == 2)
        def _():
            send_low(1)

        @pl.when(i == 3)
        def _():
            send_low(-1)
            hand_on(0)

        return carry

    lax.fori_loop(0, ng // 2, one, 0)
    send_low(0)
    obuf[my_head, 0:PC] = ol[turn[0], lax.rem(pt.x, 2)]

    for t, dy in enumerate(O_ORDER):
        for cp in w_copies(t):
            cp.wait()
        heads = [pt.head(dx, dy) for dx in range(2)]
        for dx in range(2):
            if dy == 0 and dx == 0:
                own.wait()
            else:
                for half in range(2):
                    put(ol.at[0, 0], obuf.at[heads[dx], highs if half else lows], o_send.at[0, 0], o_recv.at[half, heads[dx]],
                        me).wait_recv()
        a = jnp.concatenate([obuf[heads[0]], obuf[heads[1]]], axis=1)
        for u in range(nc):
            r = jnp.dot(a, wob[t, :, u * wn:(u + 1) * wn], preferred_element_type=jnp.float32)
            if t > 0:
                r = r + acc[:, u * wn:(u + 1) * wn]
            if t < len(O_ORDER) - 1:
                acc[:, u * wn:(u + 1) * wn] = r
            else:
                y_ref[:, u * wn:(u + 1) * wn] = r.astype(y_ref.dtype)
    for half in range(2):
        for i in range(len(near)):
            o_copy(half, i).wait_send()
        for dx in range(2):
            o_hop(half, dx).wait_send()
            o_hand(half, dx).wait_send()


def solution(mesh):
    n = mesh.shape["cp"]
    side = math.isqrt(n // 2)
    bf, f32 = jnp.bfloat16, jnp.float32
    vmem, anym = pl.BlockSpec(memory_space=pltpu.VMEM), pl.BlockSpec(memory_space=pltpu.HBM)
    dma = pltpu.SemaphoreType.DMA

    def local(x, seg, wq, wk, wv, wo):
        lq, d = x.shape
        hkv = wk.shape[1] // DH
        g = wq.shape[1] // wk.shape[1]
        gd = g * DH
        ng = 2 * side
        kv, q, segs = pl.pallas_call(
            functools.partial(_project, n, g),
            out_shape=(jax.ShapeDtypeStruct((n, 2, 2, PC, DH), bf), jax.ShapeDtypeStruct((ng, 2, g, PC, DH), bf),
                       jax.ShapeDtypeStruct((n, 2, PC), jnp.int32)),
            in_specs=[anym, vmem, anym, anym, anym],
            out_specs=(anym, anym, vmem),
            scratch_shapes=[
                pltpu.VMEM((lq, d), bf),
                pltpu.VMEM((2, side, d // side, hkv * DH), bf), pltpu.VMEM((side, d // side, hkv * gd), bf),
                pltpu.VMEM((2, lq, hkv * DH), f32), pltpu.VMEM((lq, hkv * gd), f32),
                pltpu.VMEM((n, 2, 2, PC, DH), bf), pltpu.VMEM((ng, 2, g, PC, DH), bf),
                pltpu.VMEM((ng, 2, 2, PC, DH), bf), pltpu.VMEM((ng, 2, g, PC, DH), bf),
                pltpu.VMEM((2, 2, 2, PC, DH), bf), pltpu.VMEM((2, 2, g, PC, DH), bf), pltpu.VMEM((n, 2, PC), jnp.int32),
                dma, dma((2, side)), dma((side,)), dma((ng + 2,)), dma((n,)), dma((2, 2)), dma((2, 2)), dma((2, 2)),
                dma((ng,)), dma((2 * ng,)),
                dma((ng + 2,)), dma((ng,)), dma((2, 2)), dma((2, 2)), dma((2, 2)), dma((n,)), dma((n,)), dma((n,)), dma((ng,)),
            ],
            compiler_params=pltpu.CompilerParams(collective_id=0, has_side_effects=True, vmem_limit_bytes=60 << 20),
            name="project",
        )(x, seg.reshape(1, 2, PC), wk, wv, wq)
        scale = DH ** -0.5 * math.log2(math.e)
        o = pl.pallas_call(
            functools.partial(_attend, n, g, scale),
            out_shape=jax.ShapeDtypeStruct((ng, PC, gd), bf),
            in_specs=[anym] * 3,
            out_specs=anym,
            scratch_shapes=[pltpu.SMEM((n, 2, PC), jnp.int32), pltpu.VMEM((n, 2, PC), jnp.int32),
                            pltpu.VMEM((2 * n, 2, PC, DH), bf), pltpu.VMEM((ng, g, PC, DH), bf),
                            pltpu.VMEM((ng, PC, gd), bf), pltpu.SMEM((ng,), jnp.int32)] + _pair_scratch(g) + [dma((2,)), dma, dma, dma],
            compiler_params=pltpu.CompilerParams(vmem_limit_bytes=60 << 20),
            name="attend",
        )(segs, kv, q)
        return pl.pallas_call(
            functools.partial(_combine, n, g, scale),
            out_shape=jax.ShapeDtypeStruct((lq, wo.shape[1]), bf),
            in_specs=[anym] * 5,
            out_specs=vmem,
            scratch_shapes=[pltpu.VMEM((hkv, lq, gd), bf), pltpu.VMEM((2, 2, PC, gd), bf), pltpu.VMEM((ng // 2, 2, PC, gd), bf),
                            pltpu.VMEM((side, 2 * gd, wo.shape[1]), bf), pltpu.VMEM((lq, wo.shape[1]), f32),
                            pltpu.SMEM((n, 2, PC), jnp.int32), pltpu.VMEM((n, 2, PC), jnp.int32),
                            pltpu.VMEM((n, 2, PC, DH), bf), pltpu.VMEM((ng, g, PC, DH), bf)] + _pair_scratch(g) + [
                            dma((side, 2)), dma((2, ng)), dma((2, ng)), dma((2, 2)), dma((2, 2)), dma((2,)), dma((n,)), dma((ng,))],
            compiler_params=pltpu.CompilerParams(collective_id=1, has_side_effects=True, vmem_limit_bytes=60 << 20),
            name="combine",
        )(segs, kv, q, o, wo)

    rows = P(("dp", "cp"), None)
    return jax.shard_map(local, mesh=mesh, in_specs=(rows, P(("dp", "cp")), P(), P(), P(), P()), out_specs=rows, check_vma=False)
```

```python
import functools
import math

import jax
import jax.numpy as jnp
from jax import lax
from jax.experimental import pallas as pl
from jax.experimental.pallas import tpu as pltpu
from jax.sharding import PartitionSpec as P

DH = 128
PC = 128
KB = 4
MESH = pl.DeviceIdType.MESH
NEG_INF = float("-inf")
FLOOR = -3e38


class Place:
    def __init__(self, n):
        me = lax.axis_index("cp")
        self.n, self.side = n, math.isqrt(n // 2)
        self.me = me
        self.c = lax.rem(me, 2)
        chip = me // 2
        self.x = lax.rem(chip, self.side)
        self.y = chip // self.side
        self.xin = self.x + 1 - 2 * lax.rem(self.x, 2)
        self.xcross = self.side - 1 - self.x
        self.px = lax.rem(lax.rem(self.x, 2) + self.x // 2, 2)

    def dev(self, x, y, c):
        return (y * self.side + x) * 2 + c

    def row(self, dy):
        return lax.rem(self.y + dy + self.side, self.side)

    def col(self, dx):
        return self.xin if dx else self.x

    def peer(self, dx, dy):
        return self.dev(self.col(dx), self.row(dy), self.c)

    def head(self, dx, dy):
        return lax.rem(self.px + dx, 2) * self.side + self.row(dy)

    def slot(self, dx, dy):
        return self.row(dy) * 2 + lax.rem(self.x + dx, 2)


FAR = 2
KV_ORDER = (FAR, 0, 1, -1)
Q_ORDER = (FAR, 1, -1, 0)
O_ORDER = (1, -1, FAR, 0)


def _project(n, g, x_in, seg_ref, wk, wv, wq, kv_o, q_o, segs_o, x_ref, wkvb, wqb, kvacc, qacc, kvb, qb, skv, sq, rkv, rq, segb,
             x_sem, wkv_sem, wq_sem, kv_send, kv_recv, kvf_recv, rkv_recv, rkv_send, fx_send, fs_send,
             q_send, q_recv, qf_recv, rq_recv, rq_send, seg_send, seg_recv, out_sem, qout_sem):
    pt = Place(n)
    me = pt.me
    kv_steps = [(t, dx, dy) for t, dy in enumerate(KV_ORDER) for dx in range(2)]
    q_steps = [(t, dx, dy) for t, dy in enumerate(Q_ORDER) for dx in range(2)]
    own_kv = (KV_ORDER.index(0), 0)
    own_q = (Q_ORDER.index(0), 0)
    gd = g * DH
    kr = wqb.shape[1]
    nk = wqb.shape[0]
    my_head, my_slot = pt.head(0, 0), pt.slot(0, 0)

    kv_copies = [[pltpu.make_async_copy(w.at[pl.ds(t * kr, kr)], wkvb.at[i, t], wkv_sem.at[i, t]) for i, w in enumerate((wk, wv))]
                 for t in range(nk)]
    q_copies = [pltpu.make_async_copy(wq.at[pl.ds(t * kr, kr)], wqb.at[t], wq_sem.at[t]) for t in range(nk)]
    x_copy = pltpu.make_async_copy(x_in, x_ref, x_sem)
    x_copy.start()
    for cps in kv_copies:
        for cp in cps:
            cp.start()
    for cp in q_copies:
        cp.start()

    barrier = pltpu.get_barrier_semaphore()

    @pl.loop(1, n)
    def _(i):
        pl.semaphore_signal(barrier, inc=1, device_id={"cp": lax.rem(me + i, n)}, device_id_type=MESH)

    def seg_copy(i):
        return pltpu.make_async_remote_copy(seg_ref, segb.at[pl.ds(me, 1)], seg_send.at[i], seg_recv.at[me],
                                            device_id={"cp": lax.rem(me + i, n)}, device_id_type=MESH)

    segb[pl.ds(me, 1)] = seg_ref[...]

    def put(src, dst, send, recv, dev):
        return pltpu.make_async_remote_copy(src, dst, send, recv, device_id={"cp": dev}, device_id_type=MESH)

    def kv_copy(t, dx, dy):
        return put(skv.at[pt.head(dx, dy)], kvb.at[me], kv_send.at[2 * t + dx], kv_recv.at[me], pt.peer(dx, dy))

    def q_copy(t, dx, dy):
        return put(sq.at[pt.head(dx, dy)], qb.at[my_slot], q_send.at[2 * t + dx], q_recv.at[my_slot], pt.peer(dx, dy))

    way = (1, -1)
    hops = [(half, dx) for half in range(2) for dx in range(2)]

    def kv_hop(half, dx):
        return put(skv.at[pt.head(dx, FAR), half], rkv.at[half, dx], kv_send.at[2 * half + dx if half == 0 else 2 * len(KV_ORDER) + dx],
                   rkv_recv.at[half, dx], pt.peer(0, way[half]))

    def kv_hand(half, dx):
        return put(rkv.at[half, dx], kvb.at[pt.peer(0, -way[half]), half], rkv_send.at[half, dx], kvf_recv.at[dx, half],
                   pt.peer(dx, way[half]))

    def q_hop(half, dx):
        return put(sq.at[pt.head(dx, FAR), half], rq.at[half, dx], q_send.at[2 * half + dx if half == 0 else 2 * len(Q_ORDER) + dx],
                   rq_recv.at[half, dx], pt.peer(0, way[half]))

    def q_hand(half, dx):
        return put(rq.at[half, dx], qb.at[pt.slot(0, -way[half]), half], rq_send.at[half, dx], qf_recv.at[dx, half],
                   pt.peer(dx, way[half]))

    nb = 4 * DH

    def summed(t, w, acc, c):
        cols = slice(c * nb, (c + 1) * nb)
        r = jnp.dot(x_ref[:, t * kr:(t + 1) * kr], w[:, cols], preferred_element_type=jnp.float32)
        if t > 0:
            r = r + acc[:, cols]
        if t < nk - 1:
            acc[:, cols] = r
        return r

    def kv_step(t):
        for cp in kv_copies[t]:
            cp.wait()
        for c in range(wkvb.shape[3] // nb):
            for i in range(2):
                r = summed(t, wkvb.at[i, t], kvacc.at[i], c)
                if t == nk - 1:
                    for u in range(nb // DH):
                        part = r[:, u * DH:(u + 1) * DH]
                        part = (jnp.transpose(part) if i == 1 else part).astype(jnp.bfloat16)
                        for half in range(2):
                            rows = slice(half * PC, (half + 1) * PC)
                            skv[c * (nb // DH) + u, half, i] = part[:, rows] if i == 1 else part[rows]

    def q_step(t, first, last):
        if first == 0:
            q_copies[t].wait()
        for c in range(first, last):
            r = summed(t, wqb.at[t], qacc, c)
            if t == nk - 1:
                for u in range(nb // DH):
                    col = c * (nb // DH) + u
                    part = jnp.transpose(r[:, u * DH:(u + 1) * DH]).astype(jnp.bfloat16)
                    for half in range(2):
                        sq[col // g, half, col % g] = part[:, half * PC:(half + 1) * PC]

    def send_kv(t):
        if KV_ORDER[t] == FAR:
            for hop in hops:
                kv_hop(*hop).start()
        else:
            for dx in range(2):
                if (t, dx) != own_kv:
                    kv_copy(t, dx, KV_ORDER[t]).start()

    def send_q(t):
        if Q_ORDER[t] == FAR:
            for hop in hops:
                q_hop(*hop).start()
        else:
            for dx in range(2):
                if (t, dx) != own_q:
                    q_copy(t, dx, Q_ORDER[t]).start()

    def to_cross(src, i):
        return put(kvb.at[src], kvb.at[src], fx_send.at[i], kv_recv.at[src], pt.dev(pt.xcross, pt.y, pt.c))

    def to_sibling(src, i):
        return put(kvb.at[src], kvb.at[src], fs_send.at[i], kv_recv.at[src], pt.dev(pt.x, pt.y, 1 - pt.c))

    def kv_out(src):
        return pltpu.make_async_copy(kvb.at[src], kv_o.at[src], out_sem.at[src])

    def q_out(slot):
        return pltpu.make_async_copy(qb.at[slot], q_o.at[slot], qout_sem.at[slot])

    def arrived(src):
        to_sibling(src, 0).wait_recv()

    def forward(t):
        dy = KV_ORDER[t]
        for dx in range(2):
            src = pt.peer(dx, -dy)
            if dy == FAR:
                for half in range(2):
                    put(rkv.at[half, dx], kvb.at[src, half], rkv_send.at[half, dx], kvf_recv.at[dx, half], me).wait_recv()
            elif (t, dx) != own_kv:
                arrived(src)
            to_cross(src, 2 * t + dx).start()
            to_sibling(src, 2 * t + dx).start()
            kv_out(src).start()

    def own_out():
        return pltpu.make_async_copy(skv.at[my_head], kv_o.at[me], out_sem.at[me])

    def own_q_out():
        return pltpu.make_async_copy(sq.at[my_head], q_o.at[my_slot], qout_sem.at[my_slot])

    def forward_own():
        put(skv.at[my_head], kvb.at[me], fx_send.at[2 * own_kv[0]], kv_recv.at[me], pt.dev(pt.xcross, pt.y, pt.c)).start()
        put(skv.at[my_head], kvb.at[me], fs_send.at[2 * own_kv[0]], kv_recv.at[me], pt.dev(pt.x, pt.y, 1 - pt.c)).start()
        own_out().start()

    def forward_next():
        src = pt.peer(1, 0)
        arrived(src)
        to_cross(src, 2 * own_kv[0] + 1).start()
        to_sibling(src, 2 * own_kv[0] + 1).start()
        kv_out(src).start()

    x_copy.wait()
    for t in range(nk):
        kv_step(t)
    nq = wqb.shape[2] // nb

    pl.semaphore_wait(barrier, n - 1)
    for t in range(len(KV_ORDER)):
        send_kv(t)
    forward_own()
    q_step(0, 0, nq)
    q_step(1, 0, nq)
    q_step(2, 0, nq)
    forward_next()
    for hop in hops:
        put(rkv.at[hop], rkv.at[hop], kv_send.at[0], rkv_recv.at[hop], me).wait_recv()
        kv_hand(*hop).start()
    q_step(3, 0, nq)
    own_q_out().start()
    forward(2)
    forward(3)
    forward(0)
    send_q(0)
    send_q(1)

    def mirrored(dx, dy, c):
        x = pt.side - 1 - pt.col(dx)
        return pt.dev(x, pt.row(-dy), c)

    passing = [(t, dx, KV_ORDER[t]) for t in (1, 2, 3, 0) for dx in range(2)]

    def pass_on(steps):
        for t, dx, dy in steps:
            src = mirrored(dx, dy, pt.c)
            arrived(src)
            to_sibling(src, 8 + 2 * t + dx).start()
            kv_out(src).start()

    pass_on(passing[:4])
    send_q(2)
    for hop in hops:
        put(rq.at[hop], rq.at[hop], q_send.at[0], rq_recv.at[hop], me).wait_recv()
        q_hand(*hop).start()
    send_q(3)
    pass_on(passing[4:])

    @pl.loop(1, n)
    def _(i):
        seg_copy(i).start()

    for t, dx, dy in passing:
        src = pt.dev(pt.col(dx), pt.row(-dy), 1 - pt.c)
        arrived(src)
        kv_out(src).start()
    for t, dx, dy in q_steps:
        slot = pt.slot(dx, -dy)
        if dy == FAR:
            for half in range(2):
                put(rq.at[half, dx], qb.at[slot, half], rq_send.at[half, dx], qf_recv.at[dx, half], me).wait_recv()
        elif (t, dx) != own_q:
            put(qb.at[slot], qb.at[slot], q_send.at[0], q_recv.at[slot], me).wait_recv()
        if (t, dx) != own_q:
            q_out(slot).start()
    for t, dx, dy in passing:
        src = mirrored(dx, dy, 1 - pt.c)
        arrived(src)
        kv_out(src).start()

    @pl.loop(1, n)
    def _(i):
        src = lax.rem(me + i, n)
        pltpu.make_async_remote_copy(seg_ref, segb.at[pl.ds(src, 1)], seg_send.at[i], seg_recv.at[src],
                                     device_id={"cp": src}, device_id_type=MESH).wait_recv()

    segs_o[...] = segb[...]

    @pl.loop(1, n)
    def _(i):
        seg_copy(i).wait_send()

    for hop in hops:
        kv_hop(*hop).wait_send()
        kv_hand(*hop).wait_send()
        q_hop(*hop).wait_send()
        q_hand(*hop).wait_send()
    for t, dx, dy in kv_steps:
        if dy != FAR and (t, dx) != own_kv:
            kv_copy(t, dx, dy).wait_send()
        src = pt.peer(dx, -dy)
        to_cross(src, 2 * t + dx).wait_send()
        to_sibling(src, 2 * t + dx).wait_send()
        to_sibling(src, 8 + 2 * t + dx).wait_send()
    for t, dx, dy in q_steps:
        if dy != FAR and (t, dx) != own_q:
            q_copy(t, dx, dy).wait_send()

    @pl.loop(0, n)
    def _(i):
        kv_out(i).wait()

    @pl.loop(0, n // 4)
    def _(i):
        q_out(i).wait()


class Pairs:
    def __init__(self, pt, n, g, scale, first_of, seg_v, kvs, qs, t_sc, acc_sc):
        self.pt, self.n, self.g, self.scale, self.first_of, self.seg_v, self.kvs = pt, n, g, scale, first_of, seg_v, kvs
        self.qs, self.t_sc, self.acc_sc = qs, t_sc, acc_sc

    def begins(self, row, half):
        out = []
        for u in range(2):
            src = self.pt.dev((self.pt.x // 2) * 2 + u, row, self.pt.c)
            before = jnp.where(self.seg_v[...] < self.first_of(src, half), 1.0, 0.0)
            out.append(jnp.sum(before).astype(jnp.int32))
        return out

    def __call__(self, row, half, lo, begins, store):
        pt, n, g, scale, seg_v, kvs, qs = self.pt, self.n, self.g, self.scale, self.seg_v, self.kvs, self.qs
        t_sc, acc_sc = self.t_sc, self.acc_sc
        last_piece, pieces = 2 * n - 1, kvs.shape[0]
        srcs = [pt.dev((pt.x // 2) * 2 + u, row, pt.c) for u in range(2)]
        ps = [last_piece - src if half else src for src in srcs]
        end = jnp.maximum(ps[0], ps[1])
        wide = g * PC
        acc_sc[...] = jnp.zeros_like(acc_sc)

        def queries(us):
            return jnp.concatenate([qs[2 * row + u, w] for u in us for w in range(g)], axis=1)

        def start(b):
            return jnp.minimum(lo + b * KB, pieces - KB)

        def scores(b):
            j0, js = lo + b * KB, start(b)
            k = jnp.concatenate([kvs[js + w, 0] for w in range(KB)], axis=0)
            s = jnp.dot(k, queries((0, 1)), preferred_element_type=jnp.float32) * scale
            pos = lax.broadcasted_iota(jnp.int32, (KB * PC, DH), 0) + js * PC
            tops = []
            for u in range(2):
                seen = (pos >= jnp.maximum(begins[u], j0 * PC)) & (pos < ps[u] * PC)
                for w in range(g):
                    at = slice(u * wide + w * PC, u * wide + (w + 1) * PC)
                    part = jnp.where(seen, s[:, at], NEG_INF)
                    t_sc[:, at] = part
                    tops.append(jnp.max(part, axis=0, keepdims=True))
            return jnp.concatenate(tops, axis=1)

        def step(b, carry):
            m, l, top = carry
            js = start(b)
            m_new = jnp.maximum(m, top)
            corr = jnp.exp2(m - m_new)
            p = jnp.exp2(t_sc[...] - m_new)
            l = l * corr + jnp.sum(p, axis=0, keepdims=True)
            vt = jnp.concatenate([kvs[js + w, 1] for w in range(KB)], axis=1)
            acc_sc[...] = acc_sc[...] * corr + jnp.dot(vt, p.astype(jnp.bfloat16), preferred_element_type=jnp.float32)
            return m_new, l, scores(b + 1)

        line = jnp.zeros((1, 2 * wide), jnp.float32)
        m, l, _ = lax.fori_loop(0, lax.div(end - lo + KB - 1, KB), step, (line + FLOOR, line, scores(0)))

        key = lax.broadcasted_iota(jnp.int32, (PC, PC), 0)
        query = lax.broadcasted_iota(jnp.int32, (PC, PC), 1)
        ss = [jnp.dot(kvs[ps[u], 0], queries((u,)), preferred_element_type=jnp.float32) * scale for u in range(2)]
        for u in range(2):
            at = slice(u * wide, (u + 1) * wide)
            ids = seg_v[srcs[u], pl.ds(half, 1), :]
            idb = jnp.broadcast_to(ids, (PC, PC))
            allowed = jnp.concatenate([(idb == jnp.transpose(idb)) & (key <= query)] * g, axis=1)
            keep = jnp.concatenate([ids == self.first_of(srcs[u], half)] * g, axis=1)
            s = jnp.where(allowed, ss[u], NEG_INF)
            m_old = jnp.where(keep, m[:, at], FLOOR)
            m_new = jnp.maximum(m_old, jnp.max(s, axis=0, keepdims=True))
            corr = jnp.where(keep, jnp.exp2(m_old - m_new), 0.0)
            p = jnp.exp2(s - m_new)
            ll = l[:, at] * corr + jnp.sum(p, axis=0, keepdims=True)
            acc = acc_sc[:, at] * corr + jnp.dot(kvs[ps[u], 1], p.astype(jnp.bfloat16), preferred_element_type=jnp.float32)
            o = acc * (1.0 / ll)
            for w in range(g):
                store(u, w, jnp.transpose(o[:, w * PC:(w + 1) * PC]).astype(jnp.bfloat16))


def _pair_scratch(g):
    f32 = jnp.float32
    return [pltpu.VMEM((KB * PC, 2 * g * PC), f32), pltpu.VMEM((DH, 2 * g * PC), f32)]


def _attend(n, g, scale, segs, kv, q_in, o_out, seg_s, seg_v, kvs, qs, os, lo_s, t_sc, acc_sc,
            seg_sem, kv_sem, q_sem, o_sem):
    pt = Place(n)
    last_piece = 2 * n - 1
    ng = q_in.shape[0]

    def load(p):
        owner = jnp.where(p < n, p, last_piece - p)
        return pltpu.make_async_copy(kv.at[owner, jnp.where(p < n, 0, 1)], kvs.at[p], kv_sem)

    seg_copies = [pltpu.make_async_copy(segs, seg_v, seg_sem.at[0]), pltpu.make_async_copy(segs, seg_s, seg_sem.at[1])]
    q_copies = [pltpu.make_async_copy(q_in.at[i, 1], qs.at[i], q_sem) for i in range(ng)]
    for cp in seg_copies + q_copies:
        cp.start()

    @pl.loop(0, 2 * n)
    def _(p):
        load(p).start()

    for cp in seg_copies:
        cp.wait()
    pairs = Pairs(pt, n, g, scale, lambda src, half: seg_s[src, half, 0], seg_v, kvs, qs, t_sc, acc_sc)
    for i in range(ng // 2):
        for u, at in enumerate(pairs.begins(i, 1)):
            lo_s[2 * i + u] = at
    for cp in q_copies:
        cp.wait()

    @pl.loop(0, 2 * n)
    def _(p):
        load(p).wait()

    def out(slot):
        return pltpu.make_async_copy(os.at[slot], o_out.at[slot], o_sem)

    def one(row, carry):
        def store(u, w, val):
            os[2 * row + u, :, w * DH:(w + 1) * DH] = val

        begins = [lo_s[2 * row + u] for u in range(2)]
        pairs(row, 1, lax.div(jnp.minimum(*begins), PC), begins, store)

        @pl.when(row > 0)
        def _():
            for u in range(2):
                out(2 * (row - 1) + u).start()

        return carry

    lax.fori_loop(0, ng // 2, one, 0)
    for u in range(2):
        out(ng - 2 + u).start()
    for i in range(ng):
        out(i).wait()


def _combine(n, g, scale, segs, kv, q_in, o_in, wo, y_ref, obuf, robuf, ol, wob, acc, seg_s, seg_v, kvs, qs,
             t_sc, acc_sc, w_sem, o_send, o_recv, ro_recv, ro_send, seg_sem, kv_sem, q_sem):
    pt = Place(n)
    me = pt.me
    gd = g * DH
    ng = q_in.shape[0]
    my_head, my_slot = pt.head(0, 0), pt.slot(0, 0)
    nc = 4
    wn = y_ref.shape[1] // nc
    lows, highs = pl.ds(0, PC), pl.ds(PC, PC)

    def load(p):
        return pltpu.make_async_copy(kv.at[p, 0], kvs.at[p], kv_sem.at[p])

    q_copies = [pltpu.make_async_copy(q_in.at[i, 0], qs.at[i], q_sem.at[i]) for i in range(ng)]
    seg_copies = [pltpu.make_async_copy(segs, seg_v, seg_sem.at[0]), pltpu.make_async_copy(segs, seg_s, seg_sem.at[1])]
    own = pltpu.make_async_copy(o_in.at[my_slot], obuf.at[my_head, highs], o_recv.at[1, my_head])
    for cp in seg_copies + q_copies + [own]:
        cp.start()

    @pl.loop(0, n)
    def _(p):
        load(p).start()

    def w_copies(t):
        for dx in range(2):
            h = pl.multiple_of(pt.head(dx, O_ORDER[t]) * gd, gd)
            yield pltpu.make_async_copy(wo.at[pl.ds(h, gd), :], wob.at[t, pl.ds(dx * gd, gd), :], w_sem.at[t, dx])

    for t in range(len(O_ORDER)):
        for cp in w_copies(t):
            cp.start()

    others = [(dx, dy) for dy in O_ORDER for dx in range(2) if (dx, dy) != (0, 0)]
    near = [s for s in others if s[1] != FAR]
    barrier = pltpu.get_barrier_semaphore()
    for dx, dy in others:
        pl.semaphore_signal(barrier, inc=1, device_id={"cp": pt.peer(dx, dy)}, device_id_type=MESH)
    pl.semaphore_wait(barrier, len(others))

    def put(src, dst, send, recv, dev):
        return pltpu.make_async_remote_copy(src, dst, send, recv, device_id={"cp": dev}, device_id_type=MESH)

    way = (1, -1)
    turn = {FAR: 0, 1: 1, -1: 2, 0: 3}

    def source(half, dx, dy):
        return o_in.at[pt.slot(dx, dy)] if half else ol.at[turn[dy], lax.rem(pt.x + dx, 2)]

    def o_copy(half, i):
        dx, dy = near[i]
        return put(source(half, dx, dy), obuf.at[my_head, highs if half else lows], o_send.at[half, i], o_recv.at[half, my_head],
                   pt.peer(dx, dy))

    def o_hop(half, dx):
        return put(source(half, dx, FAR), robuf.at[half, dx], o_send.at[half, len(near) + dx], ro_recv.at[half, dx],
                   pt.peer(0, way[dx]))

    def o_hand(half, dx):
        head = pt.head(0, -way[dx])
        return put(robuf.at[half, dx], obuf.at[head, highs if half else lows], ro_send.at[half, dx], o_recv.at[half, head],
                   pt.peer(dx, way[dx]))

    def hand_on(half):
        for dx in range(2):
            put(robuf.at[half, dx], robuf.at[half, dx], o_send.at[0, 0], ro_recv.at[half, dx], me).wait_recv()
            o_hand(half, dx).start()

    for dx in range(2):
        o_hop(1, dx).start()
    for i in range(len(near)):
        o_copy(1, i).start()

    for cp in seg_copies + q_copies:
        cp.wait()

    @pl.loop(0, n)
    def _(p):
        load(p).wait()

    pairs = Pairs(pt, n, g, scale, lambda src, half: seg_s[src, half, 0], seg_v, kvs, qs, t_sc, acc_sc)

    def send_low(dy):
        if dy == FAR:
            for dx in range(2):
                o_hop(0, dx).start()
        else:
            for i, (dx, to) in enumerate(near):
                if to == dy:
                    o_copy(0, i).start()

    def one(i, carry):
        turned = jnp.where(i == 2, -1, jnp.where(i == 3, 0, FAR - i))
        row = lax.rem(pt.y + turned + pt.side, pt.side)

        def store(u, w, val):
            ol[i, u, :, w * DH:(w + 1) * DH] = val

        pairs(row, 0, 0, pairs.begins(row, 0), store)

        @pl.when(i == 1)
        def _():
            send_low(FAR)
            hand_on(1)

        @pl.when(i == 2)
        def _():
            send_low(1)

        @pl.when(i == 3)
        def _():
            send_low(-1)
            hand_on(0)

        return carry

    lax.fori_loop(0, ng // 2, one, 0)
    send_low(0)
    obuf[my_head, 0:PC] = ol[turn[0], lax.rem(pt.x, 2)]

    for t, dy in enumerate(O_ORDER):
        for cp in w_copies(t):
            cp.wait()
        heads = [pt.head(dx, dy) for dx in range(2)]
        for dx in range(2):
            if dy == 0 and dx == 0:
                own.wait()
            else:
                for half in range(2):
                    put(ol.at[0, 0], obuf.at[heads[dx], highs if half else lows], o_send.at[0, 0], o_recv.at[half, heads[dx]],
                        me).wait_recv()
        a = jnp.concatenate([obuf[heads[0]], obuf[heads[1]]], axis=1)
        for u in range(nc):
            r = jnp.dot(a, wob[t, :, u * wn:(u + 1) * wn], preferred_element_type=jnp.float32)
            if t > 0:
                r = r + acc[:, u * wn:(u + 1) * wn]
            if t < len(O_ORDER) - 1:
                acc[:, u * wn:(u + 1) * wn] = r
            else:
                y_ref[:, u * wn:(u + 1) * wn] = r.astype(y_ref.dtype)
    for half in range(2):
        for i in range(len(near)):
            o_copy(half, i).wait_send()
        for dx in range(2):
            o_hop(half, dx).wait_send()
            o_hand(half, dx).wait_send()


def solution(mesh):
    n = mesh.shape["cp"]
    side = math.isqrt(n // 2)
    bf, f32 = jnp.bfloat16, jnp.float32
    vmem, anym = pl.BlockSpec(memory_space=pltpu.VMEM), pl.BlockSpec(memory_space=pltpu.HBM)
    dma = pltpu.SemaphoreType.DMA

    def local(x, seg, wq, wk, wv, wo):
        lq, d = x.shape
        hkv = wk.shape[1] // DH
        g = wq.shape[1] // wk.shape[1]
        gd = g * DH
        ng = 2 * side
        kv, q, segs = pl.pallas_call(
            functools.partial(_project, n, g),
            out_shape=(jax.ShapeDtypeStruct((n, 2, 2, PC, DH), bf), jax.ShapeDtypeStruct((ng, 2, g, PC, DH), bf),
                       jax.ShapeDtypeStruct((n, 2, PC), jnp.int32)),
            in_specs=[anym, vmem, anym, anym, anym],
            out_specs=(anym, anym, vmem),
            scratch_shapes=[
                pltpu.VMEM((lq, d), bf),
                pltpu.VMEM((2, side, d // side, hkv * DH), bf), pltpu.VMEM((side, d // side, hkv * gd), bf),
                pltpu.VMEM((2, lq, hkv * DH), f32), pltpu.VMEM((lq, hkv * gd), f32),
                pltpu.VMEM((n, 2, 2, PC, DH), bf), pltpu.VMEM((ng, 2, g, PC, DH), bf),
                pltpu.VMEM((ng, 2, 2, PC, DH), bf), pltpu.VMEM((ng, 2, g, PC, DH), bf),
                pltpu.VMEM((2, 2, 2, PC, DH), bf), pltpu.VMEM((2, 2, g, PC, DH), bf), pltpu.VMEM((n, 2, PC), jnp.int32),
                dma, dma((2, side)), dma((side,)), dma((ng + 2,)), dma((n,)), dma((2, 2)), dma((2, 2)), dma((2, 2)),
                dma((ng,)), dma((2 * ng,)),
                dma((ng + 2,)), dma((ng,)), dma((2, 2)), dma((2, 2)), dma((2, 2)), dma((n,)), dma((n,)), dma((n,)), dma((ng,)),
            ],
            compiler_params=pltpu.CompilerParams(collective_id=0, has_side_effects=True, vmem_limit_bytes=60 << 20),
            name="project",
        )(x, seg.reshape(1, 2, PC), wk, wv, wq)
        scale = DH ** -0.5 * math.log2(math.e)
        o = pl.pallas_call(
            functools.partial(_attend, n, g, scale),
            out_shape=jax.ShapeDtypeStruct((ng, PC, gd), bf),
            in_specs=[anym] * 3,
            out_specs=anym,
            scratch_shapes=[pltpu.SMEM((n, 2, PC), jnp.int32), pltpu.VMEM((n, 2, PC), jnp.int32),
                            pltpu.VMEM((2 * n, 2, PC, DH), bf), pltpu.VMEM((ng, g, PC, DH), bf),
                            pltpu.VMEM((ng, PC, gd), bf), pltpu.SMEM((ng,), jnp.int32)] + _pair_scratch(g) + [dma((2,)), dma, dma, dma],
            compiler_params=pltpu.CompilerParams(vmem_limit_bytes=60 << 20),
            name="attend",
        )(segs, kv, q)
        return pl.pallas_call(
            functools.partial(_combine, n, g, scale),
            out_shape=jax.ShapeDtypeStruct((lq, wo.shape[1]), bf),
            in_specs=[anym] * 5,
            out_specs=vmem,
            scratch_shapes=[pltpu.VMEM((hkv, lq, gd), bf), pltpu.VMEM((2, 2, PC, gd), bf), pltpu.VMEM((ng // 2, 2, PC, gd), bf),
                            pltpu.VMEM((side, 2 * gd, wo.shape[1]), bf), pltpu.VMEM((lq, wo.shape[1]), f32),
                            pltpu.SMEM((n, 2, PC), jnp.int32), pltpu.VMEM((n, 2, PC), jnp.int32),
                            pltpu.VMEM((n, 2, PC, DH), bf), pltpu.VMEM((ng, g, PC, DH), bf)] + _pair_scratch(g) + [
                            dma((side, 2)), dma((2, ng)), dma((2, ng)), dma((2, 2)), dma((2, 2)), dma((2,)), dma((n,)), dma((ng,))],
            compiler_params=pltpu.CompilerParams(collective_id=1, has_side_effects=True, vmem_limit_bytes=60 << 20),
            name="combine",
        )(segs, kv, q, o, wo)

    rows = P(("dp", "cp"), None)
    return jax.shard_map(local, mesh=mesh, in_specs=(rows, P(("dp", "cp")), P(), P(), P(), P()), out_specs=rows, check_vma=False)
```

```python
import functools
import math

import jax
import jax.numpy as jnp
from jax import lax
from jax.experimental import pallas as pl
from jax.experimental.pallas import tpu as pltpu
from jax.sharding import PartitionSpec as P

DH = 128
PC = 128
KB = 4
MESH = pl.DeviceIdType.MESH
NEG_INF = float("-inf")
FLOOR = -3e38


class Place:
    def __init__(self, n):
        me = lax.axis_index("cp")
        self.n, self.side = n, math.isqrt(n // 2)
        self.me = me
        self.c = lax.rem(me, 2)
        chip = me // 2
        self.x = lax.rem(chip, self.side)
        self.y = chip // self.side
        self.xin = self.x + 1 - 2 * lax.rem(self.x, 2)
        self.xcross = self.side - 1 - self.x
        self.px = lax.rem(lax.rem(self.x, 2) + self.x // 2, 2)

    def dev(self, x, y, c):
        return (y * self.side + x) * 2 + c

    def row(self, dy):
        return lax.rem(self.y + dy + self.side, self.side)

    def col(self, dx):
        return self.xin if dx else self.x

    def peer(self, dx, dy):
        return self.dev(self.col(dx), self.row(dy), self.c)

    def head(self, dx, dy):
        return lax.rem(self.px + dx, 2) * self.side + self.row(dy)

    def slot(self, dx, dy):
        return self.row(dy) * 2 + lax.rem(self.x + dx, 2)


FAR = 2
KV_ORDER = (FAR, 0, 1, -1)
Q_ORDER = (FAR, 1, -1, 0)
O_ORDER = (1, -1, FAR, 0)


def _project(n, g, x_in, seg_ref, wk, wv, wq, kv_o, q_o, segs_o, x_ref, wkvb, wqb, kvacc, qacc, kvb, qb, skv, sq, rkv, rq, segb,
             x_sem, wkv_sem, wq_sem, kv_send, kv_recv, kvf_recv, rkv_recv, rkv_send, fx_send, fs_send,
             q_send, q_recv, qf_recv, rq_recv, rq_send, seg_send, seg_recv, out_sem, qout_sem):
    pt = Place(n)
    me = pt.me
    kv_steps = [(t, dx, dy) for t, dy in enumerate(KV_ORDER) for dx in range(2)]
    q_steps = [(t, dx, dy) for t, dy in enumerate(Q_ORDER) for dx in range(2)]
    own_kv = (KV_ORDER.index(0), 0)
    own_q = (Q_ORDER.index(0), 0)
    gd = g * DH
    kr = wqb.shape[1]
    nk = wqb.shape[0]
    my_head, my_slot = pt.head(0, 0), pt.slot(0, 0)

    kv_copies = [[pltpu.make_async_copy(w.at[pl.ds(t * kr, kr)], wkvb.at[i, t], wkv_sem.at[i, t]) for i, w in enumerate((wk, wv))]
                 for t in range(nk)]
    q_copies = [pltpu.make_async_copy(wq.at[pl.ds(t * kr, kr)], wqb.at[t], wq_sem.at[t]) for t in range(nk)]
    x_copy = pltpu.make_async_copy(x_in, x_ref, x_sem)
    x_copy.start()
    for cps in kv_copies:
        for cp in cps:
            cp.start()
    for cp in q_copies:
        cp.start()

    barrier = pltpu.get_barrier_semaphore()

    @pl.loop(1, n)
    def _(i):
        pl.semaphore_signal(barrier, inc=1, device_id={"cp": lax.rem(me + i, n)}, device_id_type=MESH)

    def seg_copy(i):
        return pltpu.make_async_remote_copy(seg_ref, segb.at[pl.ds(me, 1)], seg_send.at[i], seg_recv.at[me],
                                            device_id={"cp": lax.rem(me + i, n)}, device_id_type=MESH)

    segb[pl.ds(me, 1)] = seg_ref[...]

    def put(src, dst, send, recv, dev):
        return pltpu.make_async_remote_copy(src, dst, send, recv, device_id={"cp": dev}, device_id_type=MESH)

    def kv_copy(t, dx, dy):
        return put(skv.at[pt.head(dx, dy)], kvb.at[me], kv_send.at[2 * t + dx], kv_recv.at[me], pt.peer(dx, dy))

    def q_copy(t, dx, dy):
        return put(sq.at[pt.head(dx, dy)], qb.at[my_slot], q_send.at[2 * t + dx], q_recv.at[my_slot], pt.peer(dx, dy))

    way = (1, -1)
    hops = [(half, dx) for half in range(2) for dx in range(2)]

    def kv_hop(half, dx):
        return put(skv.at[pt.head(dx, FAR), half], rkv.at[half, dx], kv_send.at[2 * half + dx if half == 0 else 2 * len(KV_ORDER) + dx],
                   rkv_recv.at[half, dx], pt.peer(0, way[half]))

    def kv_hand(half, dx):
        return put(rkv.at[half, dx], kvb.at[pt.peer(0, -way[half]), half], rkv_send.at[half, dx], kvf_recv.at[dx, half],
                   pt.peer(dx, way[half]))

    def q_hop(half, dx):
        return put(sq.at[pt.head(dx, FAR), half], rq.at[half, dx], q_send.at[2 * half + dx if half == 0 else 2 * len(Q_ORDER) + dx],
                   rq_recv.at[half, dx], pt.peer(0, way[half]))

    def q_hand(half, dx):
        return put(rq.at[half, dx], qb.at[pt.slot(0, -way[half]), half], rq_send.at[half, dx], qf_recv.at[dx, half],
                   pt.peer(dx, way[half]))

    nb = 4 * DH

    def summed(t, w, acc, c):
        cols = slice(c * nb, (c + 1) * nb)
        r = jnp.dot(x_ref[:, t * kr:(t + 1) * kr], w[:, cols], preferred_element_type=jnp.float32)
        if t > 0:
            r = r + acc[:, cols]
        if t < nk - 1:
            acc[:, cols] = r
        return r

    def kv_step(t):
        for cp in kv_copies[t]:
            cp.wait()
        for c in range(wkvb.shape[3] // nb):
            for i in range(2):
                r = summed(t, wkvb.at[i, t], kvacc.at[i], c)
                if t == nk - 1:
                    for u in range(nb // DH):
                        part = r[:, u * DH:(u + 1) * DH]
                        part = (jnp.transpose(part) if i == 1 else part).astype(jnp.bfloat16)
                        for half in range(2):
                            rows = slice(half * PC, (half + 1) * PC)
                            skv[c * (nb // DH) + u, half, i] = part[:, rows] if i == 1 else part[rows]

    def q_step(t, first, last):
        if first == 0:
            q_copies[t].wait()
        for c in range(first, last):
            r = summed(t, wqb.at[t], qacc, c)
            if t == nk - 1:
                for u in range(nb // DH):
                    col = c * (nb // DH) + u
                    part = jnp.transpose(r[:, u * DH:(u + 1) * DH]).astype(jnp.bfloat16)
                    for half in range(2):
                        sq[col // g, half, col % g] = part[:, half * PC:(half + 1) * PC]

    def send_kv(t):
        if KV_ORDER[t] == FAR:
            for hop in hops:
                kv_hop(*hop).start()
        else:
            for dx in range(2):
                if (t, dx) != own_kv:
                    kv_copy(t, dx, KV_ORDER[t]).start()

    def send_q(t):
        if Q_ORDER[t] == FAR:
            for hop in hops:
                q_hop(*hop).start()
        else:
            for dx in range(2):
                if (t, dx) != own_q:
                    q_copy(t, dx, Q_ORDER[t]).start()

    def to_cross(src, i):
        return put(kvb.at[src], kvb.at[src], fx_send.at[i], kv_recv.at[src], pt.dev(pt.xcross, pt.y, pt.c))

    def to_sibling(src, i):
        return put(kvb.at[src], kvb.at[src], fs_send.at[i], kv_recv.at[src], pt.dev(pt.x, pt.y, 1 - pt.c))

    def kv_out(src):
        return pltpu.make_async_copy(kvb.at[src], kv_o.at[src], out_sem.at[src])

    def q_out(slot):
        return pltpu.make_async_copy(qb.at[slot], q_o.at[slot], qout_sem.at[slot])

    def arrived(src):
        to_sibling(src, 0).wait_recv()

    def forward(t):
        dy = KV_ORDER[t]
        for dx in range(2):
            src = pt.peer(dx, -dy)
            if dy == FAR:
                for half in range(2):
                    put(rkv.at[half, dx], kvb.at[src, half], rkv_send.at[half, dx], kvf_recv.at[dx, half], me).wait_recv()
            elif (t, dx) != own_kv:
                arrived(src)
            to_cross(src, 2 * t + dx).start()
            to_sibling(src, 2 * t + dx).start()
            kv_out(src).start()

    def own_out():
        return pltpu.make_async_copy(skv.at[my_head], kv_o.at[me], out_sem.at[me])

    def own_q_out():
        return pltpu.make_async_copy(sq.at[my_head], q_o.at[my_slot], qout_sem.at[my_slot])

    def forward_own():
        put(skv.at[my_head], kvb.at[me], fx_send.at[2 * own_kv[0]], kv_recv.at[me], pt.dev(pt.xcross, pt.y, pt.c)).start()
        put(skv.at[my_head], kvb.at[me], fs_send.at[2 * own_kv[0]], kv_recv.at[me], pt.dev(pt.x, pt.y, 1 - pt.c)).start()
        own_out().start()

    def forward_next():
        src = pt.peer(1, 0)
        arrived(src)
        to_cross(src, 2 * own_kv[0] + 1).start()
        to_sibling(src, 2 * own_kv[0] + 1).start()
        kv_out(src).start()

    x_copy.wait()
    for t in range(nk):
        kv_step(t)
    nq = wqb.shape[2] // nb

    pl.semaphore_wait(barrier, n - 1)
    for t in range(len(KV_ORDER)):
        send_kv(t)
    forward_own()
    q_step(0, 0, nq)
    q_step(1, 0, nq)
    q_step(2, 0, nq)
    forward_next()
    for hop in hops:
        put(rkv.at[hop], rkv.at[hop], kv_send.at[0], rkv_recv.at[hop], me).wait_recv()
        kv_hand(*hop).start()
    q_step(3, 0, nq)
    own_q_out().start()
    send_q(0)
    forward(2)
    send_q(1)
    forward(3)
    send_q(2)
    forward(0)
    send_q(3)

    def mirrored(dx, dy, c):
        x = pt.side - 1 - pt.col(dx)
        return pt.dev(x, pt.row(-dy), c)

    passing = [(t, dx, KV_ORDER[t]) for t in (1, 2, 3, 0) for dx in range(2)]

    def pass_on(steps):
        for t, dx, dy in steps:
            src = mirrored(dx, dy, pt.c)
            arrived(src)
            to_sibling(src, 8 + 2 * t + dx).start()
            kv_out(src).start()

    pass_on(passing[:4])
    for hop in hops:
        put(rq.at[hop], rq.at[hop], q_send.at[0], rq_recv.at[hop], me).wait_recv()
        q_hand(*hop).start()
    pass_on(passing[4:])

    @pl.loop(1, n)
    def _(i):
        seg_copy(i).start()

    for t, dx, dy in passing:
        src = pt.dev(pt.col(dx), pt.row(-dy), 1 - pt.c)
        arrived(src)
        kv_out(src).start()
    for t, dx, dy in q_steps:
        slot = pt.slot(dx, -dy)
        if dy == FAR:
            for half in range(2):
                put(rq.at[half, dx], qb.at[slot, half], rq_send.at[half, dx], qf_recv.at[dx, half], me).wait_recv()
        elif (t, dx) != own_q:
            put(qb.at[slot], qb.at[slot], q_send.at[0], q_recv.at[slot], me).wait_recv()
        if (t, dx) != own_q:
            q_out(slot).start()
    for t, dx, dy in passing:
        src = mirrored(dx, dy, 1 - pt.c)
        arrived(src)
        kv_out(src).start()

    @pl.loop(1, n)
    def _(i):
        src = lax.rem(me + i, n)
        pltpu.make_async_remote_copy(seg_ref, segb.at[pl.ds(src, 1)], seg_send.at[i], seg_recv.at[src],
                                     device_id={"cp": src}, device_id_type=MESH).wait_recv()

    segs_o[...] = segb[...]

    @pl.loop(1, n)
    def _(i):
        seg_copy(i).wait_send()

    for hop in hops:
        kv_hop(*hop).wait_send()
        kv_hand(*hop).wait_send()
        q_hop(*hop).wait_send()
        q_hand(*hop).wait_send()
    for t, dx, dy in kv_steps:
        if dy != FAR and (t, dx) != own_kv:
            kv_copy(t, dx, dy).wait_send()
        src = pt.peer(dx, -dy)
        to_cross(src, 2 * t + dx).wait_send()
        to_sibling(src, 2 * t + dx).wait_send()
        to_sibling(src, 8 + 2 * t + dx).wait_send()
    for t, dx, dy in q_steps:
        if dy != FAR and (t, dx) != own_q:
            q_copy(t, dx, dy).wait_send()

    @pl.loop(0, n)
    def _(i):
        kv_out(i).wait()

    @pl.loop(0, n // 4)
    def _(i):
        q_out(i).wait()


class Pairs:
    def __init__(self, pt, n, g, scale, first_of, seg_v, kvs, qs, t_sc, acc_sc):
        self.pt, self.n, self.g, self.scale, self.first_of, self.seg_v, self.kvs = pt, n, g, scale, first_of, seg_v, kvs
        self.qs, self.t_sc, self.acc_sc = qs, t_sc, acc_sc

    def begins(self, row, half):
        out = []
        for u in range(2):
            src = self.pt.dev((self.pt.x // 2) * 2 + u, row, self.pt.c)
            before = jnp.where(self.seg_v[...] < self.first_of(src, half), 1.0, 0.0)
            out.append(jnp.sum(before).astype(jnp.int32))
        return out

    def __call__(self, row, half, lo, begins, store):
        pt, n, g, scale, seg_v, kvs, qs = self.pt, self.n, self.g, self.scale, self.seg_v, self.kvs, self.qs
        t_sc, acc_sc = self.t_sc, self.acc_sc
        last_piece, pieces = 2 * n - 1, kvs.shape[0]
        srcs = [pt.dev((pt.x // 2) * 2 + u, row, pt.c) for u in range(2)]
        ps = [last_piece - src if half else src for src in srcs]
        end = jnp.maximum(ps[0], ps[1])
        wide = g * PC
        acc_sc[...] = jnp.zeros_like(acc_sc)

        def queries(us):
            return jnp.concatenate([qs[2 * row + u, w] for u in us for w in range(g)], axis=1)

        def start(b):
            return jnp.minimum(lo + b * KB, pieces - KB)

        def scores(b):
            j0, js = lo + b * KB, start(b)
            k = jnp.concatenate([kvs[js + w, 0] for w in range(KB)], axis=0)
            s = jnp.dot(k, queries((0, 1)), preferred_element_type=jnp.float32) * scale
            pos = lax.broadcasted_iota(jnp.int32, (KB * PC, DH), 0) + js * PC
            tops = []
            for u in range(2):
                seen = (pos >= jnp.maximum(begins[u], j0 * PC)) & (pos < ps[u] * PC)
                for w in range(g):
                    at = slice(u * wide + w * PC, u * wide + (w + 1) * PC)
                    part = jnp.where(seen, s[:, at], NEG_INF)
                    t_sc[:, at] = part
                    tops.append(jnp.max(part, axis=0, keepdims=True))
            return jnp.concatenate(tops, axis=1)

        def step(b, carry):
            m, l, top = carry
            js = start(b)
            m_new = jnp.maximum(m, top)
            corr = jnp.exp2(m - m_new)
            p = jnp.exp2(t_sc[...] - m_new)
            l = l * corr + jnp.sum(p, axis=0, keepdims=True)
            vt = jnp.concatenate([kvs[js + w, 1] for w in range(KB)], axis=1)
            acc_sc[...] = acc_sc[...] * corr + jnp.dot(vt, p.astype(jnp.bfloat16), preferred_element_type=jnp.float32)
            return m_new, l, scores(b + 1)

        line = jnp.zeros((1, 2 * wide), jnp.float32)
        m, l, _ = lax.fori_loop(0, lax.div(end - lo + KB - 1, KB), step, (line + FLOOR, line, scores(0)))

        key = lax.broadcasted_iota(jnp.int32, (PC, PC), 0)
        query = lax.broadcasted_iota(jnp.int32, (PC, PC), 1)
        ss = [jnp.dot(kvs[ps[u], 0], queries((u,)), preferred_element_type=jnp.float32) * scale for u in range(2)]
        for u in range(2):
            at = slice(u * wide, (u + 1) * wide)
            ids = seg_v[srcs[u], pl.ds(half, 1), :]
            idb = jnp.broadcast_to(ids, (PC, PC))
            allowed = jnp.concatenate([(idb == jnp.transpose(idb)) & (key <= query)] * g, axis=1)
            keep = jnp.concatenate([ids == self.first_of(srcs[u], half)] * g, axis=1)
            s = jnp.where(allowed, ss[u], NEG_INF)
            m_old = jnp.where(keep, m[:, at], FLOOR)
            m_new = jnp.maximum(m_old, jnp.max(s, axis=0, keepdims=True))
            corr = jnp.where(keep, jnp.exp2(m_old - m_new), 0.0)
            p = jnp.exp2(s - m_new)
            ll = l[:, at] * corr + jnp.sum(p, axis=0, keepdims=True)
            acc = acc_sc[:, at] * corr + jnp.dot(kvs[ps[u], 1], p.astype(jnp.bfloat16), preferred_element_type=jnp.float32)
            o = acc * (1.0 / ll)
            for w in range(g):
                store(u, w, jnp.transpose(o[:, w * PC:(w + 1) * PC]).astype(jnp.bfloat16))


def _pair_scratch(g):
    f32 = jnp.float32
    return [pltpu.VMEM((KB * PC, 2 * g * PC), f32), pltpu.VMEM((DH, 2 * g * PC), f32)]


def _attend(n, g, scale, segs, kv, q_in, o_out, seg_s, seg_v, kvs, qs, os, lo_s, t_sc, acc_sc,
            seg_sem, kv_sem, q_sem, o_sem):
    pt = Place(n)
    last_piece = 2 * n - 1
    ng = q_in.shape[0]

    def load(p):
        owner = jnp.where(p < n, p, last_piece - p)
        return pltpu.make_async_copy(kv.at[owner, jnp.where(p < n, 0, 1)], kvs.at[p], kv_sem)

    seg_copies = [pltpu.make_async_copy(segs, seg_v, seg_sem.at[0]), pltpu.make_async_copy(segs, seg_s, seg_sem.at[1])]
    q_copies = [pltpu.make_async_copy(q_in.at[i, 1], qs.at[i], q_sem) for i in range(ng)]
    for cp in seg_copies + q_copies:
        cp.start()

    @pl.loop(0, 2 * n)
    def _(p):
        load(p).start()

    for cp in seg_copies:
        cp.wait()
    pairs = Pairs(pt, n, g, scale, lambda src, half: seg_s[src, half, 0], seg_v, kvs, qs, t_sc, acc_sc)
    for i in range(ng // 2):
        for u, at in enumerate(pairs.begins(i, 1)):
            lo_s[2 * i + u] = at
    for cp in q_copies:
        cp.wait()

    @pl.loop(0, 2 * n)
    def _(p):
        load(p).wait()

    def out(slot):
        return pltpu.make_async_copy(os.at[slot], o_out.at[slot], o_sem)

    def one(row, carry):
        def store(u, w, val):
            os[2 * row + u, :, w * DH:(w + 1) * DH] = val

        begins = [lo_s[2 * row + u] for u in range(2)]
        pairs(row, 1, lax.div(jnp.minimum(*begins), PC), begins, store)

        @pl.when(row > 0)
        def _():
            for u in range(2):
                out(2 * (row - 1) + u).start()

        return carry

    lax.fori_loop(0, ng // 2, one, 0)
    for u in range(2):
        out(ng - 2 + u).start()
    for i in range(ng):
        out(i).wait()


def _combine(n, g, scale, segs, kv, q_in, o_in, wo, y_ref, obuf, robuf, ol, wob, acc, seg_s, seg_v, kvs, qs,
             t_sc, acc_sc, w_sem, o_send, o_recv, ro_recv, ro_send, seg_sem, kv_sem, q_sem):
    pt = Place(n)
    me = pt.me
    gd = g * DH
    ng = q_in.shape[0]
    my_head, my_slot = pt.head(0, 0), pt.slot(0, 0)
    nc = 4
    wn = y_ref.shape[1] // nc
    lows, highs = pl.ds(0, PC), pl.ds(PC, PC)

    def load(p):
        return pltpu.make_async_copy(kv.at[p, 0], kvs.at[p], kv_sem.at[p])

    q_copies = [pltpu.make_async_copy(q_in.at[i, 0], qs.at[i], q_sem.at[i]) for i in range(ng)]
    seg_copies = [pltpu.make_async_copy(segs, seg_v, seg_sem.at[0]), pltpu.make_async_copy(segs, seg_s, seg_sem.at[1])]
    own = pltpu.make_async_copy(o_in.at[my_slot], obuf.at[my_head, highs], o_recv.at[1, my_head])
    for cp in seg_copies + q_copies + [own]:
        cp.start()

    @pl.loop(0, n)
    def _(p):
        load(p).start()

    def w_copies(t):
        for dx in range(2):
            h = pl.multiple_of(pt.head(dx, O_ORDER[t]) * gd, gd)
            yield pltpu.make_async_copy(wo.at[pl.ds(h, gd), :], wob.at[t, pl.ds(dx * gd, gd), :], w_sem.at[t, dx])

    for t in range(len(O_ORDER)):
        for cp in w_copies(t):
            cp.start()

    others = [(dx, dy) for dy in O_ORDER for dx in range(2) if (dx, dy) != (0, 0)]
    near = [s for s in others if s[1] != FAR]
    barrier = pltpu.get_barrier_semaphore()
    for dx, dy in others:
        pl.semaphore_signal(barrier, inc=1, device_id={"cp": pt.peer(dx, dy)}, device_id_type=MESH)
    pl.semaphore_wait(barrier, len(others))

    def put(src, dst, send, recv, dev):
        return pltpu.make_async_remote_copy(src, dst, send, recv, device_id={"cp": dev}, device_id_type=MESH)

    way = (1, -1)
    turn = {FAR: 0, 1: 1, -1: 2, 0: 3}

    def source(half, dx, dy):
        return o_in.at[pt.slot(dx, dy)] if half else ol.at[turn[dy], lax.rem(pt.x + dx, 2)]

    def o_copy(half, i):
        dx, dy = near[i]
        return put(source(half, dx, dy), obuf.at[my_head, highs if half else lows], o_send.at[half, i], o_recv.at[half, my_head],
                   pt.peer(dx, dy))

    def o_hop(half, dx):
        return put(source(half, dx, FAR), robuf.at[half, dx], o_send.at[half, len(near) + dx], ro_recv.at[half, dx],
                   pt.peer(0, way[dx]))

    def o_hand(half, dx):
        head = pt.head(0, -way[dx])
        return put(robuf.at[half, dx], obuf.at[head, highs if half else lows], ro_send.at[half, dx], o_recv.at[half, head],
                   pt.peer(dx, way[dx]))

    def hand_on(half):
        for dx in range(2):
            put(robuf.at[half, dx], robuf.at[half, dx], o_send.at[0, 0], ro_recv.at[half, dx], me).wait_recv()
            o_hand(half, dx).start()

    for dx in range(2):
        o_hop(1, dx).start()
    for i in range(len(near)):
        o_copy(1, i).start()

    for cp in seg_copies + q_copies:
        cp.wait()

    @pl.loop(0, n)
    def _(p):
        load(p).wait()

    pairs = Pairs(pt, n, g, scale, lambda src, half: seg_s[src, half, 0], seg_v, kvs, qs, t_sc, acc_sc)

    def send_low(dy):
        if dy == FAR:
            for dx in range(2):
                o_hop(0, dx).start()
        else:
            for i, (dx, to) in enumerate(near):
                if to == dy:
                    o_copy(0, i).start()

    def one(i, carry):
        turned = jnp.where(i == 2, -1, jnp.where(i == 3, 0, FAR - i))
        row = lax.rem(pt.y + turned + pt.side, pt.side)

        def store(u, w, val):
            ol[i, u, :, w * DH:(w + 1) * DH] = val

        pairs(row, 0, 0, pairs.begins(row, 0), store)

        @pl.when(i == 1)
        def _():
            send_low(FAR)
            hand_on(1)

        @pl.when(i == 2)
        def _():
            send_low(1)

        @pl.when(i == 3)
        def _():
            send_low(-1)
            hand_on(0)

        return carry

    lax.fori_loop(0, ng // 2, one, 0)
    send_low(0)
    obuf[my_head, 0:PC] = ol[turn[0], lax.rem(pt.x, 2)]

    for t, dy in enumerate(O_ORDER):
        for cp in w_copies(t):
            cp.wait()
        heads = [pt.head(dx, dy) for dx in range(2)]
        for dx in range(2):
            if dy == 0 and dx == 0:
                own.wait()
            else:
                for half in range(2):
                    put(ol.at[0, 0], obuf.at[heads[dx], highs if half else lows], o_send.at[0, 0], o_recv.at[half, heads[dx]],
                        me).wait_recv()
        a = jnp.concatenate([obuf[heads[0]], obuf[heads[1]]], axis=1)
        for u in range(nc):
            r = jnp.dot(a, wob[t, :, u * wn:(u + 1) * wn], preferred_element_type=jnp.float32)
            if t > 0:
                r = r + acc[:, u * wn:(u + 1) * wn]
            if t < len(O_ORDER) - 1:
                acc[:, u * wn:(u + 1) * wn] = r
            else:
                y_ref[:, u * wn:(u + 1) * wn] = r.astype(y_ref.dtype)
    for half in range(2):
        for i in range(len(near)):
            o_copy(half, i).wait_send()
        for dx in range(2):
            o_hop(half, dx).wait_send()
            o_hand(half, dx).wait_send()


def solution(mesh):
    n = mesh.shape["cp"]
    side = math.isqrt(n // 2)
    bf, f32 = jnp.bfloat16, jnp.float32
    vmem, anym = pl.BlockSpec(memory_space=pltpu.VMEM), pl.BlockSpec(memory_space=pltpu.HBM)
    dma = pltpu.SemaphoreType.DMA

    def local(x, seg, wq, wk, wv, wo):
        lq, d = x.shape
        hkv = wk.shape[1] // DH
        g = wq.shape[1] // wk.shape[1]
        gd = g * DH
        ng = 2 * side
        kv, q, segs = pl.pallas_call(
            functools.partial(_project, n, g),
            out_shape=(jax.ShapeDtypeStruct((n, 2, 2, PC, DH), bf), jax.ShapeDtypeStruct((ng, 2, g, PC, DH), bf),
                       jax.ShapeDtypeStruct((n, 2, PC), jnp.int32)),
            in_specs=[anym, vmem, anym, anym, anym],
            out_specs=(anym, anym, vmem),
            scratch_shapes=[
                pltpu.VMEM((lq, d), bf),
                pltpu.VMEM((2, side, d // side, hkv * DH), bf), pltpu.VMEM((side, d // side, hkv * gd), bf),
                pltpu.VMEM((2, lq, hkv * DH), f32), pltpu.VMEM((lq, hkv * gd), f32),
                pltpu.VMEM((n, 2, 2, PC, DH), bf), pltpu.VMEM((ng, 2, g, PC, DH), bf),
                pltpu.VMEM((ng, 2, 2, PC, DH), bf), pltpu.VMEM((ng, 2, g, PC, DH), bf),
                pltpu.VMEM((2, 2, 2, PC, DH), bf), pltpu.VMEM((2, 2, g, PC, DH), bf), pltpu.VMEM((n, 2, PC), jnp.int32),
                dma, dma((2, side)), dma((side,)), dma((ng + 2,)), dma((n,)), dma((2, 2)), dma((2, 2)), dma((2, 2)),
                dma((ng,)), dma((2 * ng,)),
                dma((ng + 2,)), dma((ng,)), dma((2, 2)), dma((2, 2)), dma((2, 2)), dma((n,)), dma((n,)), dma((n,)), dma((ng,)),
            ],
            compiler_params=pltpu.CompilerParams(collective_id=0, has_side_effects=True, vmem_limit_bytes=60 << 20),
            name="project",
        )(x, seg.reshape(1, 2, PC), wk, wv, wq)
        scale = DH ** -0.5 * math.log2(math.e)
        o = pl.pallas_call(
            functools.partial(_attend, n, g, scale),
            out_shape=jax.ShapeDtypeStruct((ng, PC, gd), bf),
            in_specs=[anym] * 3,
            out_specs=anym,
            scratch_shapes=[pltpu.SMEM((n, 2, PC), jnp.int32), pltpu.VMEM((n, 2, PC), jnp.int32),
                            pltpu.VMEM((2 * n, 2, PC, DH), bf), pltpu.VMEM((ng, g, PC, DH), bf),
                            pltpu.VMEM((ng, PC, gd), bf), pltpu.SMEM((ng,), jnp.int32)] + _pair_scratch(g) + [dma((2,)), dma, dma, dma],
            compiler_params=pltpu.CompilerParams(vmem_limit_bytes=60 << 20),
            name="attend",
        )(segs, kv, q)
        return pl.pallas_call(
            functools.partial(_combine, n, g, scale),
            out_shape=jax.ShapeDtypeStruct((lq, wo.shape[1]), bf),
            in_specs=[anym] * 5,
            out_specs=vmem,
            scratch_shapes=[pltpu.VMEM((hkv, lq, gd), bf), pltpu.VMEM((2, 2, PC, gd), bf), pltpu.VMEM((ng // 2, 2, PC, gd), bf),
                            pltpu.VMEM((side, 2 * gd, wo.shape[1]), bf), pltpu.VMEM((lq, wo.shape[1]), f32),
                            pltpu.SMEM((n, 2, PC), jnp.int32), pltpu.VMEM((n, 2, PC), jnp.int32),
                            pltpu.VMEM((n, 2, PC, DH), bf), pltpu.VMEM((ng, g, PC, DH), bf)] + _pair_scratch(g) + [
                            dma((side, 2)), dma((2, ng)), dma((2, ng)), dma((2, 2)), dma((2, 2)), dma((2,)), dma((n,)), dma((ng,))],
            compiler_params=pltpu.CompilerParams(collective_id=1, has_side_effects=True, vmem_limit_bytes=60 << 20),
            name="combine",
        )(segs, kv, q, o, wo)

    rows = P(("dp", "cp"), None)
    return jax.shard_map(local, mesh=mesh, in_specs=(rows, P(("dp", "cp")), P(), P(), P(), P()), out_specs=rows, check_vma=False)
```

```python
import functools
import math

import jax
import jax.numpy as jnp
from jax import lax
from jax.experimental import pallas as pl
from jax.experimental.pallas import tpu as pltpu
from jax.sharding import PartitionSpec as P

DH = 128
PC = 128
KB = 4
MESH = pl.DeviceIdType.MESH
NEG_INF = float("-inf")
FLOOR = -3e38


class Place:
    def __init__(self, n):
        me = lax.axis_index("cp")
        self.n, self.side = n, math.isqrt(n // 2)
        self.me = me
        self.c = lax.rem(me, 2)
        chip = me // 2
        self.x = lax.rem(chip, self.side)
        self.y = chip // self.side
        self.xin = self.x + 1 - 2 * lax.rem(self.x, 2)
        self.xcross = self.side - 1 - self.x
        self.px = lax.rem(lax.rem(self.x, 2) + self.x // 2, 2)

    def dev(self, x, y, c):
        return (y * self.side + x) * 2 + c

    def row(self, dy):
        return lax.rem(self.y + dy + self.side, self.side)

    def col(self, dx):
        return self.xin if dx else self.x

    def peer(self, dx, dy):
        return self.dev(self.col(dx), self.row(dy), self.c)

    def head(self, dx, dy):
        return lax.rem(self.px + dx, 2) * self.side + self.row(dy)

    def slot(self, dx, dy):
        return self.row(dy) * 2 + lax.rem(self.x + dx, 2)


FAR = 2
KV_ORDER = (FAR, 0, 1, -1)
Q_ORDER = (FAR, 1, -1, 0)
O_ORDER = (1, -1, FAR, 0)


def _project(n, g, x_in, seg_ref, wk, wv, wq, kv_o, q_o, segs_o, x_ref, wkvb, wqb, kvacc, qacc, kvb, qb, skv, sq, rkv, rq, segb,
             x_sem, wkv_sem, wq_sem, kv_send, kv_recv, kvf_recv, rkv_recv, rkv_send, fx_send, fs_send,
             q_send, q_recv, qf_recv, rq_recv, rq_send, seg_send, seg_recv, out_sem, qout_sem):
    pt = Place(n)
    me = pt.me
    kv_steps = [(t, dx, dy) for t, dy in enumerate(KV_ORDER) for dx in range(2)]
    q_steps = [(t, dx, dy) for t, dy in enumerate(Q_ORDER) for dx in range(2)]
    own_kv = (KV_ORDER.index(0), 0)
    own_q = (Q_ORDER.index(0), 0)
    gd = g * DH
    kr = wqb.shape[1]
    nk = wqb.shape[0]
    my_head, my_slot = pt.head(0, 0), pt.slot(0, 0)

    kv_copies = [[pltpu.make_async_copy(w.at[pl.ds(t * kr, kr)], wkvb.at[i, t], wkv_sem.at[i, t]) for i, w in enumerate((wk, wv))]
                 for t in range(nk)]
    q_copies = [pltpu.make_async_copy(wq.at[pl.ds(t * kr, kr)], wqb.at[t], wq_sem.at[t]) for t in range(nk)]
    x_copy = pltpu.make_async_copy(x_in, x_ref, x_sem)
    x_copy.start()
    for cps in kv_copies:
        for cp in cps:
            cp.start()
    for cp in q_copies:
        cp.start()

    barrier = pltpu.get_barrier_semaphore()

    @pl.loop(1, n)
    def _(i):
        pl.semaphore_signal(barrier, inc=1, device_id={"cp": lax.rem(me + i, n)}, device_id_type=MESH)

    def seg_copy(i):
        return pltpu.make_async_remote_copy(seg_ref, segb.at[pl.ds(me, 1)], seg_send.at[i], seg_recv.at[me],
                                            device_id={"cp": lax.rem(me + i, n)}, device_id_type=MESH)

    segb[pl.ds(me, 1)] = seg_ref[...]

    def put(src, dst, send, recv, dev):
        return pltpu.make_async_remote_copy(src, dst, send, recv, device_id={"cp": dev}, device_id_type=MESH)

    def kv_copy(t, dx, dy):
        return put(skv.at[pt.head(dx, dy)], kvb.at[me], kv_send.at[2 * t + dx], kv_recv.at[me], pt.peer(dx, dy))

    def q_copy(t, dx, dy):
        return put(sq.at[pt.head(dx, dy)], qb.at[my_slot], q_send.at[2 * t + dx], q_recv.at[my_slot], pt.peer(dx, dy))

    way = (1, -1)
    hops = [(half, dx) for half in range(2) for dx in range(2)]

    def kv_hop(half, dx):
        return put(skv.at[pt.head(dx, FAR), half], rkv.at[half, dx], kv_send.at[2 * half + dx if half == 0 else 2 * len(KV_ORDER) + dx],
                   rkv_recv.at[half, dx], pt.peer(0, way[half]))

    def kv_hand(half, dx):
        return put(rkv.at[half, dx], kvb.at[pt.peer(0, -way[half]), half], rkv_send.at[half, dx], kvf_recv.at[dx, half],
                   pt.peer(dx, way[half]))

    def q_hop(half, dx):
        return put(sq.at[pt.head(dx, FAR), half], rq.at[half, dx], q_send.at[2 * half + dx if half == 0 else 2 * len(Q_ORDER) + dx],
                   rq_recv.at[half, dx], pt.peer(0, way[half]))

    def q_hand(half, dx):
        return put(rq.at[half, dx], qb.at[pt.slot(0, -way[half]), half], rq_send.at[half, dx], qf_recv.at[dx, half],
                   pt.peer(dx, way[half]))

    nb = 4 * DH

    def summed(t, w, acc, c):
        cols = slice(c * nb, (c + 1) * nb)
        r = jnp.dot(x_ref[:, t * kr:(t + 1) * kr], w[:, cols], preferred_element_type=jnp.float32)
        if t > 0:
            r = r + acc[:, cols]
        if t < nk - 1:
            acc[:, cols] = r
        return r

    def kv_step(t):
        for cp in kv_copies[t]:
            cp.wait()
        for c in range(wkvb.shape[3] // nb):
            for i in range(2):
                r = summed(t, wkvb.at[i, t], kvacc.at[i], c)
                if t == nk - 1:
                    for u in range(nb // DH):
                        part = r[:, u * DH:(u + 1) * DH]
                        part = (jnp.transpose(part) if i == 1 else part).astype(jnp.bfloat16)
                        for half in range(2):
                            rows = slice(half * PC, (half + 1) * PC)
                            skv[c * (nb // DH) + u, half, i] = part[:, rows] if i == 1 else part[rows]

    def q_step(t, first, last):
        if first == 0:
            q_copies[t].wait()
        for c in range(first, last):
            r = summed(t, wqb.at[t], qacc, c)
            if t == nk - 1:
                for u in range(nb // DH):
                    col = c * (nb // DH) + u
                    part = jnp.transpose(r[:, u * DH:(u + 1) * DH]).astype(jnp.bfloat16)
                    for half in range(2):
                        sq[col // g, half, col % g] = part[:, half * PC:(half + 1) * PC]

    def send_kv(t):
        if KV_ORDER[t] == FAR:
            for hop in hops:
                kv_hop(*hop).start()
        else:
            for dx in range(2):
                if (t, dx) != own_kv:
                    kv_copy(t, dx, KV_ORDER[t]).start()

    def send_q(t):
        if Q_ORDER[t] == FAR:
            for hop in hops:
                q_hop(*hop).start()
        else:
            for dx in range(2):
                if (t, dx) != own_q:
                    q_copy(t, dx, Q_ORDER[t]).start()

    def to_cross(src, i):
        return put(kvb.at[src], kvb.at[src], fx_send.at[i], kv_recv.at[src], pt.dev(pt.xcross, pt.y, pt.c))

    def to_sibling(src, i):
        return put(kvb.at[src], kvb.at[src], fs_send.at[i], kv_recv.at[src], pt.dev(pt.x, pt.y, 1 - pt.c))

    def kv_out(src):
        return pltpu.make_async_copy(kvb.at[src], kv_o.at[src], out_sem.at[src])

    def q_out(slot):
        return pltpu.make_async_copy(qb.at[slot], q_o.at[slot], qout_sem.at[slot])

    def arrived(src):
        to_sibling(src, 0).wait_recv()

    def forward(t):
        dy = KV_ORDER[t]
        for dx in range(2):
            src = pt.peer(dx, -dy)
            if dy == FAR:
                for half in range(2):
                    put(rkv.at[half, dx], kvb.at[src, half], rkv_send.at[half, dx], kvf_recv.at[dx, half], me).wait_recv()
            elif (t, dx) != own_kv:
                arrived(src)
            to_cross(src, 2 * t + dx).start()
            to_sibling(src, 2 * t + dx).start()
            kv_out(src).start()

    def own_out():
        return pltpu.make_async_copy(skv.at[my_head], kv_o.at[me], out_sem.at[me])

    def own_q_out():
        return pltpu.make_async_copy(sq.at[my_head], q_o.at[my_slot], qout_sem.at[my_slot])

    def forward_own():
        put(skv.at[my_head], kvb.at[me], fx_send.at[2 * own_kv[0]], kv_recv.at[me], pt.dev(pt.xcross, pt.y, pt.c)).start()
        put(skv.at[my_head], kvb.at[me], fs_send.at[2 * own_kv[0]], kv_recv.at[me], pt.dev(pt.x, pt.y, 1 - pt.c)).start()
        own_out().start()

    def forward_next():
        src = pt.peer(1, 0)
        arrived(src)
        to_cross(src, 2 * own_kv[0] + 1).start()
        to_sibling(src, 2 * own_kv[0] + 1).start()
        kv_out(src).start()

    x_copy.wait()
    for t in range(nk):
        kv_step(t)
    nq = wqb.shape[2] // nb

    pl.semaphore_wait(barrier, n - 1)
    for t in range(len(KV_ORDER)):
        send_kv(t)
    forward_own()

    @pl.loop(1, n)
    def _(i):
        seg_copy(i).start()

    q_step(0, 0, nq)
    q_step(1, 0, nq)
    q_step(2, 0, nq)
    forward_next()
    for hop in hops:
        put(rkv.at[hop], rkv.at[hop], kv_send.at[0], rkv_recv.at[hop], me).wait_recv()
        kv_hand(*hop).start()
    q_step(3, 0, nq)
    own_q_out().start()
    send_q(0)
    forward(2)
    send_q(1)
    forward(3)
    send_q(2)
    forward(0)
    send_q(3)

    def mirrored(dx, dy, c):
        x = pt.side - 1 - pt.col(dx)
        return pt.dev(x, pt.row(-dy), c)

    passing = [(t, dx, KV_ORDER[t]) for t in (1, 2, 3, 0) for dx in range(2)]

    def pass_on(steps):
        for t, dx, dy in steps:
            src = mirrored(dx, dy, pt.c)
            arrived(src)
            to_sibling(src, 8 + 2 * t + dx).start()
            kv_out(src).start()

    pass_on(passing[:4])
    for hop in hops:
        put(rq.at[hop], rq.at[hop], q_send.at[0], rq_recv.at[hop], me).wait_recv()
        q_hand(*hop).start()
    pass_on(passing[4:])

    for t, dx, dy in passing:
        src = pt.dev(pt.col(dx), pt.row(-dy), 1 - pt.c)
        arrived(src)
        kv_out(src).start()
    for t, dx, dy in q_steps:
        slot = pt.slot(dx, -dy)
        if dy == FAR:
            for half in range(2):
                put(rq.at[half, dx], qb.at[slot, half], rq_send.at[half, dx], qf_recv.at[dx, half], me).wait_recv()
        elif (t, dx) != own_q:
            put(qb.at[slot], qb.at[slot], q_send.at[0], q_recv.at[slot], me).wait_recv()
        if (t, dx) != own_q:
            q_out(slot).start()
    for t, dx, dy in passing:
        src = mirrored(dx, dy, 1 - pt.c)
        arrived(src)
        kv_out(src).start()

    @pl.loop(1, n)
    def _(i):
        src = lax.rem(me + i, n)
        pltpu.make_async_remote_copy(seg_ref, segb.at[pl.ds(src, 1)], seg_send.at[i], seg_recv.at[src],
                                     device_id={"cp": src}, device_id_type=MESH).wait_recv()

    segs_o[...] = segb[...]

    @pl.loop(1, n)
    def _(i):
        seg_copy(i).wait_send()

    for hop in hops:
        kv_hop(*hop).wait_send()
        kv_hand(*hop).wait_send()
        q_hop(*hop).wait_send()
        q_hand(*hop).wait_send()
    for t, dx, dy in kv_steps:
        if dy != FAR and (t, dx) != own_kv:
            kv_copy(t, dx, dy).wait_send()
        src = pt.peer(dx, -dy)
        to_cross(src, 2 * t + dx).wait_send()
        to_sibling(src, 2 * t + dx).wait_send()
        to_sibling(src, 8 + 2 * t + dx).wait_send()
    for t, dx, dy in q_steps:
        if dy != FAR and (t, dx) != own_q:
            q_copy(t, dx, dy).wait_send()

    @pl.loop(0, n)
    def _(i):
        kv_out(i).wait()

    @pl.loop(0, n // 4)
    def _(i):
        q_out(i).wait()


class Pairs:
    def __init__(self, pt, n, g, scale, first_of, seg_v, kvs, qs, t_sc, acc_sc):
        self.pt, self.n, self.g, self.scale, self.first_of, self.seg_v, self.kvs = pt, n, g, scale, first_of, seg_v, kvs
        self.qs, self.t_sc, self.acc_sc = qs, t_sc, acc_sc

    def begins(self, row, half):
        out = []
        for u in range(2):
            src = self.pt.dev((self.pt.x // 2) * 2 + u, row, self.pt.c)
            before = jnp.where(self.seg_v[...] < self.first_of(src, half), 1.0, 0.0)
            out.append(jnp.sum(before).astype(jnp.int32))
        return out

    def __call__(self, row, half, lo, begins, store):
        pt, n, g, scale, seg_v, kvs, qs = self.pt, self.n, self.g, self.scale, self.seg_v, self.kvs, self.qs
        t_sc, acc_sc = self.t_sc, self.acc_sc
        last_piece, pieces = 2 * n - 1, kvs.shape[0]
        srcs = [pt.dev((pt.x // 2) * 2 + u, row, pt.c) for u in range(2)]
        ps = [last_piece - src if half else src for src in srcs]
        end = jnp.maximum(ps[0], ps[1])
        wide = g * PC
        acc_sc[...] = jnp.zeros_like(acc_sc)

        def queries(us):
            return jnp.concatenate([qs[2 * row + u, w] for u in us for w in range(g)], axis=1)

        def start(b):
            return jnp.minimum(lo + b * KB, pieces - KB)

        def scores(b):
            j0, js = lo + b * KB, start(b)
            k = jnp.concatenate([kvs[js + w, 0] for w in range(KB)], axis=0)
            s = jnp.dot(k, queries((0, 1)), preferred_element_type=jnp.float32) * scale
            pos = lax.broadcasted_iota(jnp.int32, (KB * PC, DH), 0) + js * PC
            tops = []
            for u in range(2):
                seen = (pos >= jnp.maximum(begins[u], j0 * PC)) & (pos < ps[u] * PC)
                for w in range(g):
                    at = slice(u * wide + w * PC, u * wide + (w + 1) * PC)
                    part = jnp.where(seen, s[:, at], NEG_INF)
                    t_sc[:, at] = part
                    tops.append(jnp.max(part, axis=0, keepdims=True))
            return jnp.concatenate(tops, axis=1)

        def step(b, carry):
            m, l, top = carry
            js = start(b)
            m_new = jnp.maximum(m, top)
            corr = jnp.exp2(m - m_new)
            p = jnp.exp2(t_sc[...] - m_new)
            l = l * corr + jnp.sum(p, axis=0, keepdims=True)
            vt = jnp.concatenate([kvs[js + w, 1] for w in range(KB)], axis=1)
            acc_sc[...] = acc_sc[...] * corr + jnp.dot(vt, p.astype(jnp.bfloat16), preferred_element_type=jnp.float32)
            return m_new, l, scores(b + 1)

        line = jnp.zeros((1, 2 * wide), jnp.float32)
        m, l, _ = lax.fori_loop(0, lax.div(end - lo + KB - 1, KB), step, (line + FLOOR, line, scores(0)))

        key = lax.broadcasted_iota(jnp.int32, (PC, PC), 0)
        query = lax.broadcasted_iota(jnp.int32, (PC, PC), 1)
        ss = [jnp.dot(kvs[ps[u], 0], queries((u,)), preferred_element_type=jnp.float32) * scale for u in range(2)]
        for u in range(2):
            at = slice(u * wide, (u + 1) * wide)
            ids = seg_v[srcs[u], pl.ds(half, 1), :]
            idb = jnp.broadcast_to(ids, (PC, PC))
            allowed = jnp.concatenate([(idb == jnp.transpose(idb)) & (key <= query)] * g, axis=1)
            keep = jnp.concatenate([ids == self.first_of(srcs[u], half)] * g, axis=1)
            s = jnp.where(allowed, ss[u], NEG_INF)
            m_old = jnp.where(keep, m[:, at], FLOOR)
            m_new = jnp.maximum(m_old, jnp.max(s, axis=0, keepdims=True))
            corr = jnp.where(keep, jnp.exp2(m_old - m_new), 0.0)
            p = jnp.exp2(s - m_new)
            ll = l[:, at] * corr + jnp.sum(p, axis=0, keepdims=True)
            acc = acc_sc[:, at] * corr + jnp.dot(kvs[ps[u], 1], p.astype(jnp.bfloat16), preferred_element_type=jnp.float32)
            o = acc * (1.0 / ll)
            for w in range(g):
                store(u, w, jnp.transpose(o[:, w * PC:(w + 1) * PC]).astype(jnp.bfloat16))


def _pair_scratch(g):
    f32 = jnp.float32
    return [pltpu.VMEM((KB * PC, 2 * g * PC), f32), pltpu.VMEM((DH, 2 * g * PC), f32)]


def _attend(n, g, scale, segs, kv, q_in, o_out, seg_s, seg_v, kvs, qs, os, lo_s, t_sc, acc_sc,
            seg_sem, kv_sem, q_sem, o_sem):
    pt = Place(n)
    last_piece = 2 * n - 1
    ng = q_in.shape[0]

    def load(p):
        owner = jnp.where(p < n, p, last_piece - p)
        return pltpu.make_async_copy(kv.at[owner, jnp.where(p < n, 0, 1)], kvs.at[p], kv_sem)

    seg_copies = [pltpu.make_async_copy(segs, seg_v, seg_sem.at[0]), pltpu.make_async_copy(segs, seg_s, seg_sem.at[1])]
    q_copies = [pltpu.make_async_copy(q_in.at[i, 1], qs.at[i], q_sem) for i in range(ng)]
    for cp in seg_copies + q_copies:
        cp.start()

    @pl.loop(0, 2 * n)
    def _(p):
        load(p).start()

    for cp in seg_copies:
        cp.wait()
    pairs = Pairs(pt, n, g, scale, lambda src, half: seg_s[src, half, 0], seg_v, kvs, qs, t_sc, acc_sc)
    for i in range(ng // 2):
        for u, at in enumerate(pairs.begins(i, 1)):
            lo_s[2 * i + u] = at
    for cp in q_copies:
        cp.wait()

    @pl.loop(0, 2 * n)
    def _(p):
        load(p).wait()

    def out(slot):
        return pltpu.make_async_copy(os.at[slot], o_out.at[slot], o_sem)

    def one(row, carry):
        def store(u, w, val):
            os[2 * row + u, :, w * DH:(w + 1) * DH] = val

        begins = [lo_s[2 * row + u] for u in range(2)]
        pairs(row, 1, lax.div(jnp.minimum(*begins), PC), begins, store)

        @pl.when(row > 0)
        def _():
            for u in range(2):
                out(2 * (row - 1) + u).start()

        return carry

    lax.fori_loop(0, ng // 2, one, 0)
    for u in range(2):
        out(ng - 2 + u).start()
    for i in range(ng):
        out(i).wait()


def _combine(n, g, scale, segs, kv, q_in, o_in, wo, y_ref, obuf, robuf, ol, wob, acc, seg_s, seg_v, kvs, qs,
             t_sc, acc_sc, w_sem, o_send, o_recv, ro_recv, ro_send, seg_sem, kv_sem, q_sem):
    pt = Place(n)
    me = pt.me
    gd = g * DH
    ng = q_in.shape[0]
    my_head, my_slot = pt.head(0, 0), pt.slot(0, 0)
    nc = 4
    wn = y_ref.shape[1] // nc
    lows, highs = pl.ds(0, PC), pl.ds(PC, PC)

    def load(p):
        return pltpu.make_async_copy(kv.at[p, 0], kvs.at[p], kv_sem.at[p])

    q_copies = [pltpu.make_async_copy(q_in.at[i, 0], qs.at[i], q_sem.at[i]) for i in range(ng)]
    seg_copies = [pltpu.make_async_copy(segs, seg_v, seg_sem.at[0]), pltpu.make_async_copy(segs, seg_s, seg_sem.at[1])]
    own = pltpu.make_async_copy(o_in.at[my_slot], obuf.at[my_head, highs], o_recv.at[1, my_head])
    for cp in seg_copies + q_copies + [own]:
        cp.start()

    @pl.loop(0, n)
    def _(p):
        load(p).start()

    def w_copies(t):
        for dx in range(2):
            h = pl.multiple_of(pt.head(dx, O_ORDER[t]) * gd, gd)
            yield pltpu.make_async_copy(wo.at[pl.ds(h, gd), :], wob.at[t, pl.ds(dx * gd, gd), :], w_sem.at[t, dx])

    for t in range(len(O_ORDER)):
        for cp in w_copies(t):
            cp.start()

    others = [(dx, dy) for dy in O_ORDER for dx in range(2) if (dx, dy) != (0, 0)]
    near = [s for s in others if s[1] != FAR]
    barrier = pltpu.get_barrier_semaphore()
    for dx, dy in others:
        pl.semaphore_signal(barrier, inc=1, device_id={"cp": pt.peer(dx, dy)}, device_id_type=MESH)
    pl.semaphore_wait(barrier, len(others))

    def put(src, dst, send, recv, dev):
        return pltpu.make_async_remote_copy(src, dst, send, recv, device_id={"cp": dev}, device_id_type=MESH)

    way = (1, -1)
    turn = {FAR: 0, 1: 1, -1: 2, 0: 3}

    def source(half, dx, dy):
        return o_in.at[pt.slot(dx, dy)] if half else ol.at[turn[dy], lax.rem(pt.x + dx, 2)]

    def o_copy(half, i):
        dx, dy = near[i]
        return put(source(half, dx, dy), obuf.at[my_head, highs if half else lows], o_send.at[half, i], o_recv.at[half, my_head],
                   pt.peer(dx, dy))

    def o_hop(half, dx):
        return put(source(half, dx, FAR), robuf.at[half, dx], o_send.at[half, len(near) + dx], ro_recv.at[half, dx],
                   pt.peer(0, way[dx]))

    def o_hand(half, dx):
        head = pt.head(0, -way[dx])
        return put(robuf.at[half, dx], obuf.at[head, highs if half else lows], ro_send.at[half, dx], o_recv.at[half, head],
                   pt.peer(dx, way[dx]))

    def hand_on(half):
        for dx in range(2):
            put(robuf.at[half, dx], robuf.at[half, dx], o_send.at[0, 0], ro_recv.at[half, dx], me).wait_recv()
            o_hand(half, dx).start()

    for dx in range(2):
        o_hop(1, dx).start()
    for i in range(len(near)):
        o_copy(1, i).start()

    for cp in seg_copies + q_copies:
        cp.wait()

    @pl.loop(0, n)
    def _(p):
        load(p).wait()

    pairs = Pairs(pt, n, g, scale, lambda src, half: seg_s[src, half, 0], seg_v, kvs, qs, t_sc, acc_sc)

    def send_low(dy):
        if dy == FAR:
            for dx in range(2):
                o_hop(0, dx).start()
        else:
            for i, (dx, to) in enumerate(near):
                if to == dy:
                    o_copy(0, i).start()

    def one(i, carry):
        turned = jnp.where(i == 2, -1, jnp.where(i == 3, 0, FAR - i))
        row = lax.rem(pt.y + turned + pt.side, pt.side)

        def store(u, w, val):
            ol[i, u, :, w * DH:(w + 1) * DH] = val

        pairs(row, 0, 0, pairs.begins(row, 0), store)

        @pl.when(i == 1)
        def _():
            send_low(FAR)
            hand_on(1)

        @pl.when(i == 2)
        def _():
            send_low(1)

        @pl.when(i == 3)
        def _():
            send_low(-1)
            hand_on(0)

        return carry

    lax.fori_loop(0, ng // 2, one, 0)
    send_low(0)
    obuf[my_head, 0:PC] = ol[turn[0], lax.rem(pt.x, 2)]

    for t, dy in enumerate(O_ORDER):
        for cp in w_copies(t):
            cp.wait()
        heads = [pt.head(dx, dy) for dx in range(2)]
        for dx in range(2):
            if dy == 0 and dx == 0:
                own.wait()
            else:
                for half in range(2):
                    put(ol.at[0, 0], obuf.at[heads[dx], highs if half else lows], o_send.at[0, 0], o_recv.at[half, heads[dx]],
                        me).wait_recv()
        a = jnp.concatenate([obuf[heads[0]], obuf[heads[1]]], axis=1)
        for u in range(nc):
            r = jnp.dot(a, wob[t, :, u * wn:(u + 1) * wn], preferred_element_type=jnp.float32)
            if t > 0:
                r = r + acc[:, u * wn:(u + 1) * wn]
            if t < len(O_ORDER) - 1:
                acc[:, u * wn:(u + 1) * wn] = r
            else:
                y_ref[:, u * wn:(u + 1) * wn] = r.astype(y_ref.dtype)
    for half in range(2):
        for i in range(len(near)):
            o_copy(half, i).wait_send()
        for dx in range(2):
            o_hop(half, dx).wait_send()
            o_hand(half, dx).wait_send()


def solution(mesh):
    n = mesh.shape["cp"]
    side = math.isqrt(n // 2)
    bf, f32 = jnp.bfloat16, jnp.float32
    vmem, anym = pl.BlockSpec(memory_space=pltpu.VMEM), pl.BlockSpec(memory_space=pltpu.HBM)
    dma = pltpu.SemaphoreType.DMA

    def local(x, seg, wq, wk, wv, wo):
        lq, d = x.shape
        hkv = wk.shape[1] // DH
        g = wq.shape[1] // wk.shape[1]
        gd = g * DH
        ng = 2 * side
        kv, q, segs = pl.pallas_call(
            functools.partial(_project, n, g),
            out_shape=(jax.ShapeDtypeStruct((n, 2, 2, PC, DH), bf), jax.ShapeDtypeStruct((ng, 2, g, PC, DH), bf),
                       jax.ShapeDtypeStruct((n, 2, PC), jnp.int32)),
            in_specs=[anym, vmem, anym, anym, anym],
            out_specs=(anym, anym, vmem),
            scratch_shapes=[
                pltpu.VMEM((lq, d), bf),
                pltpu.VMEM((2, side, d // side, hkv * DH), bf), pltpu.VMEM((side, d // side, hkv * gd), bf),
                pltpu.VMEM((2, lq, hkv * DH), f32), pltpu.VMEM((lq, hkv * gd), f32),
                pltpu.VMEM((n, 2, 2, PC, DH), bf), pltpu.VMEM((ng, 2, g, PC, DH), bf),
                pltpu.VMEM((ng, 2, 2, PC, DH), bf), pltpu.VMEM((ng, 2, g, PC, DH), bf),
                pltpu.VMEM((2, 2, 2, PC, DH), bf), pltpu.VMEM((2, 2, g, PC, DH), bf), pltpu.VMEM((n, 2, PC), jnp.int32),
                dma, dma((2, side)), dma((side,)), dma((ng + 2,)), dma((n,)), dma((2, 2)), dma((2, 2)), dma((2, 2)),
                dma((ng,)), dma((2 * ng,)),
                dma((ng + 2,)), dma((ng,)), dma((2, 2)), dma((2, 2)), dma((2, 2)), dma((n,)), dma((n,)), dma((n,)), dma((ng,)),
            ],
            compiler_params=pltpu.CompilerParams(collective_id=0, has_side_effects=True, vmem_limit_bytes=60 << 20),
            name="project",
        )(x, seg.reshape(1, 2, PC), wk, wv, wq)
        scale = DH ** -0.5 * math.log2(math.e)
        o = pl.pallas_call(
            functools.partial(_attend, n, g, scale),
            out_shape=jax.ShapeDtypeStruct((ng, PC, gd), bf),
            in_specs=[anym] * 3,
            out_specs=anym,
            scratch_shapes=[pltpu.SMEM((n, 2, PC), jnp.int32), pltpu.VMEM((n, 2, PC), jnp.int32),
                            pltpu.VMEM((2 * n, 2, PC, DH), bf), pltpu.VMEM((ng, g, PC, DH), bf),
                            pltpu.VMEM((ng, PC, gd), bf), pltpu.SMEM((ng,), jnp.int32)] + _pair_scratch(g) + [dma((2,)), dma, dma, dma],
            compiler_params=pltpu.CompilerParams(vmem_limit_bytes=60 << 20),
            name="attend",
        )(segs, kv, q)
        return pl.pallas_call(
            functools.partial(_combine, n, g, scale),
            out_shape=jax.ShapeDtypeStruct((lq, wo.shape[1]), bf),
            in_specs=[anym] * 5,
            out_specs=vmem,
            scratch_shapes=[pltpu.VMEM((hkv, lq, gd), bf), pltpu.VMEM((2, 2, PC, gd), bf), pltpu.VMEM((ng // 2, 2, PC, gd), bf),
                            pltpu.VMEM((side, 2 * gd, wo.shape[1]), bf), pltpu.VMEM((lq, wo.shape[1]), f32),
                            pltpu.SMEM((n, 2, PC), jnp.int32), pltpu.VMEM((n, 2, PC), jnp.int32),
                            pltpu.VMEM((n, 2, PC, DH), bf), pltpu.VMEM((ng, g, PC, DH), bf)] + _pair_scratch(g) + [
                            dma((side, 2)), dma((2, ng)), dma((2, ng)), dma((2, 2)), dma((2, 2)), dma((2,)), dma((n,)), dma((ng,))],
            compiler_params=pltpu.CompilerParams(collective_id=1, has_side_effects=True, vmem_limit_bytes=60 << 20),
            name="combine",
        )(segs, kv, q, o, wo)

    rows = P(("dp", "cp"), None)
    return jax.shard_map(local, mesh=mesh, in_specs=(rows, P(("dp", "cp")), P(), P(), P(), P()), out_specs=rows, check_vma=False)
```

```python
import functools
import math

import jax
import jax.numpy as jnp
from jax import lax
from jax.experimental import pallas as pl
from jax.experimental.pallas import tpu as pltpu
from jax.sharding import PartitionSpec as P

DH = 128
PC = 128
KB = 4
MESH = pl.DeviceIdType.MESH
NEG_INF = float("-inf")
FLOOR = -3e38


class Place:
    def __init__(self, n):
        me = lax.axis_index("cp")
        self.n, self.side = n, math.isqrt(n // 2)
        self.me = me
        self.c = lax.rem(me, 2)
        chip = me // 2
        self.x = lax.rem(chip, self.side)
        self.y = chip // self.side
        self.xin = self.x + 1 - 2 * lax.rem(self.x, 2)
        self.xcross = self.side - 1 - self.x
        self.px = lax.rem(lax.rem(self.x, 2) + self.x // 2, 2)

    def dev(self, x, y, c):
        return (y * self.side + x) * 2 + c

    def row(self, dy):
        return lax.rem(self.y + dy + self.side, self.side)

    def col(self, dx):
        return self.xin if dx else self.x

    def peer(self, dx, dy):
        return self.dev(self.col(dx), self.row(dy), self.c)

    def head(self, dx, dy):
        return lax.rem(self.px + dx, 2) * self.side + self.row(dy)

    def slot(self, dx, dy):
        return self.row(dy) * 2 + lax.rem(self.x + dx, 2)


FAR = 2
KV_ORDER = (FAR, 0, 1, -1)
Q_ORDER = (FAR, 1, -1, 0)
O_ORDER = (1, -1, FAR, 0)


def _project(n, g, x_ref, seg_ref, wk, wv, wq, kv_o, q_o, segs_o, wkvb, wqb, kvacc, qacc, kvb, qb, skv, sq, rkv, rq, segb,
             wkv_sem, wq_sem, kv_send, kv_recv, kvf_recv, rkv_recv, rkv_send, fx_send, fs_send,
             q_send, q_recv, qf_recv, rq_recv, rq_send, seg_send, seg_recv, out_sem, qout_sem):
    pt = Place(n)
    me = pt.me
    kv_steps = [(t, dx, dy) for t, dy in enumerate(KV_ORDER) for dx in range(2)]
    q_steps = [(t, dx, dy) for t, dy in enumerate(Q_ORDER) for dx in range(2)]
    own_kv = (KV_ORDER.index(0), 0)
    own_q = (Q_ORDER.index(0), 0)
    gd = g * DH
    kr = wqb.shape[1]
    nk = wqb.shape[0]
    my_head, my_slot = pt.head(0, 0), pt.slot(0, 0)

    kv_copies = [[pltpu.make_async_copy(w.at[pl.ds(t * kr, kr)], wkvb.at[i, t], wkv_sem.at[i, t]) for i, w in enumerate((wk, wv))]
                 for t in range(nk)]
    q_copies = [pltpu.make_async_copy(wq.at[pl.ds(t * kr, kr)], wqb.at[t], wq_sem.at[t]) for t in range(nk)]
    for cps in kv_copies:
        for cp in cps:
            cp.start()
    for cp in q_copies:
        cp.start()

    barrier = pltpu.get_barrier_semaphore()

    @pl.loop(1, n)
    def _(i):
        pl.semaphore_signal(barrier, inc=1, device_id={"cp": lax.rem(me + i, n)}, device_id_type=MESH)

    def seg_copy(i):
        return pltpu.make_async_remote_copy(seg_ref, segb.at[pl.ds(me, 1)], seg_send.at[i], seg_recv.at[me],
                                            device_id={"cp": lax.rem(me + i, n)}, device_id_type=MESH)

    segb[pl.ds(me, 1)] = seg_ref[...]

    def put(src, dst, send, recv, dev):
        return pltpu.make_async_remote_copy(src, dst, send, recv, device_id={"cp": dev}, device_id_type=MESH)

    def kv_copy(t, dx, dy):
        return put(skv.at[pt.head(dx, dy)], kvb.at[me], kv_send.at[2 * t + dx], kv_recv.at[me], pt.peer(dx, dy))

    def q_copy(t, dx, dy):
        return put(sq.at[pt.head(dx, dy)], qb.at[my_slot], q_send.at[2 * t + dx], q_recv.at[my_slot], pt.peer(dx, dy))

    way = (1, -1)
    hops = [(half, dx) for half in range(2) for dx in range(2)]

    def kv_hop(half, dx):
        return put(skv.at[pt.head(dx, FAR), half], rkv.at[half, dx], kv_send.at[2 * half + dx if half == 0 else 2 * len(KV_ORDER) + dx],
                   rkv_recv.at[half, dx], pt.peer(0, way[half]))

    def kv_hand(half, dx):
        return put(rkv.at[half, dx], kvb.at[pt.peer(0, -way[half]), half], rkv_send.at[half, dx], kvf_recv.at[dx, half],
                   pt.peer(dx, way[half]))

    def q_hop(half, dx):
        return put(sq.at[pt.head(dx, FAR), half], rq.at[half, dx], q_send.at[2 * half + dx if half == 0 else 2 * len(Q_ORDER) + dx],
                   rq_recv.at[half, dx], pt.peer(0, way[half]))

    def q_hand(half, dx):
        return put(rq.at[half, dx], qb.at[pt.slot(0, -way[half]), half], rq_send.at[half, dx], qf_recv.at[dx, half],
                   pt.peer(dx, way[half]))

    nb = 4 * DH

    def summed(t, w, acc, c):
        cols = slice(c * nb, (c + 1) * nb)
        r = jnp.dot(x_ref[:, t * kr:(t + 1) * kr], w[:, cols], preferred_element_type=jnp.float32)
        if t > 0:
            r = r + acc[:, cols]
        if t < nk - 1:
            acc[:, cols] = r
        return r

    def kv_step(t):
        for cp in kv_copies[t]:
            cp.wait()
        for c in range(wkvb.shape[3] // nb):
            for i in range(2):
                r = summed(t, wkvb.at[i, t], kvacc.at[i], c)
                if t == nk - 1:
                    for u in range(nb // DH):
                        part = r[:, u * DH:(u + 1) * DH]
                        part = (jnp.transpose(part) if i == 1 else part).astype(jnp.bfloat16)
                        for half in range(2):
                            rows = slice(half * PC, (half + 1) * PC)
                            skv[c * (nb // DH) + u, half, i] = part[:, rows] if i == 1 else part[rows]

    def q_step(t, first, last):
        if first == 0:
            q_copies[t].wait()
        for c in range(first, last):
            r = summed(t, wqb.at[t], qacc, c)
            if t == nk - 1:
                for u in range(nb // DH):
                    col = c * (nb // DH) + u
                    part = jnp.transpose(r[:, u * DH:(u + 1) * DH]).astype(jnp.bfloat16)
                    for half in range(2):
                        sq[col // g, half, col % g] = part[:, half * PC:(half + 1) * PC]

    def send_kv(t):
        if KV_ORDER[t] == FAR:
            for hop in hops:
                kv_hop(*hop).start()
        else:
            for dx in range(2):
                if (t, dx) != own_kv:
                    kv_copy(t, dx, KV_ORDER[t]).start()

    def send_q(t):
        if Q_ORDER[t] == FAR:
            for hop in hops:
                q_hop(*hop).start()
        else:
            for dx in range(2):
                if (t, dx) != own_q:
                    q_copy(t, dx, Q_ORDER[t]).start()

    def to_cross(src, i):
        return put(kvb.at[src], kvb.at[src], fx_send.at[i], kv_recv.at[src], pt.dev(pt.xcross, pt.y, pt.c))

    def to_sibling(src, i):
        return put(kvb.at[src], kvb.at[src], fs_send.at[i], kv_recv.at[src], pt.dev(pt.x, pt.y, 1 - pt.c))

    def kv_out(src):
        return pltpu.make_async_copy(kvb.at[src], kv_o.at[src], out_sem.at[src])

    def q_out(slot):
        return pltpu.make_async_copy(qb.at[slot], q_o.at[slot], qout_sem.at[slot])

    def arrived(src):
        to_sibling(src, 0).wait_recv()

    def forward(t):
        dy = KV_ORDER[t]
        for dx in range(2):
            src = pt.peer(dx, -dy)
            if dy == FAR:
                for half in range(2):
                    put(rkv.at[half, dx], kvb.at[src, half], rkv_send.at[half, dx], kvf_recv.at[dx, half], me).wait_recv()
            elif (t, dx) != own_kv:
                arrived(src)
            to_cross(src, 2 * t + dx).start()
            to_sibling(src, 2 * t + dx).start()
            kv_out(src).start()

    def own_out():
        return pltpu.make_async_copy(skv.at[my_head], kv_o.at[me], out_sem.at[me])

    def own_q_out():
        return pltpu.make_async_copy(sq.at[my_head], q_o.at[my_slot], qout_sem.at[my_slot])

    def forward_own():
        put(skv.at[my_head], kvb.at[me], fx_send.at[2 * own_kv[0]], kv_recv.at[me], pt.dev(pt.xcross, pt.y, pt.c)).start()
        put(skv.at[my_head], kvb.at[me], fs_send.at[2 * own_kv[0]], kv_recv.at[me], pt.dev(pt.x, pt.y, 1 - pt.c)).start()
        own_out().start()

    def forward_next():
        src = pt.peer(1, 0)
        arrived(src)
        to_cross(src, 2 * own_kv[0] + 1).start()
        to_sibling(src, 2 * own_kv[0] + 1).start()
        kv_out(src).start()

    for t in range(nk):
        kv_step(t)
    nq = wqb.shape[2] // nb
    q_step(0, 0, 1)

    pl.semaphore_wait(barrier, n - 1)
    for t in range(len(KV_ORDER)):
        send_kv(t)
    forward_own()
    q_step(0, 1, nq)
    q_step(1, 0, nq)
    q_step(2, 0, nq)
    forward_next()
    for hop in hops:
        put(rkv.at[hop], rkv.at[hop], kv_send.at[0], rkv_recv.at[hop], me).wait_recv()
        kv_hand(*hop).start()
    q_step(3, 0, nq)
    forward(2)
    for t in range(len(Q_ORDER)):
        send_q(t)
    own_q_out().start()
    forward(3)
    forward(0)

    @pl.loop(1, n)
    def _(i):
        seg_copy(i).start()


    def mirrored(dx, dy, c):
        x = pt.side - 1 - pt.col(dx)
        return pt.dev(x, pt.row(-dy), c)

    passing = [(t, dx, KV_ORDER[t]) for t in (1, 2, 3, 0) for dx in range(2)]

    def pass_on(steps):
        for t, dx, dy in steps:
            src = mirrored(dx, dy, pt.c)
            arrived(src)
            to_sibling(src, 8 + 2 * t + dx).start()
            kv_out(src).start()

    pass_on(passing[:2])
    for hop in hops:
        put(rq.at[hop], rq.at[hop], q_send.at[0], rq_recv.at[hop], me).wait_recv()
        q_hand(*hop).start()
    pass_on(passing[2:])

    for t, dx, dy in passing:
        src = pt.dev(pt.col(dx), pt.row(-dy), 1 - pt.c)
        arrived(src)
        kv_out(src).start()
    for t, dx, dy in q_steps:
        slot = pt.slot(dx, -dy)
        if dy == FAR:
            for half in range(2):
                put(rq.at[half, dx], qb.at[slot, half], rq_send.at[half, dx], qf_recv.at[dx, half], me).wait_recv()
        elif (t, dx) != own_q:
            put(qb.at[slot], qb.at[slot], q_send.at[0], q_recv.at[slot], me).wait_recv()
        if (t, dx) != own_q:
            q_out(slot).start()
    for t, dx, dy in passing:
        src = mirrored(dx, dy, 1 - pt.c)
        arrived(src)
        kv_out(src).start()

    @pl.loop(1, n)
    def _(i):
        src = lax.rem(me + i, n)
        pltpu.make_async_remote_copy(seg_ref, segb.at[pl.ds(src, 1)], seg_send.at[i], seg_recv.at[src],
                                     device_id={"cp": src}, device_id_type=MESH).wait_recv()

    segs_o[...] = segb[...]

    @pl.loop(1, n)
    def _(i):
        seg_copy(i).wait_send()

    for hop in hops:
        kv_hop(*hop).wait_send()
        kv_hand(*hop).wait_send()
        q_hop(*hop).wait_send()
        q_hand(*hop).wait_send()
    for t, dx, dy in kv_steps:
        if dy != FAR and (t, dx) != own_kv:
            kv_copy(t, dx, dy).wait_send()
        src = pt.peer(dx, -dy)
        to_cross(src, 2 * t + dx).wait_send()
        to_sibling(src, 2 * t + dx).wait_send()
        to_sibling(src, 8 + 2 * t + dx).wait_send()
    for t, dx, dy in q_steps:
        if dy != FAR and (t, dx) != own_q:
            q_copy(t, dx, dy).wait_send()

    @pl.loop(0, n)
    def _(i):
        kv_out(i).wait()

    @pl.loop(0, n // 4)
    def _(i):
        q_out(i).wait()


class Pairs:
    def __init__(self, pt, n, g, scale, first_of, seg_v, kvs, qs, t_sc, acc_sc):
        self.pt, self.n, self.g, self.scale, self.first_of, self.seg_v, self.kvs = pt, n, g, scale, first_of, seg_v, kvs
        self.qs, self.t_sc, self.acc_sc = qs, t_sc, acc_sc

    def begins(self, row, half):
        out = []
        for u in range(2):
            src = self.pt.dev((self.pt.x // 2) * 2 + u, row, self.pt.c)
            before = jnp.where(self.seg_v[...] < self.first_of(src, half), 1.0, 0.0)
            out.append(jnp.sum(before).astype(jnp.int32))
        return out

    def __call__(self, row, half, lo, begins, store):
        pt, n, g, scale, seg_v, kvs, qs = self.pt, self.n, self.g, self.scale, self.seg_v, self.kvs, self.qs
        t_sc, acc_sc = self.t_sc, self.acc_sc
        last_piece, pieces = 2 * n - 1, kvs.shape[0]
        srcs = [pt.dev((pt.x // 2) * 2 + u, row, pt.c) for u in range(2)]
        ps = [last_piece - src if half else src for src in srcs]
        end = jnp.maximum(ps[0], ps[1])
        wide = g * PC
        acc_sc[...] = jnp.zeros_like(acc_sc)

        def queries(us):
            return jnp.concatenate([qs[2 * row + u, w] for u in us for w in range(g)], axis=1)

        def start(b):
            return jnp.minimum(lo + b * KB, pieces - KB)

        def scores(b):
            j0, js = lo + b * KB, start(b)
            k = jnp.concatenate([kvs[js + w, 0] for w in range(KB)], axis=0)
            s = jnp.dot(k, queries((0, 1)), preferred_element_type=jnp.float32) * scale
            pos = lax.broadcasted_iota(jnp.int32, (KB * PC, DH), 0) + js * PC
            tops = []
            for u in range(2):
                seen = (pos >= jnp.maximum(begins[u], j0 * PC)) & (pos < ps[u] * PC)
                for w in range(g):
                    at = slice(u * wide + w * PC, u * wide + (w + 1) * PC)
                    part = jnp.where(seen, s[:, at], NEG_INF)
                    t_sc[:, at] = part
                    tops.append(jnp.max(part, axis=0, keepdims=True))
            return jnp.concatenate(tops, axis=1)

        def update(b, m, l, top):
            js = start(b)
            m_new = jnp.maximum(m, top)
            corr = jnp.exp2(m - m_new)
            p = jnp.exp2(t_sc[...] - m_new)
            l = l * corr + jnp.sum(p, axis=0, keepdims=True)
            vt = jnp.concatenate([kvs[js + w, 1] for w in range(KB)], axis=1)
            acc_sc[...] = acc_sc[...] * corr + jnp.dot(vt, p.astype(jnp.bfloat16), preferred_element_type=jnp.float32)
            return m_new, l

        def step(b, carry):
            return *update(b, *carry), scores(b + 1)

        line = jnp.zeros((1, 2 * wide), jnp.float32)
        last = jnp.maximum(lax.div(end - lo + KB - 1, KB) - 1, 0)
        m, l = update(last, *lax.fori_loop(0, last, step, (line + FLOOR, line, scores(0))))

        key = lax.broadcasted_iota(jnp.int32, (PC, PC), 0)
        query = lax.broadcasted_iota(jnp.int32, (PC, PC), 1)
        ss = [jnp.dot(kvs[ps[u], 0], queries((u,)), preferred_element_type=jnp.float32) * scale for u in range(2)]
        for u in range(2):
            at = slice(u * wide, (u + 1) * wide)
            ids = seg_v[srcs[u], pl.ds(half, 1), :]
            idb = jnp.broadcast_to(ids, (PC, PC))
            allowed = jnp.concatenate([(idb == jnp.transpose(idb)) & (key <= query)] * g, axis=1)
            keep = jnp.concatenate([ids == self.first_of(srcs[u], half)] * g, axis=1)
            s = jnp.where(allowed, ss[u], NEG_INF)
            m_old = jnp.where(keep, m[:, at], FLOOR)
            m_new = jnp.maximum(m_old, jnp.max(s, axis=0, keepdims=True))
            corr = jnp.where(keep, jnp.exp2(m_old - m_new), 0.0)
            p = jnp.exp2(s - m_new)
            ll = l[:, at] * corr + jnp.sum(p, axis=0, keepdims=True)
            acc = acc_sc[:, at] * corr + jnp.dot(kvs[ps[u], 1], p.astype(jnp.bfloat16), preferred_element_type=jnp.float32)
            o = acc * (1.0 / ll)
            for w in range(g):
                store(u, w, jnp.transpose(o[:, w * PC:(w + 1) * PC]).astype(jnp.bfloat16))


def _pair_scratch(g):
    f32 = jnp.float32
    return [pltpu.VMEM((KB * PC, 2 * g * PC), f32), pltpu.VMEM((DH, 2 * g * PC), f32)]


def _attend(n, g, scale, segs, kv, q_in, o_out, seg_s, seg_v, kvs, qs, os, lo_s, t_sc, acc_sc,
            seg_sem, kv_sem, q_sem, o_sem):
    pt = Place(n)
    last_piece = 2 * n - 1
    ng = q_in.shape[0]

    def load(p):
        owner = jnp.where(p < n, p, last_piece - p)
        return pltpu.make_async_copy(kv.at[owner, jnp.where(p < n, 0, 1)], kvs.at[p], kv_sem)

    seg_copies = [pltpu.make_async_copy(segs, seg_v, seg_sem.at[0]), pltpu.make_async_copy(segs, seg_s, seg_sem.at[1])]
    q_copies = [pltpu.make_async_copy(q_in.at[i, 1], qs.at[i], q_sem) for i in range(ng)]
    for cp in seg_copies + q_copies:
        cp.start()

    @pl.loop(0, 2 * n)
    def _(p):
        load(p).start()

    for cp in seg_copies:
        cp.wait()
    pairs = Pairs(pt, n, g, scale, lambda src, half: seg_s[src, half, 0], seg_v, kvs, qs, t_sc, acc_sc)
    for i in range(ng // 2):
        for u, at in enumerate(pairs.begins(i, 1)):
            lo_s[2 * i + u] = at
    for cp in q_copies:
        cp.wait()

    @pl.loop(0, 2 * n)
    def _(p):
        load(p).wait()

    def out(slot):
        return pltpu.make_async_copy(os.at[slot], o_out.at[slot], o_sem)

    def one(row, carry):
        def store(u, w, val):
            os[2 * row + u, :, w * DH:(w + 1) * DH] = val

        begins = [lo_s[2 * row + u] for u in range(2)]
        pairs(row, 1, lax.div(jnp.minimum(*begins), PC), begins, store)

        @pl.when(row > 0)
        def _():
            for u in range(2):
                out(2 * (row - 1) + u).start()

        return carry

    lax.fori_loop(0, ng // 2, one, 0)
    for u in range(2):
        out(ng - 2 + u).start()
    for i in range(ng):
        out(i).wait()


def _combine(n, g, scale, segs, kv, q_in, o_in, wo, y_ref, obuf, robuf, ol, wob, acc, seg_s, seg_v, kvs, qs,
             t_sc, acc_sc, w_sem, o_send, o_recv, ro_recv, ro_send, seg_sem, kv_sem, q_sem):
    pt = Place(n)
    me = pt.me
    gd = g * DH
    ng = q_in.shape[0]
    my_head, my_slot = pt.head(0, 0), pt.slot(0, 0)
    nc = 4
    wn = y_ref.shape[1] // nc
    lows, highs = pl.ds(0, PC), pl.ds(PC, PC)

    def load(p):
        return pltpu.make_async_copy(kv.at[p, 0], kvs.at[p], kv_sem.at[p])

    q_copies = [pltpu.make_async_copy(q_in.at[i, 0], qs.at[i], q_sem.at[i]) for i in range(ng)]
    seg_copies = [pltpu.make_async_copy(segs, seg_v, seg_sem.at[0]), pltpu.make_async_copy(segs, seg_s, seg_sem.at[1])]
    own = pltpu.make_async_copy(o_in.at[my_slot], obuf.at[my_head, highs], o_recv.at[1, my_head])
    for cp in seg_copies + q_copies + [own]:
        cp.start()

    @pl.loop(0, n)
    def _(p):
        load(p).start()

    def w_copies(t):
        for dx in range(2):
            h = pl.multiple_of(pt.head(dx, O_ORDER[t]) * gd, gd)
            yield pltpu.make_async_copy(wo.at[pl.ds(h, gd), :], wob.at[t, pl.ds(dx * gd, gd), :], w_sem.at[t, dx])

    for t in range(len(O_ORDER)):
        for cp in w_copies(t):
            cp.start()

    others = [(dx, dy) for dy in O_ORDER for dx in range(2) if (dx, dy) != (0, 0)]
    near = [s for s in others if s[1] != FAR]
    barrier = pltpu.get_barrier_semaphore()
    for dx, dy in others:
        pl.semaphore_signal(barrier, inc=1, device_id={"cp": pt.peer(dx, dy)}, device_id_type=MESH)
    pl.semaphore_wait(barrier, len(others))

    def put(src, dst, send, recv, dev):
        return pltpu.make_async_remote_copy(src, dst, send, recv, device_id={"cp": dev}, device_id_type=MESH)

    way = (1, -1)
    turn = {FAR: 0, 1: 1, -1: 2, 0: 3}

    def source(half, dx, dy):
        return o_in.at[pt.slot(dx, dy)] if half else ol.at[turn[dy], lax.rem(pt.x + dx, 2)]

    def o_copy(half, i):
        dx, dy = near[i]
        return put(source(half, dx, dy), obuf.at[my_head, highs if half else lows], o_send.at[half, i], o_recv.at[half, my_head],
                   pt.peer(dx, dy))

    def o_hop(half, dx):
        return put(source(half, dx, FAR), robuf.at[half, dx], o_send.at[half, len(near) + dx], ro_recv.at[half, dx],
                   pt.peer(0, way[dx]))

    def o_hand(half, dx):
        head = pt.head(0, -way[dx])
        return put(robuf.at[half, dx], obuf.at[head, highs if half else lows], ro_send.at[half, dx], o_recv.at[half, head],
                   pt.peer(dx, way[dx]))

    def hand_on(half):
        for dx in range(2):
            put(robuf.at[half, dx], robuf.at[half, dx], o_send.at[0, 0], ro_recv.at[half, dx], me).wait_recv()
            o_hand(half, dx).start()

    for dx in range(2):
        o_hop(1, dx).start()
    for i in range(len(near)):
        o_copy(1, i).start()

    for cp in seg_copies + q_copies:
        cp.wait()

    @pl.loop(0, n)
    def _(p):
        load(p).wait()

    pairs = Pairs(pt, n, g, scale, lambda src, half: seg_s[src, half, 0], seg_v, kvs, qs, t_sc, acc_sc)

    def send_low(dy):
        if dy == FAR:
            for dx in range(2):
                o_hop(0, dx).start()
        else:
            for i, (dx, to) in enumerate(near):
                if to == dy:
                    o_copy(0, i).start()

    def one(i, carry):
        turned = jnp.where(i == 2, -1, jnp.where(i == 3, 0, FAR - i))
        row = lax.rem(pt.y + turned + pt.side, pt.side)

        def store(u, w, val):
            ol[i, u, :, w * DH:(w + 1) * DH] = val

        pairs(row, 0, 0, pairs.begins(row, 0), store)

        @pl.when(i == 1)
        def _():
            send_low(FAR)
            hand_on(1)

        @pl.when(i == 2)
        def _():
            send_low(1)

        @pl.when(i == 3)
        def _():
            send_low(-1)
            hand_on(0)

        return carry

    lax.fori_loop(0, ng // 2, one, 0)
    send_low(0)
    obuf[my_head, 0:PC] = ol[turn[0], lax.rem(pt.x, 2)]

    for t, dy in enumerate(O_ORDER):
        for cp in w_copies(t):
            cp.wait()
        heads = [pt.head(dx, dy) for dx in range(2)]
        for dx in range(2):
            if dy == 0 and dx == 0:
                own.wait()
            else:
                for half in range(2):
                    put(ol.at[0, 0], obuf.at[heads[dx], highs if half else lows], o_send.at[0, 0], o_recv.at[half, heads[dx]],
                        me).wait_recv()
        a = jnp.concatenate([obuf[heads[0]], obuf[heads[1]]], axis=1)
        for u in range(nc):
            r = jnp.dot(a, wob[t, :, u * wn:(u + 1) * wn], preferred_element_type=jnp.float32)
            if t > 0:
                r = r + acc[:, u * wn:(u + 1) * wn]
            if t < len(O_ORDER) - 1:
                acc[:, u * wn:(u + 1) * wn] = r
            else:
                y_ref[:, u * wn:(u + 1) * wn] = r.astype(y_ref.dtype)
    for half in range(2):
        for i in range(len(near)):
            o_copy(half, i).wait_send()
        for dx in range(2):
            o_hop(half, dx).wait_send()
            o_hand(half, dx).wait_send()


def solution(mesh):
    n = mesh.shape["cp"]
    side = math.isqrt(n // 2)
    bf, f32 = jnp.bfloat16, jnp.float32
    vmem, anym = pl.BlockSpec(memory_space=pltpu.VMEM), pl.BlockSpec(memory_space=pltpu.HBM)
    dma = pltpu.SemaphoreType.DMA

    def local(x, seg, wq, wk, wv, wo):
        lq, d = x.shape
        hkv = wk.shape[1] // DH
        g = wq.shape[1] // wk.shape[1]
        gd = g * DH
        ng = 2 * side
        kv, q, segs = pl.pallas_call(
            functools.partial(_project, n, g),
            out_shape=(jax.ShapeDtypeStruct((n, 2, 2, PC, DH), bf), jax.ShapeDtypeStruct((ng, 2, g, PC, DH), bf),
                       jax.ShapeDtypeStruct((n, 2, PC), jnp.int32)),
            in_specs=[vmem, vmem, anym, anym, anym],
            out_specs=(anym, anym, vmem),
            scratch_shapes=[
                pltpu.VMEM((2, side, d // side, hkv * DH), bf), pltpu.VMEM((side, d // side, hkv * gd), bf),
                pltpu.VMEM((2, lq, hkv * DH), f32), pltpu.VMEM((lq, hkv * gd), f32),
                pltpu.VMEM((n, 2, 2, PC, DH), bf), pltpu.VMEM((ng, 2, g, PC, DH), bf),
                pltpu.VMEM((ng, 2, 2, PC, DH), bf), pltpu.VMEM((ng, 2, g, PC, DH), bf),
                pltpu.VMEM((2, 2, 2, PC, DH), bf), pltpu.VMEM((2, 2, g, PC, DH), bf), pltpu.VMEM((n, 2, PC), jnp.int32),
                dma((2, side)), dma((side,)), dma((ng + 2,)), dma((n,)), dma((2, 2)), dma((2, 2)), dma((2, 2)),
                dma((ng,)), dma((2 * ng,)),
                dma((ng + 2,)), dma((ng,)), dma((2, 2)), dma((2, 2)), dma((2, 2)), dma((n,)), dma((n,)), dma((n,)), dma((ng,)),
            ],
            compiler_params=pltpu.CompilerParams(collective_id=0, has_side_effects=True, vmem_limit_bytes=60 << 20),
            name="project",
        )(x, seg.reshape(1, 2, PC), wk, wv, wq)
        scale = DH ** -0.5 * math.log2(math.e)
        o = pl.pallas_call(
            functools.partial(_attend, n, g, scale),
            out_shape=jax.ShapeDtypeStruct((ng, PC, gd), bf),
            in_specs=[anym] * 3,
            out_specs=anym,
            scratch_shapes=[pltpu.SMEM((n, 2, PC), jnp.int32), pltpu.VMEM((n, 2, PC), jnp.int32),
                            pltpu.VMEM((2 * n, 2, PC, DH), bf), pltpu.VMEM((ng, g, PC, DH), bf),
                            pltpu.VMEM((ng, PC, gd), bf), pltpu.SMEM((ng,), jnp.int32)] + _pair_scratch(g) + [dma((2,)), dma, dma, dma],
            compiler_params=pltpu.CompilerParams(vmem_limit_bytes=60 << 20),
            name="attend",
        )(segs, kv, q)
        return pl.pallas_call(
            functools.partial(_combine, n, g, scale),
            out_shape=jax.ShapeDtypeStruct((lq, wo.shape[1]), bf),
            in_specs=[anym] * 5,
            out_specs=vmem,
            scratch_shapes=[pltpu.VMEM((hkv, lq, gd), bf), pltpu.VMEM((2, 2, PC, gd), bf), pltpu.VMEM((ng // 2, 2, PC, gd), bf),
                            pltpu.VMEM((side, 2 * gd, wo.shape[1]), bf), pltpu.VMEM((lq, wo.shape[1]), f32),
                            pltpu.SMEM((n, 2, PC), jnp.int32), pltpu.VMEM((n, 2, PC), jnp.int32),
                            pltpu.VMEM((n, 2, PC, DH), bf), pltpu.VMEM((ng, g, PC, DH), bf)] + _pair_scratch(g) + [
                            dma((side, 2)), dma((2, ng)), dma((2, ng)), dma((2, 2)), dma((2, 2)), dma((2,)), dma((n,)), dma((ng,))],
            compiler_params=pltpu.CompilerParams(collective_id=1, has_side_effects=True, vmem_limit_bytes=60 << 20),
            name="combine",
        )(segs, kv, q, o, wo)

    rows = P(("dp", "cp"), None)
    return jax.shard_map(local, mesh=mesh, in_specs=(rows, P(("dp", "cp")), P(), P(), P(), P()), out_specs=rows, check_vma=False)
```

```python
import functools
import math

import jax
import jax.numpy as jnp
from jax import lax
from jax.experimental import pallas as pl
from jax.experimental.pallas import tpu as pltpu
from jax.sharding import PartitionSpec as P

DH = 128
PC = 128
KB = 4
MESH = pl.DeviceIdType.MESH
NEG_INF = float("-inf")
FLOOR = -3e38


class Place:
    def __init__(self, n):
        me = lax.axis_index("cp")
        self.n, self.side = n, math.isqrt(n // 2)
        self.me = me
        self.c = lax.rem(me, 2)
        chip = me // 2
        self.x = lax.rem(chip, self.side)
        self.y = chip // self.side
        self.xin = self.x + 1 - 2 * lax.rem(self.x, 2)
        self.xcross = self.side - 1 - self.x
        self.px = lax.rem(lax.rem(self.x, 2) + self.x // 2, 2)

    def dev(self, x, y, c):
        return (y * self.side + x) * 2 + c

    def row(self, dy):
        return lax.rem(self.y + dy + self.side, self.side)

    def col(self, dx):
        return self.xin if dx else self.x

    def peer(self, dx, dy):
        return self.dev(self.col(dx), self.row(dy), self.c)

    def head(self, dx, dy):
        return lax.rem(self.px + dx, 2) * self.side + self.row(dy)

    def slot(self, dx, dy):
        return self.row(dy) * 2 + lax.rem(self.x + dx, 2)


FAR = 2
KV_ORDER = (FAR, 0, 1, -1)
Q_ORDER = (FAR, 1, -1, 0)
O_ORDER = (1, -1, 0, FAR)


def _project(n, g, x_ref, seg_ref, wk, wv, wq, kv_o, q_o, segs_o, wkvb, wqb, kvacc, qacc, kvb, qb, skv, sq, rkv, rq, segb,
             wkv_sem, wq_sem, kv_send, kv_recv, kvf_recv, rkv_recv, rkv_send, fx_send, fs_send,
             q_send, q_recv, qf_recv, rq_recv, rq_send, seg_send, seg_recv, out_sem, qout_sem):
    pt = Place(n)
    me = pt.me
    kv_steps = [(t, dx, dy) for t, dy in enumerate(KV_ORDER) for dx in range(2)]
    q_steps = [(t, dx, dy) for t, dy in enumerate(Q_ORDER) for dx in range(2)]
    own_kv = (KV_ORDER.index(0), 0)
    own_q = (Q_ORDER.index(0), 0)
    gd = g * DH
    kr = wqb.shape[1]
    nk = wqb.shape[0]
    my_head, my_slot = pt.head(0, 0), pt.slot(0, 0)

    kv_copies = [[pltpu.make_async_copy(w.at[pl.ds(t * kr, kr)], wkvb.at[i, t], wkv_sem.at[i, t]) for i, w in enumerate((wk, wv))]
                 for t in range(nk)]
    q_copies = [pltpu.make_async_copy(wq.at[pl.ds(t * kr, kr)], wqb.at[t], wq_sem.at[t]) for t in range(nk)]
    for cps in kv_copies:
        for cp in cps:
            cp.start()
    for cp in q_copies:
        cp.start()

    barrier = pltpu.get_barrier_semaphore()

    @pl.loop(1, n)
    def _(i):
        pl.semaphore_signal(barrier, inc=1, device_id={"cp": lax.rem(me + i, n)}, device_id_type=MESH)

    def seg_copy(i):
        return pltpu.make_async_remote_copy(seg_ref, segb.at[pl.ds(me, 1)], seg_send.at[i], seg_recv.at[me],
                                            device_id={"cp": lax.rem(me + i, n)}, device_id_type=MESH)

    segb[pl.ds(me, 1)] = seg_ref[...]

    def put(src, dst, send, recv, dev):
        return pltpu.make_async_remote_copy(src, dst, send, recv, device_id={"cp": dev}, device_id_type=MESH)

    def kv_copy(t, dx, dy):
        return put(skv.at[pt.head(dx, dy)], kvb.at[me], kv_send.at[2 * t + dx], kv_recv.at[me], pt.peer(dx, dy))

    def q_copy(t, dx, dy):
        return put(sq.at[pt.head(dx, dy)], qb.at[my_slot], q_send.at[2 * t + dx], q_recv.at[my_slot], pt.peer(dx, dy))

    way = (1, -1)
    hops = [(half, dx) for half in range(2) for dx in range(2)]

    def kv_hop(half, dx):
        return put(skv.at[pt.head(dx, FAR), half], rkv.at[half, dx], kv_send.at[2 * half + dx if half == 0 else 2 * len(KV_ORDER) + dx],
                   rkv_recv.at[half, dx], pt.peer(0, way[half]))

    def kv_hand(half, dx):
        return put(rkv.at[half, dx], kvb.at[pt.peer(0, -way[half]), half], rkv_send.at[half, dx], kvf_recv.at[dx, half],
                   pt.peer(dx, way[half]))

    def q_hop(half, dx):
        return put(sq.at[pt.head(dx, FAR), half], rq.at[half, dx], q_send.at[2 * half + dx if half == 0 else 2 * len(Q_ORDER) + dx],
                   rq_recv.at[half, dx], pt.peer(0, way[half]))

    def q_hand(half, dx):
        return put(rq.at[half, dx], qb.at[pt.slot(0, -way[half]), half], rq_send.at[half, dx], qf_recv.at[dx, half],
                   pt.peer(dx, way[half]))

    nb = 4 * DH

    def summed(t, w, acc, c):
        cols = slice(c * nb, (c + 1) * nb)
        r = jnp.dot(x_ref[:, t * kr:(t + 1) * kr], w[:, cols], preferred_element_type=jnp.float32)
        if t > 0:
            r = r + acc[:, cols]
        if t < nk - 1:
            acc[:, cols] = r
        return r

    def kv_step(t):
        for cp in kv_copies[t]:
            cp.wait()
        for c in range(wkvb.shape[3] // nb):
            for i in range(2):
                r = summed(t, wkvb.at[i, t], kvacc.at[i], c)
                if t == nk - 1:
                    for u in range(nb // DH):
                        part = r[:, u * DH:(u + 1) * DH]
                        part = (jnp.transpose(part) if i == 1 else part).astype(jnp.bfloat16)
                        for half in range(2):
                            rows = slice(half * PC, (half + 1) * PC)
                            skv[c * (nb // DH) + u, half, i] = part[:, rows] if i == 1 else part[rows]

    def q_step(t, first, last):
        if first == 0:
            q_copies[t].wait()
        for c in range(first, last):
            r = summed(t, wqb.at[t], qacc, c)
            if t == nk - 1:
                for u in range(nb // DH):
                    col = c * (nb // DH) + u
                    part = jnp.transpose(r[:, u * DH:(u + 1) * DH]).astype(jnp.bfloat16)
                    for half in range(2):
                        sq[col // g, half, col % g] = part[:, half * PC:(half + 1) * PC]

    def send_kv(t):
        if KV_ORDER[t] == FAR:
            for hop in hops:
                kv_hop(*hop).start()
        else:
            for dx in range(2):
                if (t, dx) != own_kv:
                    kv_copy(t, dx, KV_ORDER[t]).start()

    def send_q(t):
        if Q_ORDER[t] == FAR:
            for hop in hops:
                q_hop(*hop).start()
        else:
            for dx in range(2):
                if (t, dx) != own_q:
                    q_copy(t, dx, Q_ORDER[t]).start()

    def to_cross(src, i):
        return put(kvb.at[src], kvb.at[src], fx_send.at[i], kv_recv.at[src], pt.dev(pt.xcross, pt.y, pt.c))

    def to_sibling(src, i):
        return put(kvb.at[src], kvb.at[src], fs_send.at[i], kv_recv.at[src], pt.dev(pt.x, pt.y, 1 - pt.c))

    def kv_out(src):
        return pltpu.make_async_copy(kvb.at[src], kv_o.at[src], out_sem.at[src])

    def q_out(slot):
        return pltpu.make_async_copy(qb.at[slot], q_o.at[slot], qout_sem.at[slot])

    def arrived(src):
        to_sibling(src, 0).wait_recv()

    def forward(t):
        dy = KV_ORDER[t]
        for dx in range(2):
            src = pt.peer(dx, -dy)
            if dy == FAR:
                for half in range(2):
                    put(rkv.at[half, dx], kvb.at[src, half], rkv_send.at[half, dx], kvf_recv.at[dx, half], me).wait_recv()
            elif (t, dx) != own_kv:
                arrived(src)
            to_cross(src, 2 * t + dx).start()
            to_sibling(src, 2 * t + dx).start()
            kv_out(src).start()

    def own_out():
        return pltpu.make_async_copy(skv.at[my_head], kv_o.at[me], out_sem.at[me])

    def own_q_out():
        return pltpu.make_async_copy(sq.at[my_head], q_o.at[my_slot], qout_sem.at[my_slot])

    def forward_own():
        put(skv.at[my_head], kvb.at[me], fx_send.at[2 * own_kv[0]], kv_recv.at[me], pt.dev(pt.xcross, pt.y, pt.c)).start()
        put(skv.at[my_head], kvb.at[me], fs_send.at[2 * own_kv[0]], kv_recv.at[me], pt.dev(pt.x, pt.y, 1 - pt.c)).start()
        own_out().start()

    def forward_next():
        src = pt.peer(1, 0)
        arrived(src)
        to_cross(src, 2 * own_kv[0] + 1).start()
        to_sibling(src, 2 * own_kv[0] + 1).start()
        kv_out(src).start()

    for t in range(nk):
        kv_step(t)
    nq = wqb.shape[2] // nb
    q_step(0, 0, 1)

    pl.semaphore_wait(barrier, n - 1)
    for t in range(len(KV_ORDER)):
        send_kv(t)
    forward_own()
    q_step(0, 1, nq)
    q_step(1, 0, nq)
    q_step(2, 0, nq)
    forward_next()
    for hop in hops:
        put(rkv.at[hop], rkv.at[hop], kv_send.at[0], rkv_recv.at[hop], me).wait_recv()
        kv_hand(*hop).start()
    q_step(3, 0, nq)
    forward(2)
    for t in range(len(Q_ORDER)):
        send_q(t)
    own_q_out().start()
    forward(3)
    forward(0)

    @pl.loop(1, n)
    def _(i):
        seg_copy(i).start()


    def mirrored(dx, dy, c):
        x = pt.side - 1 - pt.col(dx)
        return pt.dev(x, pt.row(-dy), c)

    passing = [(t, dx, KV_ORDER[t]) for t in (1, 2, 3, 0) for dx in range(2)]

    def pass_on(steps):
        for t, dx, dy in steps:
            src = mirrored(dx, dy, pt.c)
            arrived(src)
            to_sibling(src, 8 + 2 * t + dx).start()
            kv_out(src).start()

    pass_on(passing[:2])
    for hop in hops:
        put(rq.at[hop], rq.at[hop], q_send.at[0], rq_recv.at[hop], me).wait_recv()
        q_hand(*hop).start()
    pass_on(passing[2:])

    for t, dx, dy in passing:
        src = pt.dev(pt.col(dx), pt.row(-dy), 1 - pt.c)
        arrived(src)
        kv_out(src).start()
    for t, dx, dy in q_steps:
        slot = pt.slot(dx, -dy)
        if dy == FAR:
            for half in range(2):
                put(rq.at[half, dx], qb.at[slot, half], rq_send.at[half, dx], qf_recv.at[dx, half], me).wait_recv()
        elif (t, dx) != own_q:
            put(qb.at[slot], qb.at[slot], q_send.at[0], q_recv.at[slot], me).wait_recv()
        if (t, dx) != own_q:
            q_out(slot).start()
    for t, dx, dy in passing:
        src = mirrored(dx, dy, 1 - pt.c)
        arrived(src)
        kv_out(src).start()

    @pl.loop(1, n)
    def _(i):
        src = lax.rem(me + i, n)
        pltpu.make_async_remote_copy(seg_ref, segb.at[pl.ds(src, 1)], seg_send.at[i], seg_recv.at[src],
                                     device_id={"cp": src}, device_id_type=MESH).wait_recv()

    segs_o[...] = segb[...]

    @pl.loop(1, n)
    def _(i):
        seg_copy(i).wait_send()

    for hop in hops:
        kv_hop(*hop).wait_send()
        kv_hand(*hop).wait_send()
        q_hop(*hop).wait_send()
        q_hand(*hop).wait_send()
    for t, dx, dy in kv_steps:
        if dy != FAR and (t, dx) != own_kv:
            kv_copy(t, dx, dy).wait_send()
        src = pt.peer(dx, -dy)
        to_cross(src, 2 * t + dx).wait_send()
        to_sibling(src, 2 * t + dx).wait_send()
        to_sibling(src, 8 + 2 * t + dx).wait_send()
    for t, dx, dy in q_steps:
        if dy != FAR and (t, dx) != own_q:
            q_copy(t, dx, dy).wait_send()

    @pl.loop(0, n)
    def _(i):
        kv_out(i).wait()

    @pl.loop(0, n // 4)
    def _(i):
        q_out(i).wait()


class Pairs:
    def __init__(self, pt, n, g, scale, first_of, seg_v, kvs, qs, t_sc, acc_sc):
        self.pt, self.n, self.g, self.scale, self.first_of, self.seg_v, self.kvs = pt, n, g, scale, first_of, seg_v, kvs
        self.qs, self.t_sc, self.acc_sc = qs, t_sc, acc_sc

    def begins(self, row, half):
        out = []
        for u in range(2):
            src = self.pt.dev((self.pt.x // 2) * 2 + u, row, self.pt.c)
            before = jnp.where(self.seg_v[...] < self.first_of(src, half), 1.0, 0.0)
            out.append(jnp.sum(before).astype(jnp.int32))
        return out

    def __call__(self, row, half, lo, begins, store):
        pt, n, g, scale, seg_v, kvs, qs = self.pt, self.n, self.g, self.scale, self.seg_v, self.kvs, self.qs
        t_sc, acc_sc = self.t_sc, self.acc_sc
        last_piece, pieces = 2 * n - 1, kvs.shape[0]
        srcs = [pt.dev((pt.x // 2) * 2 + u, row, pt.c) for u in range(2)]
        ps = [last_piece - src if half else src for src in srcs]
        end = jnp.maximum(ps[0], ps[1])
        wide = g * PC
        acc_sc[...] = jnp.zeros_like(acc_sc)

        def queries(us):
            return jnp.concatenate([qs[2 * row + u, w] for u in us for w in range(g)], axis=1)

        def start(b):
            return jnp.minimum(lo + b * KB, pieces - KB)

        def scores(b):
            j0, js = lo + b * KB, start(b)
            k = jnp.concatenate([kvs[js + w, 0] for w in range(KB)], axis=0)
            s = jnp.dot(k, queries((0, 1)), preferred_element_type=jnp.float32) * scale
            pos = lax.broadcasted_iota(jnp.int32, (KB * PC, DH), 0) + js * PC
            tops = []
            for u in range(2):
                seen = (pos >= jnp.maximum(begins[u], j0 * PC)) & (pos < ps[u] * PC)
                for w in range(g):
                    at = slice(u * wide + w * PC, u * wide + (w + 1) * PC)
                    part = jnp.where(seen, s[:, at], NEG_INF)
                    t_sc[:, at] = part
                    tops.append(jnp.max(part, axis=0, keepdims=True))
            return jnp.concatenate(tops, axis=1)

        def update(b, m, l, top):
            js = start(b)
            m_new = jnp.maximum(m, top)
            corr = jnp.exp2(m - m_new)
            p = jnp.exp2(t_sc[...] - m_new)
            l = l * corr + jnp.sum(p, axis=0, keepdims=True)
            vt = jnp.concatenate([kvs[js + w, 1] for w in range(KB)], axis=1)
            acc_sc[...] = acc_sc[...] * corr + jnp.dot(vt, p.astype(jnp.bfloat16), preferred_element_type=jnp.float32)
            return m_new, l

        def step(b, carry):
            return *update(b, *carry), scores(b + 1)

        line = jnp.zeros((1, 2 * wide), jnp.float32)
        last = jnp.maximum(lax.div(end - lo + KB - 1, KB) - 1, 0)
        m, l = update(last, *lax.fori_loop(0, last, step, (line + FLOOR, line, scores(0))))

        key = lax.broadcasted_iota(jnp.int32, (PC, PC), 0)
        query = lax.broadcasted_iota(jnp.int32, (PC, PC), 1)
        ss = [jnp.dot(kvs[ps[u], 0], queries((u,)), preferred_element_type=jnp.float32) * scale for u in range(2)]
        for u in range(2):
            at = slice(u * wide, (u + 1) * wide)
            ids = seg_v[srcs[u], pl.ds(half, 1), :]
            idb = jnp.broadcast_to(ids, (PC, PC))
            allowed = jnp.concatenate([(idb == jnp.transpose(idb)) & (key <= query)] * g, axis=1)
            keep = jnp.concatenate([ids == self.first_of(srcs[u], half)] * g, axis=1)
            s = jnp.where(allowed, ss[u], NEG_INF)
            m_old = jnp.where(keep, m[:, at], FLOOR)
            m_new = jnp.maximum(m_old, jnp.max(s, axis=0, keepdims=True))
            corr = jnp.where(keep, jnp.exp2(m_old - m_new), 0.0)
            p = jnp.exp2(s - m_new)
            ll = l[:, at] * corr + jnp.sum(p, axis=0, keepdims=True)
            acc = acc_sc[:, at] * corr + jnp.dot(kvs[ps[u], 1], p.astype(jnp.bfloat16), preferred_element_type=jnp.float32)
            o = acc * (1.0 / ll)
            for w in range(g):
                store(u, w, jnp.transpose(o[:, w * PC:(w + 1) * PC]).astype(jnp.bfloat16))


def _pair_scratch(g):
    f32 = jnp.float32
    return [pltpu.VMEM((KB * PC, 2 * g * PC), f32), pltpu.VMEM((DH, 2 * g * PC), f32)]


def _attend(n, g, scale, segs, kv, q_in, o_out, seg_s, seg_v, kvs, qs, os, lo_s, t_sc, acc_sc,
            seg_sem, kv_sem, q_sem, o_sem):
    pt = Place(n)
    last_piece = 2 * n - 1
    ng = q_in.shape[0]

    def load(p):
        owner = jnp.where(p < n, p, last_piece - p)
        return pltpu.make_async_copy(kv.at[owner, jnp.where(p < n, 0, 1)], kvs.at[p], kv_sem)

    seg_copies = [pltpu.make_async_copy(segs, seg_v, seg_sem.at[0]), pltpu.make_async_copy(segs, seg_s, seg_sem.at[1])]
    q_copies = [pltpu.make_async_copy(q_in.at[i, 1], qs.at[i], q_sem) for i in range(ng)]
    for cp in seg_copies + q_copies:
        cp.start()

    @pl.loop(0, 2 * n)
    def _(p):
        load(p).start()

    for cp in seg_copies:
        cp.wait()
    pairs = Pairs(pt, n, g, scale, lambda src, half: seg_s[src, half, 0], seg_v, kvs, qs, t_sc, acc_sc)
    for i in range(ng // 2):
        for u, at in enumerate(pairs.begins(i, 1)):
            lo_s[2 * i + u] = at
    for cp in q_copies:
        cp.wait()

    @pl.loop(0, 2 * n)
    def _(p):
        load(p).wait()

    def out(slot):
        return pltpu.make_async_copy(os.at[slot], o_out.at[slot], o_sem)

    def one(row, carry):
        def store(u, w, val):
            os[2 * row + u, :, w * DH:(w + 1) * DH] = val

        begins = [lo_s[2 * row + u] for u in range(2)]
        pairs(row, 1, lax.div(jnp.minimum(*begins), PC), begins, store)

        @pl.when(row > 0)
        def _():
            for u in range(2):
                out(2 * (row - 1) + u).start()

        return carry

    lax.fori_loop(0, ng // 2, one, 0)
    for u in range(2):
        out(ng - 2 + u).start()
    for i in range(ng):
        out(i).wait()


def _combine(n, g, scale, segs, kv, q_in, o_in, wo, y_ref, obuf, robuf, ol, wob, acc, seg_s, seg_v, kvs, qs,
             t_sc, acc_sc, w_sem, o_send, o_recv, ro_recv, ro_send, seg_sem, kv_sem, q_sem):
    pt = Place(n)
    me = pt.me
    gd = g * DH
    ng = q_in.shape[0]
    my_head, my_slot = pt.head(0, 0), pt.slot(0, 0)
    nc = 4
    wn = y_ref.shape[1] // nc
    lows, highs = pl.ds(0, PC), pl.ds(PC, PC)

    def load(p):
        return pltpu.make_async_copy(kv.at[p, 0], kvs.at[p], kv_sem.at[p])

    q_copies = [pltpu.make_async_copy(q_in.at[i, 0], qs.at[i], q_sem.at[i]) for i in range(ng)]
    seg_copies = [pltpu.make_async_copy(segs, seg_v, seg_sem.at[0]), pltpu.make_async_copy(segs, seg_s, seg_sem.at[1])]
    own = pltpu.make_async_copy(o_in.at[my_slot], obuf.at[my_head, highs], o_recv.at[1, my_head])
    for cp in seg_copies + q_copies + [own]:
        cp.start()

    @pl.loop(0, n)
    def _(p):
        load(p).start()

    def w_copies(t):
        for dx in range(2):
            h = pl.multiple_of(pt.head(dx, O_ORDER[t]) * gd, gd)
            yield pltpu.make_async_copy(wo.at[pl.ds(h, gd), :], wob.at[t, pl.ds(dx * gd, gd), :], w_sem.at[t, dx])

    for t in range(len(O_ORDER)):
        for cp in w_copies(t):
            cp.start()

    others = [(dx, dy) for dy in O_ORDER for dx in range(2) if (dx, dy) != (0, 0)]
    near = [s for s in others if s[1] != FAR]
    barrier = pltpu.get_barrier_semaphore()
    for dx, dy in others:
        pl.semaphore_signal(barrier, inc=1, device_id={"cp": pt.peer(dx, dy)}, device_id_type=MESH)
    pl.semaphore_wait(barrier, len(others))

    def put(src, dst, send, recv, dev):
        return pltpu.make_async_remote_copy(src, dst, send, recv, device_id={"cp": dev}, device_id_type=MESH)

    way = (1, -1)
    turn = {FAR: 0, 1: 1, -1: 2, 0: 3}

    def source(half, dx, dy):
        return o_in.at[pt.slot(dx, dy)] if half else ol.at[turn[dy], lax.rem(pt.x + dx, 2)]

    def o_copy(half, i):
        dx, dy = near[i]
        return put(source(half, dx, dy), obuf.at[my_head, highs if half else lows], o_send.at[half, i], o_recv.at[half, my_head],
                   pt.peer(dx, dy))

    def o_hop(half, dx):
        return put(source(half, dx, FAR), robuf.at[half, dx], o_send.at[half, len(near) + dx], ro_recv.at[half, dx],
                   pt.peer(0, way[dx]))

    def o_hand(half, dx):
        head = pt.head(0, -way[dx])
        return put(robuf.at[half, dx], obuf.at[head, highs if half else lows], ro_send.at[half, dx], o_recv.at[half, head],
                   pt.peer(dx, way[dx]))

    def hand_on(half):
        for dx in range(2):
            put(robuf.at[half, dx], robuf.at[half, dx], o_send.at[0, 0], ro_recv.at[half, dx], me).wait_recv()
            o_hand(half, dx).start()

    for dx in range(2):
        o_hop(1, dx).start()
    for i in range(len(near)):
        o_copy(1, i).start()

    for cp in seg_copies + q_copies:
        cp.wait()

    @pl.loop(0, n)
    def _(p):
        load(p).wait()

    pairs = Pairs(pt, n, g, scale, lambda src, half: seg_s[src, half, 0], seg_v, kvs, qs, t_sc, acc_sc)

    def send_low(dy):
        if dy == FAR:
            for dx in range(2):
                o_hop(0, dx).start()
        else:
            for i, (dx, to) in enumerate(near):
                if to == dy:
                    o_copy(0, i).start()

    def one(i, carry):
        turned = jnp.where(i == 2, -1, jnp.where(i == 3, 0, FAR - i))
        row = lax.rem(pt.y + turned + pt.side, pt.side)

        def store(u, w, val):
            ol[i, u, :, w * DH:(w + 1) * DH] = val

        pairs(row, 0, 0, pairs.begins(row, 0), store)

        @pl.when(i == 1)
        def _():
            send_low(FAR)
            hand_on(1)

        @pl.when(i == 2)
        def _():
            send_low(1)

        @pl.when(i == 3)
        def _():
            send_low(-1)

        return carry

    lax.fori_loop(0, ng // 2, one, 0)
    send_low(0)
    obuf[my_head, 0:PC] = ol[turn[0], lax.rem(pt.x, 2)]
    hand_on(0)

    for t, dy in enumerate(O_ORDER):
        for cp in w_copies(t):
            cp.wait()
        heads = [pt.head(dx, dy) for dx in range(2)]
        for dx in range(2):
            if dy == 0 and dx == 0:
                own.wait()
            else:
                for half in range(2):
                    put(ol.at[0, 0], obuf.at[heads[dx], highs if half else lows], o_send.at[0, 0], o_recv.at[half, heads[dx]],
                        me).wait_recv()
        a = jnp.concatenate([obuf[heads[0]], obuf[heads[1]]], axis=1)
        for u in range(nc):
            r = jnp.dot(a, wob[t, :, u * wn:(u + 1) * wn], preferred_element_type=jnp.float32)
            if t > 0:
                r = r + acc[:, u * wn:(u + 1) * wn]
            if t < len(O_ORDER) - 1:
                acc[:, u * wn:(u + 1) * wn] = r
            else:
                y_ref[:, u * wn:(u + 1) * wn] = r.astype(y_ref.dtype)
    for half in range(2):
        for i in range(len(near)):
            o_copy(half, i).wait_send()
        for dx in range(2):
            o_hop(half, dx).wait_send()
            o_hand(half, dx).wait_send()


def solution(mesh):
    n = mesh.shape["cp"]
    side = math.isqrt(n // 2)
    bf, f32 = jnp.bfloat16, jnp.float32
    vmem, anym = pl.BlockSpec(memory_space=pltpu.VMEM), pl.BlockSpec(memory_space=pltpu.HBM)
    dma = pltpu.SemaphoreType.DMA

    def local(x, seg, wq, wk, wv, wo):
        lq, d = x.shape
        hkv = wk.shape[1] // DH
        g = wq.shape[1] // wk.shape[1]
        gd = g * DH
        ng = 2 * side
        kv, q, segs = pl.pallas_call(
            functools.partial(_project, n, g),
            out_shape=(jax.ShapeDtypeStruct((n, 2, 2, PC, DH), bf), jax.ShapeDtypeStruct((ng, 2, g, PC, DH), bf),
                       jax.ShapeDtypeStruct((n, 2, PC), jnp.int32)),
            in_specs=[vmem, vmem, anym, anym, anym],
            out_specs=(anym, anym, vmem),
            scratch_shapes=[
                pltpu.VMEM((2, side, d // side, hkv * DH), bf), pltpu.VMEM((side, d // side, hkv * gd), bf),
                pltpu.VMEM((2, lq, hkv * DH), f32), pltpu.VMEM((lq, hkv * gd), f32),
                pltpu.VMEM((n, 2, 2, PC, DH), bf), pltpu.VMEM((ng, 2, g, PC, DH), bf),
                pltpu.VMEM((ng, 2, 2, PC, DH), bf), pltpu.VMEM((ng, 2, g, PC, DH), bf),
                pltpu.VMEM((2, 2, 2, PC, DH), bf), pltpu.VMEM((2, 2, g, PC, DH), bf), pltpu.VMEM((n, 2, PC), jnp.int32),
                dma((2, side)), dma((side,)), dma((ng + 2,)), dma((n,)), dma((2, 2)), dma((2, 2)), dma((2, 2)),
                dma((ng,)), dma((2 * ng,)),
                dma((ng + 2,)), dma((ng,)), dma((2, 2)), dma((2, 2)), dma((2, 2)), dma((n,)), dma((n,)), dma((n,)), dma((ng,)),
            ],
            compiler_params=pltpu.CompilerParams(collective_id=0, has_side_effects=True, vmem_limit_bytes=60 << 20),
            name="project",
        )(x, seg.reshape(1, 2, PC), wk, wv, wq)
        scale = DH ** -0.5 * math.log2(math.e)
        o = pl.pallas_call(
            functools.partial(_attend, n, g, scale),
            out_shape=jax.ShapeDtypeStruct((ng, PC, gd), bf),
            in_specs=[anym] * 3,
            out_specs=anym,
            scratch_shapes=[pltpu.SMEM((n, 2, PC), jnp.int32), pltpu.VMEM((n, 2, PC), jnp.int32),
                            pltpu.VMEM((2 * n, 2, PC, DH), bf), pltpu.VMEM((ng, g, PC, DH), bf),
                            pltpu.VMEM((ng, PC, gd), bf), pltpu.SMEM((ng,), jnp.int32)] + _pair_scratch(g) + [dma((2,)), dma, dma, dma],
            compiler_params=pltpu.CompilerParams(vmem_limit_bytes=60 << 20),
            name="attend",
        )(segs, kv, q)
        return pl.pallas_call(
            functools.partial(_combine, n, g, scale),
            out_shape=jax.ShapeDtypeStruct((lq, wo.shape[1]), bf),
            in_specs=[anym] * 5,
            out_specs=vmem,
            scratch_shapes=[pltpu.VMEM((hkv, lq, gd), bf), pltpu.VMEM((2, 2, PC, gd), bf), pltpu.VMEM((ng // 2, 2, PC, gd), bf),
                            pltpu.VMEM((side, 2 * gd, wo.shape[1]), bf), pltpu.VMEM((lq, wo.shape[1]), f32),
                            pltpu.SMEM((n, 2, PC), jnp.int32), pltpu.VMEM((n, 2, PC), jnp.int32),
                            pltpu.VMEM((n, 2, PC, DH), bf), pltpu.VMEM((ng, g, PC, DH), bf)] + _pair_scratch(g) + [
                            dma((side, 2)), dma((2, ng)), dma((2, ng)), dma((2, 2)), dma((2, 2)), dma((2,)), dma((n,)), dma((ng,))],
            compiler_params=pltpu.CompilerParams(collective_id=1, has_side_effects=True, vmem_limit_bytes=60 << 20),
            name="combine",
        )(segs, kv, q, o, wo)

    rows = P(("dp", "cp"), None)
    return jax.shard_map(local, mesh=mesh, in_specs=(rows, P(("dp", "cp")), P(), P(), P(), P()), out_specs=rows, check_vma=False)
```
